32 devices in a mesh: groups: 2 (over x), expert: 16 (over z, y, core).
Axes of the slice: x: 2, y: 2, z: 4, core: 2. Of those that a mesh axis runs over, the one named last changes fastest.
Arguments:
- tokens: bfloat16 [512, 6144], P(('groups', 'expert')), parts along dimension 0, may hold values from -6 to 6
- route_ids: int32 [512, 2], P(('groups', 'expert')), parts along dimension 0, may hold values from 0 to 7, all different within a row; in each aligned block of 16 rows (0 to 15, 16 to 31, ...) at most 6 rows name the same one
- route_logits: float32 [512, 2], P(('groups', 'expert')), parts along dimension 0, may hold values from -6 to 6
- old_place: int32 [16], replicated, may hold values from 0 to 15, each once
- new_place: int32 [16], replicated, may hold values from 0 to 15, each once
- held_gate: bfloat16 [32, 6144, 128], P(('groups', 'expert')), parts along dimension 0, may hold values from -0.078125 to 0.078125
- held_up: bfloat16 [32, 6144, 128], P(('groups', 'expert')), parts along dimension 0, may hold values from -0.078125 to 0.078125
- held_down: bfloat16 [32, 6144, 128], P(('groups', 'expert')), parts along dimension 0, may hold values from -0.375 to 0.375
Outputs:
- moe_output: bfloat16 [512, 6144], P(('groups', 'expert')), parts along dimension 0
- moved_gate: bfloat16 [32, 6144, 128], P(('groups', 'expert')), parts along dimension 0
- moved_up: bfloat16 [32, 6144, 128], P(('groups', 'expert')), parts along dimension 0
- moved_down: bfloat16 [32, 6144, 128], P(('groups', 'expert')), parts along dimension 0
The draws below stay inside these ranges and needn't reach their ends.
There are 2 independent parts, one for each index of `groups`. The reference program is written for one: setup_inputs(seed, part) draws one part's arguments, and reference() takes and returns one part's arrays. A program takes and returns all parts, laid end to end along the dimension named above; an argument that names none is the same for every part. Nothing has to cross between parts.
Inputs may be any that keep to these rules, and one draw needn't show every extreme that they name: `route_ids`: within the rows of one device (aligned blocks of 16 rows) no expert is named by more than 6 rows, a bound that some block reaches; the two ids of a row differ. `old_place`: each device appears once. `new_place`: each device appears once.
All inputs are finite; a program needn't handle non-finite values.
Results may differ from the reference program's by a relative error of at most 0.0058.
Values may be sent and summed in bfloat16 or wider, within the bound.
A program may use at most 128 MiB of HBM per device.

```python
import math
import jax
import jax.numpy as jnp
import numpy as np
from jax import lax

D = 6144
F_SLOT = 128
EXPERTS = 8
TOP = 2
TOK_DEV = 16
CAP = 6
BLOCKS = 2
HIDDEN_SIZE = 256
TOKENS = 256
N_EXPERT = 16


def levels(stream_key, shape, pieces, low, top_value):
    gain, own = 1.0, jax.random.fold_in(stream_key, 6)
    for axis_at, shards_of in pieces:
        heights = jnp.exp(jax.random.uniform(jax.random.fold_in(own, axis_at), (shards_of,), jnp.float32, low / len(pieces), top_value / len(pieces)))
        gain = gain * jnp.repeat(heights, shape[axis_at] // shards_of).reshape([-1 if axis == axis_at else 1 for axis in range(len(shape))])
    return gain


def routed_block(key, own, number, rows, count, top, limit, slope):
    sequence = jax.random.permutation(key, count)
    heavy_load, usual = load_shares(count, rows * top, limit, slope, True), load_shares(count, rows * top, limit, slope, False)
    places = jnp.arange(count)

    def named(tallies, rotation):
        used = int((tallies > 0).sum())
        fixed = max(1, used // 4)
        shifted = fixed + (places - fixed + rotation * (used - fixed)) % max(1, count - fixed)
        return jnp.zeros((count,), jnp.int32).at[sequence[jnp.where(places < fixed, places, shifted)]].set(jnp.asarray(tallies, jnp.int32))

    tallies = jnp.where(number % 4 == 0, named(heavy_load, number // 4), named(usual, number - number // 4 - 1))
    mixed = jax.random.permutation(jax.random.fold_in(own, 3), count)
    giver, taker = mixed[0:count // 2 * 2:2], mixed[1:count // 2 * 2:2]
    room = jnp.minimum(tallies[giver] - 1, limit - tallies[taker]) // 2
    room = jnp.where((giver == sequence[0]) | (taker == sequence[0]) | (tallies[taker] == 0), 0, jnp.maximum(room, 0))
    shifted = jax.random.randint(jax.random.fold_in(own, 4), (count // 2,), 0, 1 << 20) % (room + 1)
    tallies = tallies.at[giver].add(-shifted).at[taker].add(shifted)
    items = jnp.searchsorted(jnp.cumsum(tallies), jnp.arange(rows * top), side="right").astype(jnp.int32)
    table = items.reshape(top, rows).T
    table = table[jax.random.permutation(jax.random.fold_in(own, 1), rows)]
    rotation = jax.random.randint(jax.random.fold_in(own, 2), (rows, 1), 0, top)
    return jnp.take_along_axis(table, (jnp.arange(top)[None, :] + rotation) % top, axis=1)


def load_shares(count, total, most, skew, full):
    loads = [(1 << 20) // math.isqrt(rank ** skew) + 1 for rank in range(1, count + 1)]
    largest = most if full else min(most, max(-(-total // count), total * loads[0] // sum(loads)))
    least = 1 if total - largest >= count - 1 else 0
    holding, spare = [largest] + [least] * (count - 1), total - largest - least * (count - 1)
    while spare > 0:
        movable = [i for i in range(1, count) if holding[i] < largest] or [i for i in range(1, count) if holding[i] < most]
        mass, left = sum([loads[i] for i in movable]), spare
        for i in movable:
            extra = min(most - holding[i], max(1, left * loads[i] // mass), spare)
            holding[i] = holding[i] + extra
            spare = spare - extra
    return np.array(holding)


def noise(stream_key, extent, spread, bound, pieces=(), kind=jnp.bfloat16):
    drawn = jax.random.normal(stream_key, extent, jnp.float32) * spread
    if len(pieces) > 0:
        drawn = levels(stream_key, extent, pieces, -0.22, 0.18) * drawn
    return jnp.clip(drawn, min=-bound, max=bound).astype(kind)


def setup_inputs(seed: int = 0, part: int = 0) -> dict:
    streams_of = jax.random.split(jax.random.key(seed), 9)
    part_keys = jax.random.split(jax.random.fold_in(streams_of[8], part), 9)
    tokens = noise(part_keys[0], (TOKENS, D), 1.0, 6.0, ((0, 16),))
    route_ids_keys = jax.random.split(jax.random.fold_in(part_keys[1], 1), TOKENS // TOK_DEV)
    route_ids_turns = jax.random.permutation(jax.random.fold_in(part_keys[1], 3), TOKENS // TOK_DEV)
    route_ids = jax.vmap(lambda own, number: routed_block(jax.random.fold_in(part_keys[1], 2), own, number, TOK_DEV, EXPERTS, TOP, CAP, 2))(route_ids_keys, route_ids_turns).reshape((TOKENS, TOP))
    route_logits = noise(part_keys[2], (TOKENS, TOP), 1.5, 6.0, ((0, 16),), jnp.float32)
    old_place = jax.random.permutation(streams_of[3], N_EXPERT).astype(jnp.int32)
    new_place = jax.random.permutation(streams_of[4], N_EXPERT).astype(jnp.int32)
    held_gate = noise(part_keys[5], (N_EXPERT, D, F_SLOT), D ** -0.5, 0.078125, ((0, 16),))
    held_up = noise(part_keys[6], (N_EXPERT, D, F_SLOT), D ** -0.5, 0.078125, ((0, 16),))
    held_down = noise(part_keys[7], (N_EXPERT, D, F_SLOT), HIDDEN_SIZE ** -0.5, 0.375, ((0, 16),))
    return dict(tokens=tokens, route_ids=route_ids, route_logits=route_logits, old_place=old_place, new_place=new_place, held_gate=held_gate, held_up=held_up, held_down=held_down)


def reference(tokens, route_ids, route_logits, old_place, new_place, held_gate, held_up, held_down):
    device_ids = jnp.arange(N_EXPERT, dtype=jnp.int32)
    slot_new_at = jnp.sum(jnp.where(new_place[:, None] == device_ids[None, :], device_ids[:, None], 0), axis=0).astype(jnp.int32)
    source_of = jnp.take(old_place, slot_new_at).astype(jnp.int32)
    moved_gate = jnp.take(held_gate, source_of, axis=0)
    moved_up = jnp.take(held_up, source_of, axis=0)
    moved_down = jnp.take(held_down, source_of, axis=0)
    first_weight = 1.0 / (1.0 + jnp.exp(route_logits[:, 1] - route_logits[:, 0]))
    second_weight = 1.0 / (1.0 + jnp.exp(route_logits[:, 0] - route_logits[:, 1]))
    weights = jnp.stack([first_weight, second_weight], axis=1).astype(jnp.float32)
    expert_ids = jnp.arange(EXPERTS, dtype=jnp.int32)
    route_hits = route_ids[:, :, None] == expert_ids[None, None, :]
    coefficient = jnp.sum(jnp.where(route_hits, weights[:, :, None], 0.0), axis=1).astype(jnp.float32)
    routed = jnp.any(route_hits, axis=1)

    def listing(column):
        return jnp.nonzero(column, size=N_EXPERT * CAP, fill_value=TOKENS)[0].astype(jnp.int32)

    index_table = jax.vmap(listing)(routed.T)
    padded_tokens = jnp.concatenate([tokens, jnp.zeros((1, D), jnp.bfloat16)], axis=0)
    padded_coeff = jnp.concatenate([coefficient, jnp.zeros((1, EXPERTS), jnp.float32)], axis=0)

    def apply_slot(slot_index, accumulated):
        expert_index = slot_index // BLOCKS
        row_index = jnp.take(index_table, expert_index, axis=0).astype(jnp.int32)
        slot_rows = jnp.take(padded_tokens, row_index, axis=0)
        holder = jnp.take(old_place, slot_index).astype(jnp.int32)
        w_gate = jnp.take(held_gate, holder, axis=0)
        w_up = jnp.take(held_up, holder, axis=0)
        w_down = jnp.take(held_down, holder, axis=0)
        gate_value = jnp.dot(slot_rows, w_gate, preferred_element_type=jnp.float32)
        up_value = jnp.dot(slot_rows, w_up, preferred_element_type=jnp.float32)
        hidden = (jax.nn.silu(gate_value) * up_value).astype(jnp.bfloat16)
        partial_value = jnp.dot(hidden, w_down.T, preferred_element_type=jnp.float32).astype(jnp.bfloat16)
        partial_value = lax.optimization_barrier(partial_value).astype(jnp.float32)
        scaling = jnp.take(padded_coeff, row_index, axis=0)[:, expert_index]
        return accumulated.at[row_index].add(scaling[:, None] * partial_value)

    start = jnp.zeros((TOKENS + 1, D), jnp.float32)
    summed = lax.fori_loop(0, N_EXPERT, apply_slot, start)
    moe_output = summed[:TOKENS].astype(jnp.bfloat16)
    return moe_output, moved_gate, moved_up, moved_down
```

```python
import functools

import jax
import jax.numpy as jnp
from jax import lax
from jax.experimental import pallas as pl
from jax.experimental.pallas import tpu as pltpu
from jax.sharding import PartitionSpec as P

EXPERTS = 8
LANES = 128
MESH = pl.DeviceIdType.MESH
VMEM_BYTES = 63_000_000


def near_square_root(n):
    size = 1
    while size * size < n:
        size *= 2
    return size


def layer_kernel(
    n,
    most,
    table,
    tok,
    coef,
    held_g,
    held_u,
    held_d,
    out,
    moved_g,
    moved_u,
    moved_d,
    tok_all,
    coef_all,
    w_gu,
    w_d,
    pieces_g,
    pieces_u,
    pieces_d,
    crossed_g,
    crossed_u,
    crossed_d,
    ordered,
    hidden,
    contrib,
    part_in,
    plane_sum,
    half_in,
    cross_out,
    cross_in,
    load_sem,
    tok_send,
    fwd_send,
    plane_send,
    tok_recv,
    one_send,
    one_recv,
    two_send,
    two_recv,
    three_send,
    three_recv,
    part_send,
    part_recv,
    half_send,
    half_recv,
    cross_send,
    cross_recv,
):
    me = lax.axis_index("expert")
    half = n // 2
    base = (me // half) * half
    lane = me - base
    twin = lax.rem(me + half, n)
    rows, width = tok.shape
    band = width // half
    size = near_square_root(n)
    planes = n // size
    half_planes = planes // 2
    plane = me // size
    seat = me - plane * size
    my_plane_of_half = lane // size
    held = (held_g, held_u, held_d)
    moved = (moved_g, moved_u, moved_d)
    pieces = (pieces_g, pieces_u, pieces_d)
    crossed = (crossed_g, crossed_u, crossed_d)

    barrier = pltpu.get_barrier_semaphore()

    @pl.loop(1, n)
    def _(k):
        pl.semaphore_signal(
            barrier, inc=1, device_id={"expert": lax.rem(me + k, n)}, device_id_type=MESH
        )

    loads = (
        pltpu.make_async_copy(held_g.at[0], w_gu.at[:, pl.ds(0, LANES)], load_sem.at[0]),
        pltpu.make_async_copy(held_u.at[0], w_gu.at[:, pl.ds(LANES, LANES)], load_sem.at[1]),
        pltpu.make_async_copy(held_d.at[0], w_d, load_sem.at[2]),
    )
    for load in loads:
        load.start()

    def token_rows(owner):
        return pl.ds(pl.multiple_of(owner * rows, rows), rows)

    def band_rows(owner):
        return pl.ds(pl.multiple_of(owner * band, band), band)

    def near(k):
        return base + lax.rem(lane + k, half)

    def column(k):
        return base + lax.rem(lane + k * size, half)

    def mate(k):
        return plane * size + lax.rem(seat + k, size)

    def seated(other_plane):
        return other_plane * size + seat

    tok_all[token_rows(me), :] = tok[...]
    coef_all[token_rows(me), :] = coef[...]
    pl.semaphore_wait(barrier, n - 1)

    def send(source, target, send_sem, recv_sem, peer):
        return pltpu.make_async_remote_copy(
            src_ref=source, dst_ref=target, send_sem=send_sem, recv_sem=recv_sem,
            device_id={"expert": peer}, device_id_type=MESH,
        )

    def own_tokens(peer):
        at = token_rows(me)
        return (
            send(tok, tok_all.at[at], tok_send.at[0, peer], tok_recv.at[0, me], peer),
            send(coef, coef_all.at[at], tok_send.at[1, peer], tok_recv.at[1, me], peer),
        )

    def passed_tokens(owner, peer, sems):
        at = token_rows(owner)
        return (
            send(tok_all.at[at], tok_all.at[at], sems[0], tok_recv.at[0, owner], peer),
            send(coef_all.at[at], coef_all.at[at], sems[1], tok_recv.at[1, owner], peer),
        )

    def twin_tokens(peer):
        return passed_tokens(twin, peer, (fwd_send.at[0, peer], fwd_send.at[1, peer]))

    def plane_tokens(other_plane, k):
        sems = (plane_send.at[0, other_plane, k], plane_send.at[1, other_plane, k])
        return passed_tokens(seated(other_plane), mate(k), sems)

    def tokens_arrive(owner):
        pltpu.make_async_copy(tok, tok_all.at[token_rows(owner)], tok_recv.at[0, owner]).wait()
        pltpu.make_async_copy(coef, coef_all.at[token_rows(owner)], tok_recv.at[1, owner]).wait()

    def spread(array):
        pltpu.make_async_copy(
            held[array].at[0, band_rows(lane)], pieces[array].at[lane], one_recv.at[array]
        ).start()

        @pl.loop(1, half)
        def _(k):
            peer = near(k)
            send(
                held[array].at[0, band_rows(peer - base)], pieces[array].at[lane],
                one_send.at[array], one_recv.at[array], peer,
            ).start()

    def swap(array):
        return send(
            ordered.at[array, pl.ds(0, most)], crossed[array],
            two_send.at[array], two_recv.at[array], twin,
        )

    def cross_over(array):
        pltpu.make_async_copy(pieces[array], pieces[array], one_recv.at[array]).wait()

        @pl.loop(0, most)
        def _(m):
            ordered[array, m] = pieces[array][table[base + m]]

        swap(array).start()

    def deliver(array):
        swap(array).wait()

        @pl.loop(0, half)
        def _(place):
            at = base + place
            own = pieces[array][table[2 * n + at]]
            other = crossed[array][table[3 * n + at]]
            ordered[array, place] = jnp.where(table[n + at] == 1, other, own)

        pltpu.make_async_copy(
            ordered.at[array, lane], moved[array].at[0, band_rows(lane)], three_recv.at[array]
        ).start()

        @pl.loop(1, half)
        def _(k):
            peer = near(k)
            send(
                ordered.at[array, peer - base], moved[array].at[0, band_rows(lane)],
                three_send.at[array], three_recv.at[array], peer,
            ).start()

    for copy in own_tokens(twin):
        copy.start()

    @pl.loop(1, half_planes)
    def _(k):
        for copy in own_tokens(column(k)):
            copy.start()

    @pl.loop(1, size)
    def _(k):
        for copy in own_tokens(mate(k)):
            copy.start()

    spread(0)
    tokens_arrive(twin)

    @pl.loop(1, half_planes)
    def _(k):
        for copy in twin_tokens(column(k)):
            copy.start()

    spread(1)

    @pl.loop(1, half_planes)
    def _(k):
        tokens_arrive(column(k))
        tokens_arrive(lax.rem(column(k) + half, n))

    @pl.loop(1, planes)
    def _(shift):
        @pl.loop(1, size)
        def _(k):
            for copy in plane_tokens(lax.rem(plane + shift, planes), k):
                copy.start()

    spread(2)
    cross_over(0)
    cross_over(1)

    @pl.loop(0, planes)
    def _(other_plane):
        @pl.loop(1, size)
        def _(k):
            tokens_arrive(other_plane * size + lax.rem(seat + k, size))

    for load in loads:
        load.wait()

    step = min(256, n * rows)
    columns = 512

    @pl.loop(0, n * rows // step)
    def _(block):
        at = pl.ds(pl.multiple_of(block * step, step), step)
        both = jnp.dot(tok_all[at, :], w_gu[...], preferred_element_type=jnp.float32)
        gate_value = both[:, :LANES]
        up_value = both[:, LANES:]
        hidden[...] = (gate_value / (1.0 + jnp.exp(-gate_value)) * up_value).astype(jnp.bfloat16)
        lanes = lax.broadcasted_iota(jnp.int32, (step, LANES), 1)
        scale = jnp.sum(jnp.where(lanes == me, coef_all[at, :], 0.0), axis=1, keepdims=True)

        @pl.loop(0, width // columns)
        def _(part):
            cols = pl.ds(pl.multiple_of(part * columns, columns), columns)
            value = lax.dot_general(
                hidden[...], w_d[cols, :], (((1,), (1,)), ((), ())),
                preferred_element_type=jnp.float32,
            )
            value = value.astype(jnp.bfloat16).astype(jnp.float32)
            contrib[at, cols] = (value * scale).astype(jnp.bfloat16)

    def part_copy(k, other_plane):
        peer = mate(k)
        owner = other_plane * size + lax.rem(seat + k, size)
        return send(
            contrib.at[token_rows(owner)], part_in.at[seat, other_plane],
            part_send.at[k, other_plane], part_recv.at[seat, other_plane], peer,
        )

    def half_copy(k, kind):
        peer = column(k)
        target = peer // size if kind == 0 else lax.rem(peer // size + half_planes, planes)
        return send(
            plane_sum.at[target], half_in.at[kind, my_plane_of_half],
            half_send.at[kind, k], half_recv.at[kind, my_plane_of_half], peer,
        )

    @pl.loop(0, planes)
    def _(other_plane):
        @pl.loop(1, size)
        def _(k):
            part_copy(k, other_plane).start()

    def add_plane():
        @pl.loop(0, planes)
        def _(other_plane):
            @pl.loop(1, size)
            def _(k):
                spot = part_in.at[lax.rem(seat + k, size), other_plane]
                pltpu.make_async_copy(
                    spot, spot, part_recv.at[lax.rem(seat + k, size), other_plane]
                ).wait()

            @pl.loop(0, width // columns)
            def _(part):
                cols = pl.ds(pl.multiple_of(part * columns, columns), columns)

                def more(k, total):
                    other = lax.rem(seat + k, size)
                    return total + part_in[other, other_plane, :, cols].astype(jnp.float32)

                total = contrib[token_rows(seated(other_plane)), cols].astype(jnp.float32)
                total = lax.fori_loop(1, size, more, total)
                plane_sum[other_plane, :, cols] = total.astype(jnp.bfloat16)

        for kind in (1, 0):

            @pl.loop(1, half_planes)
            def _(k):
                half_copy(k, kind).start()

    def add_half(kind, own_plane, extra, target):
        @pl.loop(1, half_planes)
        def _(k):
            other = lax.rem(my_plane_of_half + k, half_planes)
            spot = half_in.at[kind, other]
            pltpu.make_async_copy(spot, spot, half_recv.at[kind, other]).wait()

        @pl.loop(0, width // columns)
        def _(part):
            cols = pl.ds(pl.multiple_of(part * columns, columns), columns)

            def more(k, total):
                other = lax.rem(my_plane_of_half + k, half_planes)
                return total + half_in[kind, other, :, cols].astype(jnp.float32)

            total = plane_sum[own_plane, :, cols].astype(jnp.float32)
            if extra is not None:
                total = total + extra[:, cols].astype(jnp.float32)
            target[:, cols] = lax.fori_loop(1, half_planes, more, total).astype(jnp.bfloat16)

    deliver(0)
    cross_over(2)
    add_plane()
    deliver(1)
    add_half(1, lax.rem(plane + half_planes, planes), None, cross_out)
    cross = send(cross_out, cross_in, cross_send, cross_recv, twin)
    cross.start()
    deliver(2)
    cross.wait()
    add_half(0, plane, cross_in, out)

    for copy in own_tokens(twin):
        copy.wait_send()

    @pl.loop(1, half_planes)
    def _(k):
        for copy in own_tokens(column(k)):
            copy.wait_send()
        for copy in twin_tokens(column(k)):
            copy.wait_send()
        half_copy(k, 0).wait_send()
        half_copy(k, 1).wait_send()

    @pl.loop(1, size)
    def _(k):
        for copy in own_tokens(mate(k)):
            copy.wait_send()

        @pl.loop(0, planes)
        def _(other_plane):
            part_copy(k, other_plane).wait_send()

        @pl.loop(1, planes)
        def _(shift):
            for copy in plane_tokens(lax.rem(plane + shift, planes), k):
                copy.wait_send()

    for array in range(3):
        sent = pieces[array].at[pl.ds(0, half - 1)]
        pltpu.make_async_copy(sent, sent, one_send.at[array]).wait()
        pltpu.make_async_copy(sent, sent, three_send.at[array]).wait()
        pltpu.make_async_copy(
            moved[array].at[0], moved[array].at[0], three_recv.at[array]
        ).wait()


def call_layer(n, most, which, table, tokens, coef, held_gate, held_up, held_down):
    rows, width = tokens.shape
    half = n // 2
    band = width // half
    size = near_square_root(n)
    planes = n // size
    vmem = pl.BlockSpec(memory_space=pltpu.VMEM)
    anywhere = pl.BlockSpec(memory_space=pl.ANY)
    dma = pltpu.SemaphoreType.DMA
    moved_shape = jax.ShapeDtypeStruct(held_gate.shape, held_gate.dtype)

    def block(*shape):
        return pltpu.VMEM(shape, jnp.bfloat16)

    return pl.pallas_call(
        functools.partial(layer_kernel, n, most),
        out_shape=(jax.ShapeDtypeStruct((rows, width), jnp.bfloat16),) + (moved_shape,) * 3,
        in_specs=[pl.BlockSpec(memory_space=pltpu.SMEM), vmem, vmem] + [anywhere] * 3,
        out_specs=(vmem, anywhere, anywhere, anywhere),
        scratch_shapes=[
            block(n * rows, width),
            pltpu.VMEM((n * rows, LANES), jnp.float32),
            block(width, 2 * LANES),
            block(width, LANES),
            block(half, band, LANES),
            block(half, band, LANES),
            block(half, band, LANES),
            block(most, band, LANES),
            block(most, band, LANES),
            block(most, band, LANES),
            block(3, half, band, LANES),
            block(min(256, n * rows), LANES),
            block(n * rows, width),
            block(size, planes, rows, width),
            block(planes, rows, width),
            block(2, planes // 2, rows, width),
            block(rows, width),
            block(rows, width),
            dma((3,)),
            dma((2, n)),
            dma((2, n)),
            dma((2, planes, size)),
            dma((2, n)),
            dma((3,)),
            dma((3,)),
            dma((3,)),
            dma((3,)),
            dma((3,)),
            dma((3,)),
            dma((size, planes)),
            dma((size, planes)),
            dma((2, planes // 2)),
            dma((2, planes // 2)),
            dma,
            dma,
        ],
        compiler_params=pltpu.CompilerParams(
            collective_id=which, has_side_effects=True, vmem_limit_bytes=VMEM_BYTES
        ),
    )(table, tokens, coef, held_gate, held_up, held_down)


def chunk_plan(quarter, cuts):
    plan = []
    for array in range(3):
        start = 0
        for cut in cuts[array]:
            size = quarter * cut // 16
            plan.append((array, start, size))
            start += size
        assert start == quarter
    return tuple(plan)


def line_kernel(n, most, plan, table, tok, coef, held_g, held_u, held_d, out, moved_g, moved_u, moved_d, *rest):
    count = len(plan)
    gathered, rest = rest[:count], rest[count:]
    crossed, rest = rest[:count], rest[count:]
    (
        leaving, ordered, tok_all, coef_all, w_g, w_u, w_d, hidden, contrib,
        pair_in, side_out, side_in, plane_sum, chain_in, chain_out,
        load_sem, tok_send, tok_recv,
        one_send, one_recv, two_send, two_recv, cross_send, cross_recv,
        back_send, back_recv, three_send, three_recv,
        pair_send, pair_recv, side_send, side_recv, chain_send, chain_recv,
    ) = rest
    size = 4
    last = n // size - 1
    me = lax.axis_index("expert")
    plane = me // size
    seat = me - plane * size
    half = plane // 2
    base = half * (n // 2)
    own_at = lax.rem(plane, 2) * size
    other_at = size - own_at
    inner = (plane == 1) | (plane == 2)
    outer = (plane == 0) | (plane == last)
    side = lax.rem(seat + 2, size)
    pair = seat + 1 - 2 * lax.rem(seat, 2)
    diagonal = lax.rem(pair + 2, size)
    rows, width = tok.shape
    quarter = width // size
    held = (held_g, held_u, held_d)
    moved = (moved_g, moved_u, moved_d)

    def at_plane(other, other_seat):
        return other * size + other_seat

    barrier = pltpu.get_barrier_semaphore()

    def greet(peer):
        pl.semaphore_signal(barrier, inc=1, device_id={"expert": peer}, device_id_type=MESH)

    @pl.loop(1, size)
    def _(k):
        greet(at_plane(plane, lax.rem(seat + k, size)))

    @pl.when(plane > 0)
    def _():
        greet(me - size)

    @pl.when(plane < last)
    def _():
        greet(me + size)

    loads = (
        pltpu.make_async_copy(held_g.at[0], w_g, load_sem.at[0]),
        pltpu.make_async_copy(held_u.at[0], w_u, load_sem.at[1]),
        pltpu.make_async_copy(held_d.at[0], w_d, load_sem.at[2]),
    )
    for load in loads:
        load.start()

    def token_rows(owner):
        return pl.ds(pl.multiple_of(owner * rows, rows), rows)

    tok_all[token_rows(me), :] = tok[...]
    coef_all[token_rows(me), :] = coef[...]

    @pl.when(inner)
    def _():
        pl.semaphore_wait(barrier, size + 1)

    @pl.when(outer)
    def _():
        pl.semaphore_wait(barrier, size)

    def send(source, target, send_sem, recv_sem, peer):
        return pltpu.make_async_remote_copy(
            src_ref=source, dst_ref=target, send_sem=send_sem, recv_sem=recv_sem,
            device_id={"expert": peer}, device_id_type=MESH,
        )

    def landed(spot, sem):
        pltpu.make_async_copy(spot, spot, sem).wait()

    def tokens_to(owner_plane, owner_seat, peer, path):
        owner = at_plane(owner_plane, owner_seat)
        at = token_rows(owner)
        return (
            send(tok_all.at[at], tok_all.at[at], tok_send.at[0, owner_plane, path], tok_recv.at[0, owner], peer),
            send(coef_all.at[at], coef_all.at[at], tok_send.at[1, owner_plane, path], tok_recv.at[1, owner], peer),
        )

    def tokens_arrive(owner_plane, owner_seat):
        owner = at_plane(owner_plane, owner_seat)
        landed(tok_all.at[token_rows(owner)], tok_recv.at[0, owner])
        landed(coef_all.at[token_rows(owner)], tok_recv.at[1, owner])

    def start(copies):
        for copy in copies:
            copy.start()

    def up(q):
        return tokens_to(q, seat, me + size, 0)

    def down(q):
        return tokens_to(q, seat, me - size, 1)

    def across(q):
        return tokens_to(q, seat, at_plane(plane, side), 2)

    def beside(q):
        return tokens_to(q, seat, at_plane(plane, pair), 3)

    def beside_again(q):
        return tokens_to(q, side, at_plane(plane, pair), 4)

    def own_tokens_along():
        @pl.when(plane < last)
        def _():
            start(up(plane))

        @pl.when(plane > 0)
        def _():
            start(down(plane))

    def own_tokens_across():
        start(across(plane))
        start(beside(plane))

    def tokens_step(far):
        @pl.when(plane >= far)
        def _():
            q = plane - far
            tokens_arrive(q, seat)

            @pl.when(plane < last)
            def _():
                start(up(q))

            start(across(q))
            start(beside(q))

        @pl.when(plane + far <= last)
        def _():
            q = plane + far
            tokens_arrive(q, seat)

            @pl.when(plane > 0)
            def _():
                start(down(q))

            start(across(q))
            start(beside(q))

    def tokens_relay(far):
        @pl.when(plane >= far)
        def _():
            tokens_arrive(plane - far, side)
            start(beside_again(plane - far))

        if far:

            @pl.when(plane + far <= last)
            def _():
                tokens_arrive(plane + far, side)
                start(beside_again(plane + far))

    def tokens_finish():
        @pl.loop(0, last + 1)
        def _(q):
            tokens_arrive(q, pair)
            tokens_arrive(q, diagonal)

    def band(chunk, owner):
        _, first, length = plan[chunk]
        return pl.ds(pl.multiple_of(owner * quarter + first, 16), length)

    def spread(chunk):
        array = plan[chunk][0]
        spot = gathered[chunk].at[own_at + seat]
        pltpu.make_async_copy(held[array].at[0, band(chunk, seat)], spot, one_recv.at[chunk]).start()
        for k in (2, 1, 3):
            peer = lax.rem(seat + k, size)
            send(
                held[array].at[0, band(chunk, peer)], spot, one_send.at[chunk],
                one_recv.at[chunk], at_plane(plane, peer),
            ).start()

    def own_part(chunk):
        return gathered[chunk].at[pl.ds(own_at, size)]

    def other_part(chunk):
        return gathered[chunk].at[pl.ds(other_at, size)]

    def inward(chunk):
        return send(
            own_part(chunk), own_part(chunk), two_send.at[chunk], two_recv.at[chunk],
            at_plane(1 + half, seat),
        )

    def over(chunk):
        return send(
            leaving_of(chunk), crossed[chunk], cross_send.at[chunk], cross_recv.at[chunk],
            at_plane(last - plane, seat),
        )

    def outward(chunk):
        return send(
            ordered_of(chunk).at[pl.ds(other_at, size)], own_part(chunk), back_send.at[chunk],
            back_recv.at[chunk], at_plane(last * half, seat),
        )

    def flat_at(chunk):
        return sum(length for _, _, length in plan[:chunk]), plan[chunk][2]

    def leaving_of(chunk):
        first, length = flat_at(chunk)
        return leaving.at[:, pl.ds(first, length)]

    def ordered_of(chunk):
        first, length = flat_at(chunk)
        return ordered.at[:, pl.ds(first, length)]

    def deliver(chunk, piece_of):
        array = plan[chunk][0]
        target = moved[array].at[0, band(chunk, seat)]
        for k in (2, 1, 3):
            peer = lax.rem(seat + k, size)
            send(
                piece_of(peer), target, three_send.at[chunk], three_recv.at[array],
                at_plane(plane, peer),
            ).start()
        pltpu.make_async_copy(piece_of(seat), target, three_recv.at[array]).start()

    def outer_in(chunk):
        @pl.when(outer)
        def _():
            landed(own_part(chunk), one_recv.at[chunk])
            inward(chunk).start()

    def inner_in(chunk):
        @pl.when(inner)
        def _():
            landed(own_part(chunk), one_recv.at[chunk])
            landed(other_part(chunk), two_recv.at[chunk])
            first, length = flat_at(chunk)

            @pl.loop(0, most)
            def _(m):
                leaving[m, pl.ds(first, length)] = gathered[chunk][table[base + m]]

            over(chunk).start()

    def inner_out(chunk):
        @pl.when(inner)
        def _():
            landed(crossed[chunk], cross_recv.at[chunk])
            first, length = flat_at(chunk)

            @pl.loop(0, 2 * size)
            def _(place):
                at = base + place
                own = gathered[chunk][table[2 * n + at]]
                other = crossed[chunk][table[3 * n + at]]
                ordered[place, pl.ds(first, length)] = jnp.where(table[n + at] == 1, other, own)

            outward(chunk).start()
            deliver(chunk, lambda s: ordered_of(chunk).at[own_at + s])

    def outer_out(chunk):
        @pl.when(outer)
        def _():
            landed(other_part(chunk), back_recv.at[chunk])
            deliver(chunk, lambda s: gathered[chunk].at[other_at + s])

    block = size * rows
    columns = 512

    def wait_loads():
        for load in loads:
            load.wait()

    def compute(q):
        at = pl.ds(pl.multiple_of(q * block, block), block)
        gate_value = jnp.dot(tok_all[at, :], w_g[...], preferred_element_type=jnp.float32)
        up_value = jnp.dot(tok_all[at, :], w_u[...], preferred_element_type=jnp.float32)
        hidden[...] = (gate_value / (1.0 + jnp.exp(-gate_value)) * up_value).astype(jnp.bfloat16)
        lanes = lax.broadcasted_iota(jnp.int32, (block, LANES), 1)
        scale = jnp.sum(jnp.where(lanes == me, coef_all[at, :], 0.0), axis=1, keepdims=True)

        @pl.loop(0, width // columns)
        def _(part):
            cols = pl.ds(pl.multiple_of(part * columns, columns), columns)
            value = lax.dot_general(
                hidden[...], w_d[cols, :], (((1,), (1,)), ((), ())),
                preferred_element_type=jnp.float32,
            )
            value = value.astype(jnp.bfloat16).astype(jnp.float32)
            contrib[at, cols] = (value * scale).astype(jnp.bfloat16)

        start((pair_copy(q, 0), pair_copy(q, 1)))

    def seat_of(row, core_seat):
        return row * 2 + lax.rem(core_seat, 2)

    def pair_copy(q, row):
        owner = at_plane(q, seat_of(row, pair))
        return send(
            contrib.at[token_rows(owner)], pair_in.at[q, row], pair_send.at[q, row],
            pair_recv.at[q, row], at_plane(plane, pair),
        )

    def side_copy(q):
        return send(
            side_out.at[q], side_in.at[q], side_send.at[q], side_recv.at[q],
            at_plane(plane, side),
        )

    def add_rows(parts, target):
        @pl.loop(0, width // columns)
        def _(part):
            cols = pl.ds(pl.multiple_of(part * columns, columns), columns)
            total = sum(source(cols).astype(jnp.float32) for source in parts)
            target(cols, total.astype(jnp.bfloat16))

    my_row = seat // 2

    def pair_add(q):
        landed(pair_in.at[q, 0], pair_recv.at[q, 0])
        landed(pair_in.at[q, 1], pair_recv.at[q, 1])

        def put(cols, value):
            side_out[q, :, cols] = value

        add_rows(
            (
                lambda cols: contrib[token_rows(at_plane(q, side)), cols],
                lambda cols: pair_in[q, 1 - my_row, :, cols],
            ),
            put,
        )
        side_copy(q).start()

    def side_add(q):
        landed(side_in.at[q], side_recv.at[q])

        def put(cols, value):
            plane_sum[q, :, cols] = value

        add_rows(
            (
                lambda cols: contrib[token_rows(at_plane(q, seat)), cols],
                lambda cols: pair_in[q, my_row, :, cols],
                lambda cols: side_in[q, :, cols],
            ),
            put,
        )

    def chain_copy(way, q, source):
        return send(
            source.at[q], chain_in.at[way, q], chain_send.at[way, q], chain_recv.at[way, q],
            me + size if way == 0 else me - size,
        )

    def chain_step(way, q):
        ends = plane == (0 if way == 0 else last)
        passes = (q > plane) if way == 0 else (q < plane)

        @pl.when(passes & ends)
        def _():
            chain_copy(way, q, plane_sum).start()

        @pl.when(passes & jnp.logical_not(ends))
        def _():
            landed(chain_in.at[way, q], chain_recv.at[way, q])

            def put(cols, value):
                chain_out[way, q, :, cols] = value

            add_rows(
                (lambda cols: plane_sum[q, :, cols], lambda cols: chain_in[way, q, :, cols]), put
            )
            chain_copy(way, q, chain_out.at[way]).start()

    def finish_rows():
        def put(cols, value):
            out[:, cols] = value

        @pl.when(plane > 0)
        def _():
            landed(chain_in.at[0, plane], chain_recv.at[0, plane])

        @pl.when(plane < last)
        def _():
            landed(chain_in.at[1, plane], chain_recv.at[1, plane])

        mine = lambda cols: plane_sum[plane, :, cols]
        below = lambda cols: chain_in[0, plane, :, cols]
        above = lambda cols: chain_in[1, plane, :, cols]

        @pl.when(plane == 0)
        def _():
            add_rows((mine, above), put)

        @pl.when(plane == last)
        def _():
            add_rows((mine, below), put)

        @pl.when(inner)
        def _():
            add_rows((mine, below, above), put)

    def compute_all():
        @pl.loop(0, last + 1)
        def _(q):
            compute(q)

    def pair_all():
        @pl.loop(0, last + 1)
        def _(q):
            pair_add(q)

    def side_all():
        @pl.loop(0, last + 1)
        def _(q):
            side_add(q)

    def chain_all():
        for q in range(last, 0, -1):
            chain_step(0, q)
        for q in range(last):
            chain_step(1, q)

    steps = {
        "own_along": own_tokens_along, "own_across": own_tokens_across, "tok": tokens_step,
        "relay": tokens_relay, "tok_end": tokens_finish, "spread": spread, "oi": outer_in,
        "ii": inner_in, "io": inner_out, "oo": outer_out, "loads": wait_loads,
        "compute": compute_all, "pair": pair_all, "side": side_all, "chain": chain_all,
        "rows": finish_rows,
    }
    for name, *arguments in line_order(count):
        steps[name](*arguments)

    for q in range(last + 1):

        def gone(copies):
            for copy in copies:
                copy.wait_send()

        @pl.when((q <= plane) & (plane < last))
        def _():
            gone(up(q))

        @pl.when((q >= plane) & (plane > 0))
        def _():
            gone(down(q))

        gone(across(q) + beside(q) + beside_again(q))
        gone((pair_copy(q, 0), pair_copy(q, 1), side_copy(q)))

        @pl.when((q > plane) & (plane < last))
        def _():
            chain_copy(0, q, plane_sum).wait_send()

        @pl.when((q < plane) & (plane > 0))
        def _():
            chain_copy(1, q, plane_sum).wait_send()

    for chunk in range(count):
        sent = gathered[chunk].at[pl.ds(0, size - 1)]
        landed(sent, one_send.at[chunk])
        landed(sent, three_send.at[chunk])

        @pl.when(outer)
        def _():
            inward(chunk).wait_send()

        @pl.when(inner)
        def _():
            over(chunk).wait_send()
            outward(chunk).wait_send()

    for array in range(3):
        landed(moved[array].at[0], three_recv.at[array])


def line_order(count):
    order = [("own_along",), ("spread", 0), ("own_across",), ("spread", 1), ("spread", 2)]
    spread_next = 3
    waiting = {
        0: [("tok", 1)],
        1: [("tok", 2), ("relay", 0)],
        2: [("tok", 3), ("relay", 1)],
        3: [("relay", 2), ("relay", 3), ("tok_end",)],
        4: [("loads",), ("compute",)],
        5: [("pair",)],
        6: [("side",)],
        7: [("chain",)],
    }
    late = []
    for turn in range(count + 4):
        if turn < count:
            order.append(("oi", turn))
        if spread_next < count:
            order.append(("spread", spread_next))
            spread_next += 1
        if turn in waiting:
            order.extend(waiting[turn])
        if 0 <= turn - 1 < count:
            order.append(("ii", turn - 1))
        if 0 <= turn - 2 < count:
            order.append(("io", turn - 2))
        if 0 <= turn - 3 < count:
            order.append(("oo", turn - 3))
    order.append(("rows",))
    return order


def call_line(n, most, which, table, tokens, coef, held_gate, held_up, held_down):
    rows, width = tokens.shape
    size = 4
    planes = n // size
    quarter = width // size
    plan = chunk_plan(quarter, ((4, 4, 4, 4),) * 3)
    count = len(plan)
    vmem = pl.BlockSpec(memory_space=pltpu.VMEM)
    anywhere = pl.BlockSpec(memory_space=pl.ANY)
    dma = pltpu.SemaphoreType.DMA
    moved_shape = jax.ShapeDtypeStruct(held_gate.shape, held_gate.dtype)

    def block(*shape):
        return pltpu.VMEM(shape, jnp.bfloat16)

    return pl.pallas_call(
        functools.partial(line_kernel, n, most, plan),
        out_shape=(jax.ShapeDtypeStruct((rows, width), jnp.bfloat16),) + (moved_shape,) * 3,
        in_specs=[pl.BlockSpec(memory_space=pltpu.SMEM), vmem, vmem] + [anywhere] * 3,
        out_specs=(vmem, anywhere, anywhere, anywhere),
        scratch_shapes=[
            *(block(2 * size, length, LANES) for _, _, length in plan),
            *(block(most, length, LANES) for _, _, length in plan),
            block(most, 3 * quarter, LANES),
            block(2 * size, 3 * quarter, LANES),
            block(n * rows, width),
            pltpu.VMEM((n * rows, LANES), jnp.float32),
            block(width, LANES),
            block(width, LANES),
            block(width, LANES),
            block(size * rows, LANES),
            block(n * rows, width),
            block(planes, 2, rows, width),
            block(planes, rows, width),
            block(planes, rows, width),
            block(planes, rows, width),
            block(2, planes, rows, width),
            block(2, planes, rows, width),
            dma((3,)),
            dma((2, planes, 5)),
            dma((2, n)),
            dma((count,)),
            dma((count,)),
            dma((count,)),
            dma((count,)),
            dma((count,)),
            dma((count,)),
            dma((count,)),
            dma((count,)),
            dma((count,)),
            dma((3,)),
            dma((planes, 2)),
            dma((planes, 2)),
            dma((planes,)),
            dma((planes,)),
            dma((2, planes)),
            dma((2, planes)),
        ],
        compiler_params=pltpu.CompilerParams(
            collective_id=which, has_side_effects=True, vmem_limit_bytes=VMEM_BYTES
        ),
    )(table, tokens, coef, held_gate, held_up, held_down)


def per_device(
    tokens, route_ids, route_logits, old_place, new_place, held_gate, held_up, held_down
):
    n = lax.axis_size("expert")
    half = n // 2
    device_ids = jnp.arange(n, dtype=jnp.int32)
    blocks = n // EXPERTS
    at_old = (old_place[:, None] == device_ids[None, :]).astype(jnp.int32)
    dest_of = jnp.sum(at_old * new_place[:, None], axis=0)
    expert_at = jnp.sum(at_old * device_ids[:, None], axis=0) // blocks
    half_of = device_ids // half
    crosses = (dest_of // half != half_of).astype(jnp.int32)
    earlier = (half_of[:, None] == half_of[None, :]) & (device_ids[:, None] < device_ids[None, :])
    turn = jnp.sum(earlier.astype(jnp.int32) * crosses[:, None], axis=0)
    lane_of = device_ids - half_of * half
    leaving = (half_of[:, None] * half + turn[:, None] == device_ids[None, :]).astype(jnp.int32)
    leaving = jnp.sum(leaving * (crosses * lane_of)[:, None], axis=0)
    arriving = (dest_of[:, None] == device_ids[None, :]).astype(jnp.int32)
    table = jnp.concatenate([
        leaving,
        jnp.sum(arriving * crosses[:, None], axis=0),
        jnp.sum(arriving * ((1 - crosses) * lane_of)[:, None], axis=0),
        jnp.sum(arriving * (crosses * turn)[:, None], axis=0),
    ])
    first_weight = 1.0 / (1.0 + jnp.exp(route_logits[:, 1] - route_logits[:, 0]))
    second_weight = 1.0 / (1.0 + jnp.exp(route_logits[:, 0] - route_logits[:, 1]))
    coef = jnp.where(route_ids[:, 0:1] == expert_at[None, :], first_weight[:, None], 0.0)
    coef = coef + jnp.where(route_ids[:, 1:2] == expert_at[None, :], second_weight[:, None], 0.0)
    coef = jnp.pad(coef, ((0, 0), (0, LANES - n)))
    table, coef = lax.optimization_barrier((table, coef))
    in_line = near_square_root(n) == 4 and n == 16
    shares = (4, 5, 6, 8) if in_line else (3, 4, 5, 6, 8)
    levels = sorted({max(1, half * eighths // 8) for eighths in shares})
    call = call_line if in_line else call_layer
    crossing = jnp.sum(crosses) // 2
    level = sum((crossing > most).astype(jnp.int32) for most in levels[:-1])
    branches = [functools.partial(call, n, most, i) for i, most in enumerate(levels)]
    return lax.switch(level, branches, table, tokens, coef, held_gate, held_up, held_down)


def solution(mesh):
    split = ("groups", "expert")
    placed = (
        P(split, None),
        P(split, None),
        P(split, None),
        P(),
        P(),
        P(split, None, None),
        P(split, None, None),
        P(split, None, None),
    )
    return jax.shard_map(
        per_device,
        mesh=mesh,
        in_specs=placed,
        out_specs=(
            P(split, None),
            P(split, None, None),
            P(split, None, None),
            P(split, None, None),
        ),
        check_vma=False,
    )
```

```python
import functools

import jax
import jax.numpy as jnp
from jax import lax
from jax.experimental import pallas as pl
from jax.experimental.pallas import tpu as pltpu
from jax.sharding import PartitionSpec as P

EXPERTS = 8
LANES = 128
MESH = pl.DeviceIdType.MESH
VMEM_BYTES = 63_000_000


def near_square_root(n):
    size = 1
    while size * size < n:
        size *= 2
    return size


def layer_kernel(
    n,
    most,
    table,
    tok,
    coef,
    held_g,
    held_u,
    held_d,
    out,
    moved_g,
    moved_u,
    moved_d,
    tok_all,
    coef_all,
    w_gu,
    w_d,
    pieces_g,
    pieces_u,
    pieces_d,
    crossed_g,
    crossed_u,
    crossed_d,
    ordered,
    hidden,
    contrib,
    part_in,
    plane_sum,
    half_in,
    cross_out,
    cross_in,
    load_sem,
    tok_send,
    fwd_send,
    plane_send,
    tok_recv,
    one_send,
    one_recv,
    two_send,
    two_recv,
    three_send,
    three_recv,
    part_send,
    part_recv,
    half_send,
    half_recv,
    cross_send,
    cross_recv,
):
    me = lax.axis_index("expert")
    half = n // 2
    base = (me // half) * half
    lane = me - base
    twin = lax.rem(me + half, n)
    rows, width = tok.shape
    band = width // half
    size = near_square_root(n)
    planes = n // size
    half_planes = planes // 2
    plane = me // size
    seat = me - plane * size
    my_plane_of_half = lane // size
    held = (held_g, held_u, held_d)
    moved = (moved_g, moved_u, moved_d)
    pieces = (pieces_g, pieces_u, pieces_d)
    crossed = (crossed_g, crossed_u, crossed_d)

    barrier = pltpu.get_barrier_semaphore()

    @pl.loop(1, n)
    def _(k):
        pl.semaphore_signal(
            barrier, inc=1, device_id={"expert": lax.rem(me + k, n)}, device_id_type=MESH
        )

    loads = (
        pltpu.make_async_copy(held_g.at[0], w_gu.at[:, pl.ds(0, LANES)], load_sem.at[0]),
        pltpu.make_async_copy(held_u.at[0], w_gu.at[:, pl.ds(LANES, LANES)], load_sem.at[1]),
        pltpu.make_async_copy(held_d.at[0], w_d, load_sem.at[2]),
    )
    for load in loads:
        load.start()

    def token_rows(owner):
        return pl.ds(pl.multiple_of(owner * rows, rows), rows)

    def band_rows(owner):
        return pl.ds(pl.multiple_of(owner * band, band), band)

    def near(k):
        return base + lax.rem(lane + k, half)

    def column(k):
        return base + lax.rem(lane + k * size, half)

    def mate(k):
        return plane * size + lax.rem(seat + k, size)

    def seated(other_plane):
        return other_plane * size + seat

    tok_all[token_rows(me), :] = tok[...]
    coef_all[token_rows(me), :] = coef[...]
    pl.semaphore_wait(barrier, n - 1)

    def send(source, target, send_sem, recv_sem, peer):
        return pltpu.make_async_remote_copy(
            src_ref=source, dst_ref=target, send_sem=send_sem, recv_sem=recv_sem,
            device_id={"expert": peer}, device_id_type=MESH,
        )

    def own_tokens(peer):
        at = token_rows(me)
        return (
            send(tok, tok_all.at[at], tok_send.at[0, peer], tok_recv.at[0, me], peer),
            send(coef, coef_all.at[at], tok_send.at[1, peer], tok_recv.at[1, me], peer),
        )

    def passed_tokens(owner, peer, sems):
        at = token_rows(owner)
        return (
            send(tok_all.at[at], tok_all.at[at], sems[0], tok_recv.at[0, owner], peer),
            send(coef_all.at[at], coef_all.at[at], sems[1], tok_recv.at[1, owner], peer),
        )

    def twin_tokens(peer):
        return passed_tokens(twin, peer, (fwd_send.at[0, peer], fwd_send.at[1, peer]))

    def plane_tokens(other_plane, k):
        sems = (plane_send.at[0, other_plane, k], plane_send.at[1, other_plane, k])
        return passed_tokens(seated(other_plane), mate(k), sems)

    def tokens_arrive(owner):
        pltpu.make_async_copy(tok, tok_all.at[token_rows(owner)], tok_recv.at[0, owner]).wait()
        pltpu.make_async_copy(coef, coef_all.at[token_rows(owner)], tok_recv.at[1, owner]).wait()

    def spread(array):
        pltpu.make_async_copy(
            held[array].at[0, band_rows(lane)], pieces[array].at[lane], one_recv.at[array]
        ).start()

        @pl.loop(1, half)
        def _(k):
            peer = near(k)
            send(
                held[array].at[0, band_rows(peer - base)], pieces[array].at[lane],
                one_send.at[array], one_recv.at[array], peer,
            ).start()

    def swap(array):
        return send(
            ordered.at[array, pl.ds(0, most)], crossed[array],
            two_send.at[array], two_recv.at[array], twin,
        )

    def cross_over(array):
        pltpu.make_async_copy(pieces[array], pieces[array], one_recv.at[array]).wait()

        @pl.loop(0, most)
        def _(m):
            ordered[array, m] = pieces[array][table[base + m]]

        swap(array).start()

    def deliver(array):
        swap(array).wait()

        @pl.loop(0, half)
        def _(place):
            at = base + place
            own = pieces[array][table[2 * n + at]]
            other = crossed[array][table[3 * n + at]]
            ordered[array, place] = jnp.where(table[n + at] == 1, other, own)

        pltpu.make_async_copy(
            ordered.at[array, lane], moved[array].at[0, band_rows(lane)], three_recv.at[array]
        ).start()

        @pl.loop(1, half)
        def _(k):
            peer = near(k)
            send(
                ordered.at[array, peer - base], moved[array].at[0, band_rows(lane)],
                three_send.at[array], three_recv.at[array], peer,
            ).start()

    for copy in own_tokens(twin):
        copy.start()

    @pl.loop(1, half_planes)
    def _(k):
        for copy in own_tokens(column(k)):
            copy.start()

    @pl.loop(1, size)
    def _(k):
        for copy in own_tokens(mate(k)):
            copy.start()

    spread(0)
    tokens_arrive(twin)

    @pl.loop(1, half_planes)
    def _(k):
        for copy in twin_tokens(column(k)):
            copy.start()

    spread(1)

    @pl.loop(1, half_planes)
    def _(k):
        tokens_arrive(column(k))
        tokens_arrive(lax.rem(column(k) + half, n))

    @pl.loop(1, planes)
    def _(shift):
        @pl.loop(1, size)
        def _(k):
            for copy in plane_tokens(lax.rem(plane + shift, planes), k):
                copy.start()

    spread(2)
    cross_over(0)
    cross_over(1)

    @pl.loop(0, planes)
    def _(other_plane):
        @pl.loop(1, size)
        def _(k):
            tokens_arrive(other_plane * size + lax.rem(seat + k, size))

    for load in loads:
        load.wait()

    step = min(256, n * rows)
    columns = 512

    @pl.loop(0, n * rows // step)
    def _(block):
        at = pl.ds(pl.multiple_of(block * step, step), step)
        both = jnp.dot(tok_all[at, :], w_gu[...], preferred_element_type=jnp.float32)
        gate_value = both[:, :LANES]
        up_value = both[:, LANES:]
        hidden[...] = (gate_value / (1.0 + jnp.exp(-gate_value)) * up_value).astype(jnp.bfloat16)
        lanes = lax.broadcasted_iota(jnp.int32, (step, LANES), 1)
        scale = jnp.sum(jnp.where(lanes == me, coef_all[at, :], 0.0), axis=1, keepdims=True)

        @pl.loop(0, width // columns)
        def _(part):
            cols = pl.ds(pl.multiple_of(part * columns, columns), columns)
            value = lax.dot_general(
                hidden[...], w_d[cols, :], (((1,), (1,)), ((), ())),
                preferred_element_type=jnp.float32,
            )
            value = value.astype(jnp.bfloat16).astype(jnp.float32)
            contrib[at, cols] = (value * scale).astype(jnp.bfloat16)

    def part_copy(k, other_plane):
        peer = mate(k)
        owner = other_plane * size + lax.rem(seat + k, size)
        return send(
            contrib.at[token_rows(owner)], part_in.at[seat, other_plane],
            part_send.at[k, other_plane], part_recv.at[seat, other_plane], peer,
        )

    def half_copy(k, kind):
        peer = column(k)
        target = peer // size if kind == 0 else lax.rem(peer // size + half_planes, planes)
        return send(
            plane_sum.at[target], half_in.at[kind, my_plane_of_half],
            half_send.at[kind, k], half_recv.at[kind, my_plane_of_half], peer,
        )

    @pl.loop(0, planes)
    def _(other_plane):
        @pl.loop(1, size)
        def _(k):
            part_copy(k, other_plane).start()

    def add_plane():
        @pl.loop(0, planes)
        def _(other_plane):
            @pl.loop(1, size)
            def _(k):
                spot = part_in.at[lax.rem(seat + k, size), other_plane]
                pltpu.make_async_copy(
                    spot, spot, part_recv.at[lax.rem(seat + k, size), other_plane]
                ).wait()

            @pl.loop(0, width // columns)
            def _(part):
                cols = pl.ds(pl.multiple_of(part * columns, columns), columns)

                def more(k, total):
                    other = lax.rem(seat + k, size)
                    return total + part_in[other, other_plane, :, cols].astype(jnp.float32)

                total = contrib[token_rows(seated(other_plane)), cols].astype(jnp.float32)
                total = lax.fori_loop(1, size, more, total)
                plane_sum[other_plane, :, cols] = total.astype(jnp.bfloat16)

        for kind in (1, 0):

            @pl.loop(1, half_planes)
            def _(k):
                half_copy(k, kind).start()

    def add_half(kind, own_plane, extra, target):
        @pl.loop(1, half_planes)
        def _(k):
            other = lax.rem(my_plane_of_half + k, half_planes)
            spot = half_in.at[kind, other]
            pltpu.make_async_copy(spot, spot, half_recv.at[kind, other]).wait()

        @pl.loop(0, width // columns)
        def _(part):
            cols = pl.ds(pl.multiple_of(part * columns, columns), columns)

            def more(k, total):
                other = lax.rem(my_plane_of_half + k, half_planes)
                return total + half_in[kind, other, :, cols].astype(jnp.float32)

            total = plane_sum[own_plane, :, cols].astype(jnp.float32)
            if extra is not None:
                total = total + extra[:, cols].astype(jnp.float32)
            target[:, cols] = lax.fori_loop(1, half_planes, more, total).astype(jnp.bfloat16)

    deliver(0)
    cross_over(2)
    add_plane()
    deliver(1)
    add_half(1, lax.rem(plane + half_planes, planes), None, cross_out)
    cross = send(cross_out, cross_in, cross_send, cross_recv, twin)
    cross.start()
    deliver(2)
    cross.wait()
    add_half(0, plane, cross_in, out)

    for copy in own_tokens(twin):
        copy.wait_send()

    @pl.loop(1, half_planes)
    def _(k):
        for copy in own_tokens(column(k)):
            copy.wait_send()
        for copy in twin_tokens(column(k)):
            copy.wait_send()
        half_copy(k, 0).wait_send()
        half_copy(k, 1).wait_send()

    @pl.loop(1, size)
    def _(k):
        for copy in own_tokens(mate(k)):
            copy.wait_send()

        @pl.loop(0, planes)
        def _(other_plane):
            part_copy(k, other_plane).wait_send()

        @pl.loop(1, planes)
        def _(shift):
            for copy in plane_tokens(lax.rem(plane + shift, planes), k):
                copy.wait_send()

    for array in range(3):
        sent = pieces[array].at[pl.ds(0, half - 1)]
        pltpu.make_async_copy(sent, sent, one_send.at[array]).wait()
        pltpu.make_async_copy(sent, sent, three_send.at[array]).wait()
        pltpu.make_async_copy(
            moved[array].at[0], moved[array].at[0], three_recv.at[array]
        ).wait()


def call_layer(n, most, which, table, tokens, coef, held_gate, held_up, held_down):
    rows, width = tokens.shape
    half = n // 2
    band = width // half
    size = near_square_root(n)
    planes = n // size
    vmem = pl.BlockSpec(memory_space=pltpu.VMEM)
    anywhere = pl.BlockSpec(memory_space=pl.ANY)
    dma = pltpu.SemaphoreType.DMA
    moved_shape = jax.ShapeDtypeStruct(held_gate.shape, held_gate.dtype)

    def block(*shape):
        return pltpu.VMEM(shape, jnp.bfloat16)

    return pl.pallas_call(
        functools.partial(layer_kernel, n, most),
        out_shape=(jax.ShapeDtypeStruct((rows, width), jnp.bfloat16),) + (moved_shape,) * 3,
        in_specs=[pl.BlockSpec(memory_space=pltpu.SMEM), vmem, vmem] + [anywhere] * 3,
        out_specs=(vmem, anywhere, anywhere, anywhere),
        scratch_shapes=[
            block(n * rows, width),
            pltpu.VMEM((n * rows, LANES), jnp.float32),
            block(width, 2 * LANES),
            block(width, LANES),
            block(half, band, LANES),
            block(half, band, LANES),
            block(half, band, LANES),
            block(most, band, LANES),
            block(most, band, LANES),
            block(most, band, LANES),
            block(3, half, band, LANES),
            block(min(256, n * rows), LANES),
            block(n * rows, width),
            block(size, planes, rows, width),
            block(planes, rows, width),
            block(2, planes // 2, rows, width),
            block(rows, width),
            block(rows, width),
            dma((3,)),
            dma((2, n)),
            dma((2, n)),
            dma((2, planes, size)),
            dma((2, n)),
            dma((3,)),
            dma((3,)),
            dma((3,)),
            dma((3,)),
            dma((3,)),
            dma((3,)),
            dma((size, planes)),
            dma((size, planes)),
            dma((2, planes // 2)),
            dma((2, planes // 2)),
            dma,
            dma,
        ],
        compiler_params=pltpu.CompilerParams(
            collective_id=which, has_side_effects=True, vmem_limit_bytes=VMEM_BYTES
        ),
    )(table, tokens, coef, held_gate, held_up, held_down)


O, I, J, K = range(4)
(
    OWN, SEAT_TOKENS, SIDE_TOKENS, SPREAD, OUTER_IN, INNER_IN, INNER_OUT, OUTER_OUT,
    COMPUTE, PAIR_ADD, SIDE_ADD, FINISH,
) = range(12)


def chunk_plan(quarter, cuts):
    plan = []
    for array in range(3):
        start = 0
        for cut in cuts[array]:
            size = quarter * cut // 16
            plan.append((array, start, size))
            start += size
        assert start == quarter
    return tuple(plan)


def line_kernel(
    n, most, plan, order, table, tok, coef, held_g, held_u, held_d, out, moved_g, moved_u, moved_d, *rest
):
    count = len(plan)
    gathered, rest = rest[:count], rest[count:]
    crossed, rest = rest[:count], rest[count:]
    (
        leaving, ordered, tok_all, coef_all, w_gu, w_d, hidden, contrib,
        pair_in, side_out, side_in, chain_in, chain_out, over_in, both_in, both_out,
        load_sem, tok_send, tok_recv,
        one_send, one_recv, two_send, two_recv, cross_send, cross_recv,
        back_send, back_recv, three_send, three_recv,
        pair_send, pair_recv, side_send, side_recv, chain_send, chain_recv,
        over_recv, both_send, both_recv,
    ) = rest
    size = 4
    last = n // size - 1
    me = lax.axis_index("expert")
    plane = me // size
    seat = me - plane * size
    half = plane // 2
    base = half * (n // 2)
    own_at = lax.rem(plane, 2) * size
    other_at = size - own_at
    inner = (plane == 1) | (plane == 2)
    outer = (plane == 0) | (plane == last)
    side = lax.rem(seat + 2, size)
    pair = seat + 1 - 2 * lax.rem(seat, 2)
    diagonal = lax.rem(pair + 2, size)
    my_row = seat // 2
    rows, width = tok.shape
    quarter = width // size
    held = (held_g, held_u, held_d)
    moved = (moved_g, moved_u, moved_d)
    plane_of = (last * half, 1 + half, last - 1 - half, last - last * half)

    def at_plane(other, other_seat):
        return other * size + other_seat

    near_outer, near_inner = at_plane(plane_of[O], seat), at_plane(plane_of[I], seat)
    far_inner = at_plane(plane_of[J], seat)
    beside, across = at_plane(plane, pair), at_plane(plane, side)

    barrier = pltpu.get_barrier_semaphore()

    def greet(peer):
        pl.semaphore_signal(barrier, inc=1, device_id={"expert": peer}, device_id_type=MESH)

    @pl.loop(1, size)
    def _(k):
        greet(at_plane(plane, lax.rem(seat + k, size)))

    @pl.when(outer)
    def _():
        greet(near_inner)

    @pl.when(inner)
    def _():
        greet(near_outer)
        greet(far_inner)

    loads = (
        pltpu.make_async_copy(held_g.at[0], w_gu.at[:, pl.ds(0, LANES)], load_sem.at[0]),
        pltpu.make_async_copy(held_u.at[0], w_gu.at[:, pl.ds(LANES, LANES)], load_sem.at[1]),
        pltpu.make_async_copy(held_d.at[0], w_d, load_sem.at[2]),
    )

    def token_rows(owner):
        return pl.ds(pl.multiple_of(owner * rows, rows), rows)

    tok_all[token_rows(me), :] = tok[...]
    coef_all[token_rows(me), :] = coef[...]

    @pl.when(inner)
    def _():
        pl.semaphore_wait(barrier, size + 1)

    @pl.when(outer)
    def _():
        pl.semaphore_wait(barrier, size)

    def send(source, target, send_sem, recv_sem, peer):
        return pltpu.make_async_remote_copy(
            src_ref=source, dst_ref=target, send_sem=send_sem, recv_sem=recv_sem,
            device_id={"expert": peer}, device_id_type=MESH,
        )

    def landed(spot, sem):
        pltpu.make_async_copy(spot, spot, sem).wait()

    sent = {True: [], False: []}

    def go(role, *copies):
        for copy in copies:
            copy.start()
        sent[role].extend(copies)

    def tokens_to(q, owner_seat, peer, path, own=False):
        owner_plane = plane_of[q]
        owner = at_plane(owner_plane, owner_seat)
        at = token_rows(owner)
        token_source, coef_source = (tok, coef) if own else (tok_all.at[at], coef_all.at[at])
        return (
            send(token_source, tok_all.at[at], tok_send.at[0, owner_plane, path], tok_recv.at[0, owner], peer),
            send(coef_source, coef_all.at[at], tok_send.at[1, owner_plane, path], tok_recv.at[1, owner], peer),
        )

    def tokens_arrive(q, owner_seat):
        owner = at_plane(plane_of[q], owner_seat)
        landed(tok_all.at[token_rows(owner)], tok_recv.at[0, owner])
        landed(coef_all.at[token_rows(owner)], tok_recv.at[1, owner])

    def own_tokens(is_outer):
        if is_outer:
            go(True, *tokens_to(O, seat, near_inner, 0, True))
        else:
            go(False, *tokens_to(I, seat, near_outer, 0, True))
            go(False, *tokens_to(I, seat, far_inner, 1, True))
        mine = O if is_outer else I
        go(is_outer, *tokens_to(mine, seat, across, 2, True))
        go(is_outer, *tokens_to(mine, seat, beside, 3, True))

    def seat_tokens(is_outer, q):
        tokens_arrive(q, seat)
        if not is_outer:
            if q == O:
                go(False, *tokens_to(q, seat, far_inner, 1))
            else:
                go(False, *tokens_to(q, seat, near_outer, 0))
        if (is_outer, q) not in ((True, I), (False, O)):
            go(is_outer, *tokens_to(q, seat, across, 2))
        go(is_outer, *tokens_to(q, seat, beside, 3))

    def side_tokens(is_outer, q):
        tokens_arrive(q, side)
        if (is_outer, q) == (True, O):
            go(True, *tokens_to(q, side, near_inner, 5))
        if (is_outer, q) == (False, I):
            go(False, *tokens_to(q, side, near_outer, 5))
        go(is_outer, *tokens_to(q, side, beside, 4))

    def band(chunk, owner):
        _, first, length = plan[chunk]
        return pl.ds(pl.multiple_of(owner * quarter + first, 16), length)

    def spread(is_outer, chunk):
        array = plan[chunk][0]
        spot = gathered[chunk].at[own_at + seat]
        pltpu.make_async_copy(held[array].at[0, band(chunk, seat)], spot, one_recv.at[chunk]).start()
        for k in (2, 1, 3):
            peer = lax.rem(seat + k, size)
            send(
                held[array].at[0, band(chunk, peer)], spot, one_send.at[chunk],
                one_recv.at[chunk], at_plane(plane, peer),
            ).start()

    def own_part(chunk):
        return gathered[chunk].at[pl.ds(own_at, size)]

    def other_part(chunk):
        return gathered[chunk].at[pl.ds(other_at, size)]

    def flat_at(chunk):
        return pl.ds(sum(length for _, _, length in plan[:chunk]), plan[chunk][2])

    def deliver(chunk, piece_of):
        array = plan[chunk][0]
        target = moved[array].at[0, band(chunk, seat)]
        for k in (2, 1, 3):
            peer = lax.rem(seat + k, size)
            send(
                piece_of(peer), target, three_send.at[chunk], three_recv.at[array],
                at_plane(plane, peer),
            ).start()
        pltpu.make_async_copy(piece_of(seat), target, three_recv.at[array]).start()

    def outer_in(is_outer, chunk):
        landed(own_part(chunk), one_recv.at[chunk])
        go(True, send(
            own_part(chunk), own_part(chunk), two_send.at[chunk], two_recv.at[chunk], near_inner
        ))

    def inner_in(is_outer, chunk):
        landed(own_part(chunk), one_recv.at[chunk])
        landed(other_part(chunk), two_recv.at[chunk])
        flat = flat_at(chunk)

        @pl.loop(0, most)
        def _(m):
            leaving[m, flat] = gathered[chunk][table[base + m]]

        go(False, send(
            leaving.at[:, flat], crossed[chunk], cross_send.at[chunk], cross_recv.at[chunk], far_inner
        ))

    def inner_out(is_outer, chunk):
        landed(crossed[chunk], cross_recv.at[chunk])
        flat = flat_at(chunk)

        @pl.loop(0, 2 * size)
        def _(place):
            at = base + place
            own = gathered[chunk][table[2 * n + at]]
            other = crossed[chunk][table[3 * n + at]]
            ordered[place, flat] = jnp.where(table[n + at] == 1, other, own)

        go(False, send(
            ordered.at[pl.ds(other_at, size), flat], own_part(chunk), back_send.at[chunk],
            back_recv.at[chunk], near_outer,
        ))
        deliver(chunk, lambda s: ordered.at[own_at + s, flat])

    def outer_out(is_outer, chunk):
        landed(other_part(chunk), back_recv.at[chunk])
        deliver(chunk, lambda s: gathered[chunk].at[other_at + s])

    block = size * rows
    columns = 512

    def compute(is_outer, q):
        tokens_arrive(q, pair)
        tokens_arrive(q, diagonal)
        at = pl.ds(pl.multiple_of(plane_of[q] * block, block), block)

        def more(part, both):
            depth = pl.ds(pl.multiple_of(part * quarter, quarter), quarter)
            return both + jnp.dot(
                tok_all[at, depth], w_gu[depth, :], preferred_element_type=jnp.float32
            )

        both = lax.fori_loop(0, size, more, jnp.zeros((block, 2 * LANES), jnp.float32))
        gate_value = both[:, :LANES]
        up_value = both[:, LANES:]
        hidden[...] = (gate_value / (1.0 + jnp.exp(-gate_value)) * up_value).astype(jnp.bfloat16)
        lanes = lax.broadcasted_iota(jnp.int32, (block, LANES), 1)
        scale = jnp.sum(jnp.where(lanes == me, coef_all[at, :], 0.0), axis=1, keepdims=True)

        @pl.loop(0, width // columns)
        def _(part):
            cols = pl.ds(pl.multiple_of(part * columns, columns), columns)
            value = lax.dot_general(
                hidden[...], w_d[cols, :], (((1,), (1,)), ((), ())),
                preferred_element_type=jnp.float32,
            )
            value = value.astype(jnp.bfloat16).astype(jnp.float32)
            contrib[at, cols] = (value * scale).astype(jnp.bfloat16)

        for row in range(2):
            owner = at_plane(plane_of[q], row * 2 + lax.rem(pair, 2))
            go(is_outer, send(
                contrib.at[token_rows(owner)], pair_in.at[plane_of[q], row],
                pair_send.at[plane_of[q], row], pair_recv.at[plane_of[q], row], beside,
            ))

    def add_rows(parts, target):
        @pl.loop(0, width // columns)
        def _(part):
            cols = pl.ds(pl.multiple_of(part * columns, columns), columns)
            total = sum(source(cols).astype(jnp.float32) for source in parts)
            target[:, cols] = total.astype(jnp.bfloat16)

    def chip_part(q, mine):
        owner_seat, row = (seat, my_row) if mine else (side, 1 - my_row)
        return [
            lambda cols: contrib[token_rows(at_plane(plane_of[q], owner_seat)), cols],
            lambda cols: pair_in[plane_of[q], row, :, cols],
        ]

    def taken(source, sem):
        landed(source, sem)
        return lambda cols: source[:, cols]

    def side_taken(q):
        return taken(side_in.at[plane_of[q]], side_recv.at[plane_of[q]])

    def chain_taken(q):
        return taken(chain_in.at[plane_of[q]], chain_recv.at[plane_of[q]])

    def over_taken(q):
        return taken(over_in.at[plane_of[q]], over_recv.at[plane_of[q]])

    def both_taken():
        return taken(both_in, both_recv)

    def pass_on(is_outer, q, parts):
        at = plane_of[q]
        add_rows(parts, chain_out.at[at])
        if is_outer:
            copy = send(chain_out.at[at], chain_in.at[at], chain_send.at[at], chain_recv.at[at], near_inner)
        elif q == O:
            copy = send(chain_out.at[at], chain_in.at[at], chain_send.at[at], chain_recv.at[at], near_outer)
        else:
            copy = send(chain_out.at[at], over_in.at[at], chain_send.at[at], over_recv.at[at], far_inner)
        go(is_outer, copy)

    def pass_both(is_outer, q):
        add_rows(chip_part(q, False), both_out)
        go(is_outer, send(both_out, both_in, both_send, both_recv, near_inner if is_outer else near_outer))

    def pair_add(is_outer, q):
        at = plane_of[q]
        for row in range(2):
            landed(pair_in.at[at, row], pair_recv.at[at, row])
        if (is_outer, q) == (True, I):
            pass_both(True, q)
            pass_on(True, q, chip_part(q, True))
            return
        if (is_outer, q) == (False, O):
            pass_both(False, q)
            return
        parts = chip_part(q, False)
        if q == (O if is_outer else I):
            parts = parts + [both_taken()]
        add_rows(parts, side_out.at[at])
        go(is_outer, send(side_out.at[at], side_in.at[at], side_send.at[at], side_recv.at[at], across))

    def side_add(is_outer, q):
        parts = chip_part(q, True)
        if is_outer or q != O:
            parts.append(side_taken(q))
        if not is_outer:
            parts.append(over_taken(q) if q == O else chain_taken(q))
        pass_on(is_outer, q, parts)

    def finish_rows(is_outer):
        q = O if is_outer else I
        parts = chip_part(q, True) + [side_taken(q), chain_taken(q)]
        if not is_outer:
            parts.append(over_taken(q))
        add_rows(parts, out)

    steps = (
        own_tokens, seat_tokens, side_tokens, spread, outer_in, inner_in, inner_out, outer_out,
        compute, pair_add, side_add, finish_rows,
    )

    for is_outer, role in ((True, outer), (False, inner)):

        @pl.when(role)
        def _():
            loaded = False
            for place, (name, *arguments) in enumerate(order[0 if is_outer else 1]):
                if name == COMPUTE and not loaded:
                    for load in loads:
                        load.wait()
                    loaded = True
                steps[name](is_outer, *arguments)
                if place == START_LOADS:
                    for load in loads:
                        load.start()
            for copy in sent[is_outer]:
                copy.wait_send()

    for chunk in range(count):
        left = gathered[chunk].at[pl.ds(0, size - 1)]
        landed(left, one_send.at[chunk])
        landed(left, three_send.at[chunk])

    for array in range(3):
        landed(moved[array].at[0], three_recv.at[array])


START_LOADS = 6
LINE_ORDERS = {
    4: (
        ((1, 1, 2, 2, 2, 2, 2, 2, 2), (2, 2, 2, 2, 2, 2, 2, 2), (2, 2, 2, 2, 2, 2, 2, 1, 1)),
        (
            (
            (SPREAD, 0), (SPREAD, 1), (SPREAD, 2), (SPREAD, 3), (OWN,), (OUTER_IN, 0),
            (OUTER_IN, 1), (SPREAD, 4), (SEAT_TOKENS, I), (OUTER_IN, 2), (SPREAD, 5),
            (OUTER_IN, 3), (SPREAD, 6), (SPREAD, 7), (SIDE_TOKENS, I), (SIDE_TOKENS, O),
            (SPREAD, 8), (COMPUTE, I), (SPREAD, 9), (OUTER_IN, 4), (COMPUTE, O), (PAIR_ADD, I),
            (SEAT_TOKENS, J), (OUTER_IN, 5), (OUTER_IN, 6), (SEAT_TOKENS, K), (OUTER_IN, 7),
            (OUTER_OUT, 0), (OUTER_IN, 8), (OUTER_OUT, 1), (OUTER_IN, 9), (SPREAD, 10),
            (OUTER_OUT, 2), (SIDE_TOKENS, J), (COMPUTE, J), (SPREAD, 11), (SIDE_TOKENS, K),
            (OUTER_OUT, 3), (PAIR_ADD, J), (COMPUTE, K), (OUTER_IN, 10), (PAIR_ADD, O),
            (PAIR_ADD, K), (OUTER_IN, 11), (OUTER_OUT, 4), (SIDE_ADD, J), (SPREAD, 12),
            (OUTER_OUT, 5), (SPREAD, 13), (SIDE_ADD, K), (OUTER_OUT, 6), (SPREAD, 14),
            (OUTER_IN, 12), (OUTER_OUT, 7), (SPREAD, 15), (OUTER_IN, 13), (OUTER_OUT, 8),
            (SPREAD, 16), (OUTER_IN, 14), (OUTER_OUT, 9), (SPREAD, 17), (OUTER_IN, 15),
            (OUTER_OUT, 10), (SPREAD, 18), (OUTER_IN, 16), (OUTER_OUT, 11), (SPREAD, 19),
            (OUTER_IN, 17), (SPREAD, 20), (SPREAD, 21), (OUTER_IN, 18), (FINISH,), (SPREAD, 22),
            (SPREAD, 23), (OUTER_IN, 19), (OUTER_OUT, 12), (OUTER_IN, 20), (SPREAD, 24),
            (OUTER_IN, 21), (SPREAD, 25), (OUTER_OUT, 13), (OUTER_IN, 22), (OUTER_IN, 23),
            (OUTER_OUT, 14), (OUTER_IN, 24), (OUTER_IN, 25), (OUTER_OUT, 15), (OUTER_OUT, 16),
            (OUTER_OUT, 17), (OUTER_OUT, 18), (OUTER_OUT, 19), (OUTER_OUT, 20), (OUTER_OUT, 21),
            (OUTER_OUT, 22), (OUTER_OUT, 23), (OUTER_OUT, 24), (OUTER_OUT, 25),
            ),
            (
            (OWN,), (SPREAD, 0), (SPREAD, 1), (SPREAD, 2), (SPREAD, 3), (SPREAD, 4),
            (SIDE_TOKENS, I), (SEAT_TOKENS, J), (SEAT_TOKENS, O), (COMPUTE, I), (INNER_IN, 0),
            (INNER_IN, 1), (SPREAD, 5), (SEAT_TOKENS, K), (INNER_OUT, 0), (INNER_IN, 2),
            (INNER_OUT, 1), (SIDE_TOKENS, J), (INNER_IN, 3), (SPREAD, 6), (COMPUTE, J),
            (SPREAD, 7), (INNER_OUT, 2), (SIDE_TOKENS, O), (PAIR_ADD, J), (COMPUTE, O),
            (INNER_OUT, 3), (INNER_IN, 4), (SIDE_TOKENS, K), (PAIR_ADD, O), (COMPUTE, K),
            (PAIR_ADD, I), (PAIR_ADD, K), (INNER_OUT, 4), (INNER_IN, 5), (SPREAD, 8),
            (INNER_IN, 6), (SPREAD, 9), (INNER_OUT, 5), (INNER_IN, 7), (SPREAD, 10),
            (INNER_OUT, 6), (INNER_IN, 8), (SPREAD, 11), (INNER_OUT, 7), (INNER_IN, 9),
            (SPREAD, 12), (INNER_OUT, 8), (INNER_IN, 10), (SPREAD, 13), (INNER_OUT, 9),
            (INNER_IN, 11), (SPREAD, 14), (INNER_OUT, 10), (SIDE_ADD, J), (SPREAD, 15),
            (INNER_OUT, 11), (SIDE_ADD, K), (SPREAD, 16), (FINISH,), (SPREAD, 17), (INNER_IN, 12),
            (SPREAD, 18), (SIDE_ADD, O), (SPREAD, 19), (INNER_IN, 13), (SPREAD, 20),
            (INNER_OUT, 12), (INNER_IN, 14), (SPREAD, 21), (INNER_OUT, 13), (INNER_IN, 15),
            (SPREAD, 22), (INNER_OUT, 14), (INNER_IN, 16), (SPREAD, 23), (INNER_OUT, 15),
            (INNER_IN, 17), (SPREAD, 24), (SPREAD, 25), (INNER_OUT, 16), (INNER_IN, 18),
            (INNER_OUT, 17), (INNER_IN, 19), (INNER_OUT, 18), (INNER_IN, 20), (INNER_OUT, 19),
            (INNER_IN, 21), (INNER_OUT, 20), (INNER_IN, 22), (INNER_OUT, 21), (INNER_IN, 23),
            (INNER_IN, 24), (INNER_OUT, 22), (INNER_IN, 25), (INNER_OUT, 23), (INNER_OUT, 24),
            (INNER_OUT, 25),
            ),
        ),
    ),
    5: (
        ((1, 1, 2, 2, 2, 2, 2, 2, 2), (2, 2, 2, 2, 2, 2, 2, 2), (2, 2, 2, 2, 2, 2, 2, 1, 1)),
        (
            (
            (SPREAD, 0), (SPREAD, 1), (SPREAD, 2), (SPREAD, 3), (SPREAD, 4), (SPREAD, 5),
            (SPREAD, 6), (SPREAD, 7), (SPREAD, 8), (SPREAD, 9), (SPREAD, 10), (OWN,),
            (OUTER_IN, 0), (OUTER_IN, 1), (SPREAD, 11), (OUTER_IN, 2), (SEAT_TOKENS, I),
            (SPREAD, 12), (OUTER_IN, 3), (SPREAD, 13), (OUTER_IN, 4), (SPREAD, 14), (OUTER_IN, 5),
            (SEAT_TOKENS, J), (OUTER_IN, 6), (OUTER_IN, 7), (SPREAD, 15), (OUTER_IN, 8),
            (SEAT_TOKENS, K), (OUTER_IN, 9), (OUTER_OUT, 0), (OUTER_IN, 10), (OUTER_OUT, 1),
            (SPREAD, 16), (SIDE_TOKENS, O), (SPREAD, 17), (COMPUTE, O), (SPREAD, 18),
            (OUTER_OUT, 2), (OUTER_IN, 11), (OUTER_IN, 12), (OUTER_IN, 13), (SIDE_TOKENS, I),
            (SPREAD, 19), (OUTER_IN, 14), (COMPUTE, I), (SPREAD, 20), (OUTER_OUT, 3),
            (SIDE_TOKENS, J), (PAIR_ADD, I), (SPREAD, 21), (COMPUTE, J), (SPREAD, 22),
            (OUTER_OUT, 4), (OUTER_IN, 15), (PAIR_ADD, J), (SIDE_TOKENS, K), (OUTER_OUT, 5),
            (COMPUTE, K), (OUTER_IN, 16), (OUTER_OUT, 6), (PAIR_ADD, K), (OUTER_IN, 17),
            (OUTER_IN, 18), (OUTER_OUT, 7), (OUTER_IN, 19), (OUTER_IN, 20), (SPREAD, 23),
            (OUTER_OUT, 8), (OUTER_IN, 21), (SPREAD, 24), (OUTER_IN, 22), (SPREAD, 25),
            (PAIR_ADD, O), (OUTER_OUT, 9), (SIDE_ADD, J), (OUTER_OUT, 10), (OUTER_OUT, 11),
            (SIDE_ADD, K), (OUTER_OUT, 12), (OUTER_IN, 23), (OUTER_OUT, 13), (OUTER_IN, 24),
            (OUTER_IN, 25), (OUTER_OUT, 14), (OUTER_OUT, 15), (OUTER_OUT, 16), (OUTER_OUT, 17),
            (OUTER_OUT, 18), (OUTER_OUT, 19), (OUTER_OUT, 20), (OUTER_OUT, 21), (OUTER_OUT, 22),
            (FINISH,), (OUTER_OUT, 23), (OUTER_OUT, 24), (OUTER_OUT, 25),
            ),
            (
            (SPREAD, 0), (SPREAD, 1), (SPREAD, 2), (SPREAD, 3), (SPREAD, 4), (SPREAD, 5),
            (SPREAD, 6), (SPREAD, 7), (SPREAD, 8), (SPREAD, 9), (SPREAD, 10), (OWN,), (SPREAD, 11),
            (SEAT_TOKENS, O), (SEAT_TOKENS, J), (INNER_IN, 0), (INNER_IN, 1), (SPREAD, 12),
            (SEAT_TOKENS, K), (INNER_IN, 2), (INNER_OUT, 0), (INNER_OUT, 1), (INNER_IN, 3),
            (SPREAD, 13), (SPREAD, 14), (INNER_OUT, 2), (INNER_IN, 4), (SPREAD, 15),
            (SIDE_TOKENS, I), (INNER_IN, 5), (SPREAD, 16), (COMPUTE, I), (SPREAD, 17),
            (INNER_OUT, 3), (INNER_IN, 6), (SIDE_TOKENS, J), (INNER_OUT, 4), (COMPUTE, J),
            (INNER_IN, 7), (SPREAD, 18), (SPREAD, 19), (PAIR_ADD, J), (INNER_OUT, 5),
            (SIDE_TOKENS, K), (INNER_IN, 8), (COMPUTE, K), (INNER_OUT, 6), (INNER_IN, 9),
            (PAIR_ADD, K), (INNER_IN, 10), (INNER_OUT, 7), (SIDE_TOKENS, O), (COMPUTE, O),
            (SPREAD, 20), (INNER_OUT, 8), (INNER_IN, 11), (PAIR_ADD, O), (SPREAD, 21),
            (INNER_OUT, 9), (INNER_IN, 12), (SPREAD, 22), (INNER_OUT, 10), (INNER_IN, 13),
            (SPREAD, 23), (INNER_IN, 14), (SPREAD, 24), (INNER_OUT, 11), (SPREAD, 25),
            (PAIR_ADD, I), (INNER_OUT, 12), (INNER_OUT, 13), (INNER_IN, 15), (INNER_OUT, 14),
            (INNER_IN, 16), (INNER_IN, 17), (INNER_OUT, 15), (INNER_IN, 18), (INNER_OUT, 16),
            (INNER_IN, 19), (INNER_OUT, 17), (INNER_IN, 20), (INNER_OUT, 18), (INNER_IN, 21),
            (INNER_IN, 22), (INNER_OUT, 19), (SIDE_ADD, J), (INNER_OUT, 20), (SIDE_ADD, K),
            (INNER_OUT, 21), (INNER_IN, 23), (INNER_IN, 24), (INNER_OUT, 22), (INNER_IN, 25),
            (FINISH,), (SIDE_ADD, O), (INNER_OUT, 23), (INNER_OUT, 24), (INNER_OUT, 25),
            ),
        ),
    ),
    6: (
        ((1, 1, 2, 2, 2, 2, 2, 2, 2), (2, 2, 2, 2, 2, 2, 2, 2), (2, 2, 2, 2, 2, 2, 2, 1, 1)),
        (
            (
            (SPREAD, 0), (SPREAD, 1), (SPREAD, 2), (SPREAD, 3), (OWN,), (OUTER_IN, 0),
            (OUTER_IN, 1), (SPREAD, 4), (OUTER_IN, 2), (SEAT_TOKENS, I), (SPREAD, 5),
            (OUTER_IN, 3), (SPREAD, 6), (SPREAD, 7), (SEAT_TOKENS, J), (SIDE_TOKENS, O),
            (COMPUTE, O), (OUTER_IN, 4), (SIDE_TOKENS, I), (OUTER_IN, 5), (SPREAD, 8),
            (COMPUTE, I), (OUTER_IN, 6), (OUTER_IN, 7), (SPREAD, 9), (SEAT_TOKENS, K),
            (PAIR_ADD, I), (OUTER_OUT, 0), (OUTER_OUT, 1), (SIDE_TOKENS, J), (COMPUTE, J),
            (OUTER_IN, 8), (SPREAD, 10), (OUTER_IN, 9), (SPREAD, 11), (PAIR_ADD, J),
            (SIDE_TOKENS, K), (OUTER_OUT, 2), (COMPUTE, K), (OUTER_IN, 10), (PAIR_ADD, O),
            (PAIR_ADD, K), (OUTER_IN, 11), (OUTER_OUT, 3), (SIDE_ADD, J), (OUTER_OUT, 4),
            (OUTER_OUT, 5), (SPREAD, 12), (SIDE_ADD, K), (SPREAD, 13), (OUTER_OUT, 6),
            (SPREAD, 14), (SPREAD, 15), (OUTER_IN, 12), (OUTER_OUT, 7), (OUTER_IN, 13),
            (SPREAD, 16), (SPREAD, 17), (OUTER_IN, 14), (OUTER_OUT, 8), (OUTER_IN, 15),
            (SPREAD, 18), (SPREAD, 19), (OUTER_IN, 16), (OUTER_OUT, 9), (OUTER_IN, 17),
            (SPREAD, 20), (SPREAD, 21), (OUTER_IN, 18), (OUTER_OUT, 10), (OUTER_IN, 19),
            (SPREAD, 22), (SPREAD, 23), (OUTER_IN, 20), (OUTER_OUT, 11), (OUTER_IN, 21),
            (SPREAD, 24), (SPREAD, 25), (OUTER_IN, 22), (OUTER_IN, 23), (FINISH,), (OUTER_IN, 24),
            (OUTER_IN, 25), (OUTER_OUT, 12), (OUTER_OUT, 13), (OUTER_OUT, 14), (OUTER_OUT, 15),
            (OUTER_OUT, 16), (OUTER_OUT, 17), (OUTER_OUT, 18), (OUTER_OUT, 19), (OUTER_OUT, 20),
            (OUTER_OUT, 21), (OUTER_OUT, 22), (OUTER_OUT, 23), (OUTER_OUT, 24), (OUTER_OUT, 25),
            ),
            (
            (OWN,), (SPREAD, 0), (SPREAD, 1), (SPREAD, 2), (SPREAD, 3), (SPREAD, 4),
            (SEAT_TOKENS, J), (SIDE_TOKENS, I), (SEAT_TOKENS, O), (COMPUTE, I), (INNER_IN, 0),
            (INNER_IN, 1), (SPREAD, 5), (SEAT_TOKENS, K), (INNER_IN, 2), (INNER_OUT, 0),
            (SIDE_TOKENS, J), (INNER_OUT, 1), (INNER_IN, 3), (SPREAD, 6), (COMPUTE, J),
            (SPREAD, 7), (SIDE_TOKENS, O), (SPREAD, 8), (PAIR_ADD, J), (COMPUTE, O),
            (INNER_OUT, 2), (INNER_IN, 4), (SIDE_TOKENS, K), (PAIR_ADD, O), (COMPUTE, K),
            (INNER_OUT, 3), (INNER_IN, 5), (PAIR_ADD, K), (INNER_IN, 6), (INNER_OUT, 4),
            (INNER_IN, 7), (SPREAD, 9), (SPREAD, 10), (INNER_OUT, 5), (PAIR_ADD, I),
            (INNER_OUT, 6), (INNER_IN, 8), (SPREAD, 11), (SPREAD, 12), (INNER_OUT, 7),
            (INNER_IN, 9), (SPREAD, 13), (INNER_IN, 10), (SPREAD, 14), (INNER_OUT, 8),
            (INNER_IN, 11), (SPREAD, 15), (SPREAD, 16), (INNER_OUT, 9), (SIDE_ADD, J),
            (SPREAD, 17), (SIDE_ADD, K), (SPREAD, 18), (INNER_OUT, 10), (INNER_IN, 12),
            (SPREAD, 19), (SPREAD, 20), (INNER_OUT, 11), (INNER_IN, 13), (SPREAD, 21), (FINISH,),
            (INNER_IN, 14), (SPREAD, 22), (SPREAD, 23), (SIDE_ADD, O), (INNER_IN, 15),
            (SPREAD, 24), (SPREAD, 25), (INNER_IN, 16), (INNER_OUT, 12), (INNER_IN, 17),
            (INNER_OUT, 13), (INNER_IN, 18), (INNER_IN, 19), (INNER_OUT, 14), (INNER_IN, 20),
            (INNER_OUT, 15), (INNER_IN, 21), (INNER_IN, 22), (INNER_OUT, 16), (INNER_IN, 23),
            (INNER_IN, 24), (INNER_OUT, 17), (INNER_IN, 25), (INNER_OUT, 18), (INNER_OUT, 19),
            (INNER_OUT, 20), (INNER_OUT, 21), (INNER_OUT, 22), (INNER_OUT, 23), (INNER_OUT, 24),
            (INNER_OUT, 25),
            ),
        ),
    ),
    8: (
        ((1, 1, 2, 2, 2, 2, 2, 2, 2), (2, 2, 2, 2, 2, 2, 2, 2), (2, 2, 2, 2, 2, 2, 2, 1, 1)),
        (
            (
            (SPREAD, 0), (SPREAD, 1), (SPREAD, 2), (SPREAD, 3), (SPREAD, 4), (SPREAD, 5),
            (SPREAD, 6), (SPREAD, 7), (SPREAD, 8), (SPREAD, 9), (SPREAD, 10), (OWN,),
            (OUTER_IN, 0), (OUTER_IN, 1), (SPREAD, 11), (OUTER_IN, 2), (SEAT_TOKENS, I),
            (SPREAD, 12), (OUTER_IN, 3), (SPREAD, 13), (OUTER_IN, 4), (SPREAD, 14),
            (SIDE_TOKENS, I), (OUTER_IN, 5), (SPREAD, 15), (COMPUTE, I), (OUTER_IN, 6),
            (SPREAD, 16), (SEAT_TOKENS, J), (OUTER_IN, 7), (PAIR_ADD, I), (OUTER_IN, 8),
            (SEAT_TOKENS, K), (OUTER_IN, 9), (OUTER_OUT, 0), (OUTER_IN, 10), (OUTER_OUT, 1),
            (SIDE_TOKENS, O), (SPREAD, 17), (COMPUTE, O), (OUTER_IN, 11), (SPREAD, 18),
            (OUTER_IN, 12), (SPREAD, 19), (OUTER_IN, 13), (SPREAD, 20), (OUTER_IN, 14),
            (OUTER_OUT, 2), (OUTER_IN, 15), (SPREAD, 21), (OUTER_IN, 16), (SPREAD, 22),
            (SPREAD, 23), (SIDE_TOKENS, J), (OUTER_OUT, 3), (COMPUTE, J), (SPREAD, 24),
            (SIDE_TOKENS, K), (SPREAD, 25), (PAIR_ADD, J), (COMPUTE, K), (OUTER_IN, 17),
            (OUTER_OUT, 4), (PAIR_ADD, K), (OUTER_IN, 18), (OUTER_IN, 19), (OUTER_IN, 20),
            (OUTER_OUT, 5), (OUTER_IN, 21), (OUTER_IN, 22), (OUTER_IN, 23), (OUTER_IN, 24),
            (OUTER_IN, 25), (OUTER_OUT, 6), (SIDE_ADD, J), (PAIR_ADD, O), (OUTER_OUT, 7),
            (SIDE_ADD, K), (OUTER_OUT, 8), (OUTER_OUT, 9), (OUTER_OUT, 10), (OUTER_OUT, 11),
            (OUTER_OUT, 12), (OUTER_OUT, 13), (OUTER_OUT, 14), (OUTER_OUT, 15), (OUTER_OUT, 16),
            (OUTER_OUT, 17), (OUTER_OUT, 18), (OUTER_OUT, 19), (OUTER_OUT, 20), (OUTER_OUT, 21),
            (OUTER_OUT, 22), (OUTER_OUT, 23), (OUTER_OUT, 24), (OUTER_OUT, 25), (FINISH,),
            ),
            (
            (OWN,), (SPREAD, 0), (SPREAD, 1), (SPREAD, 2), (SPREAD, 3), (SPREAD, 4), (SPREAD, 5),
            (SPREAD, 6), (SPREAD, 7), (SPREAD, 8), (SPREAD, 9), (SPREAD, 10), (SPREAD, 11),
            (SIDE_TOKENS, I), (SEAT_TOKENS, J), (SEAT_TOKENS, O), (COMPUTE, I), (INNER_IN, 0),
            (INNER_IN, 1), (SPREAD, 12), (SEAT_TOKENS, K), (INNER_IN, 2), (INNER_OUT, 0),
            (SPREAD, 13), (INNER_IN, 3), (SPREAD, 14), (INNER_OUT, 1), (INNER_IN, 4), (SPREAD, 15),
            (SPREAD, 16), (INNER_IN, 5), (SPREAD, 17), (INNER_OUT, 2), (INNER_IN, 6), (SPREAD, 18),
            (SIDE_TOKENS, J), (SPREAD, 19), (COMPUTE, J), (INNER_IN, 7), (SPREAD, 20),
            (INNER_OUT, 3), (PAIR_ADD, J), (SIDE_TOKENS, K), (PAIR_ADD, I), (COMPUTE, K),
            (PAIR_ADD, K), (INNER_OUT, 4), (INNER_IN, 8), (INNER_IN, 9), (INNER_OUT, 5),
            (INNER_IN, 10), (SPREAD, 21), (SPREAD, 22), (SIDE_TOKENS, O), (SPREAD, 23),
            (COMPUTE, O), (SPREAD, 24), (SPREAD, 25), (INNER_OUT, 6), (INNER_IN, 11),
            (PAIR_ADD, O), (INNER_IN, 12), (INNER_OUT, 7), (INNER_IN, 13), (INNER_IN, 14),
            (INNER_OUT, 8), (INNER_IN, 15), (INNER_IN, 16), (INNER_OUT, 9), (INNER_IN, 17),
            (INNER_IN, 18), (INNER_OUT, 10), (INNER_IN, 19), (INNER_IN, 20), (INNER_OUT, 11),
            (INNER_IN, 21), (INNER_IN, 22), (INNER_OUT, 12), (INNER_IN, 23), (INNER_IN, 24),
            (INNER_IN, 25), (INNER_OUT, 13), (SIDE_ADD, J), (SIDE_ADD, K), (INNER_OUT, 14),
            (INNER_OUT, 15), (INNER_OUT, 16), (INNER_OUT, 17), (INNER_OUT, 18), (INNER_OUT, 19),
            (INNER_OUT, 20), (INNER_OUT, 21), (INNER_OUT, 22), (INNER_OUT, 23), (INNER_OUT, 24),
            (INNER_OUT, 25), (FINISH,), (SIDE_ADD, O),
            ),
        ),
    ),
}


def call_line(n, most, which, table, tokens, coef, held_gate, held_up, held_down):
    rows, width = tokens.shape
    size = 4
    planes = n // size
    quarter = width // size
    cuts, order = LINE_ORDERS[most]
    plan = chunk_plan(quarter, cuts)
    count = len(plan)
    vmem = pl.BlockSpec(memory_space=pltpu.VMEM)
    anywhere = pl.BlockSpec(memory_space=pl.ANY)
    dma = pltpu.SemaphoreType.DMA
    moved_shape = jax.ShapeDtypeStruct(held_gate.shape, held_gate.dtype)

    def block(*shape):
        return pltpu.VMEM(shape, jnp.bfloat16)

    return pl.pallas_call(
        functools.partial(line_kernel, n, most, plan, order),
        out_shape=(jax.ShapeDtypeStruct((rows, width), jnp.bfloat16),) + (moved_shape,) * 3,
        in_specs=[pl.BlockSpec(memory_space=pltpu.SMEM), vmem, vmem] + [anywhere] * 3,
        out_specs=(vmem, anywhere, anywhere, anywhere),
        scratch_shapes=[
            *(block(2 * size, length, LANES) for _, _, length in plan),
            *(block(most, length, LANES) for _, _, length in plan),
            block(most, 3 * quarter, LANES),
            block(2 * size, 3 * quarter, LANES),
            block(n * rows, width),
            pltpu.VMEM((n * rows, LANES), jnp.float32),
            block(width, 2 * LANES),
            block(width, LANES),
            block(size * rows, LANES),
            block(n * rows, width),
            block(planes, 2, rows, width),
            block(planes, rows, width),
            block(planes, rows, width),
            block(planes, rows, width),
            block(planes, rows, width),
            block(planes, rows, width),
            block(rows, width),
            block(rows, width),
            dma((3,)),
            dma((2, planes, 6)),
            dma((2, n)),
            dma((count,)),
            dma((count,)),
            dma((count,)),
            dma((count,)),
            dma((count,)),
            dma((count,)),
            dma((count,)),
            dma((count,)),
            dma((count,)),
            dma((3,)),
            dma((planes, 2)),
            dma((planes, 2)),
            dma((planes,)),
            dma((planes,)),
            dma((planes,)),
            dma((planes,)),
            dma((planes,)),
            dma,
            dma,
        ],
        compiler_params=pltpu.CompilerParams(
            collective_id=which, has_side_effects=True, vmem_limit_bytes=VMEM_BYTES
        ),
    )(table, tokens, coef, held_gate, held_up, held_down)


def per_device(
    tokens, route_ids, route_logits, old_place, new_place, held_gate, held_up, held_down
):
    n = lax.axis_size("expert")
    half = n // 2
    device_ids = jnp.arange(n, dtype=jnp.int32)
    blocks = n // EXPERTS
    at_old = (old_place[:, None] == device_ids[None, :]).astype(jnp.int32)
    dest_of = jnp.sum(at_old * new_place[:, None], axis=0)
    expert_at = jnp.sum(at_old * device_ids[:, None], axis=0) // blocks
    half_of = device_ids // half
    crosses = (dest_of // half != half_of).astype(jnp.int32)
    earlier = (half_of[:, None] == half_of[None, :]) & (device_ids[:, None] < device_ids[None, :])
    turn = jnp.sum(earlier.astype(jnp.int32) * crosses[:, None], axis=0)
    lane_of = device_ids - half_of * half
    leaving = (half_of[:, None] * half + turn[:, None] == device_ids[None, :]).astype(jnp.int32)
    leaving = jnp.sum(leaving * (crosses * lane_of)[:, None], axis=0)
    arriving = (dest_of[:, None] == device_ids[None, :]).astype(jnp.int32)
    table = jnp.concatenate([
        leaving,
        jnp.sum(arriving * crosses[:, None], axis=0),
        jnp.sum(arriving * ((1 - crosses) * lane_of)[:, None], axis=0),
        jnp.sum(arriving * (crosses * turn)[:, None], axis=0),
    ])
    first_weight = 1.0 / (1.0 + jnp.exp(route_logits[:, 1] - route_logits[:, 0]))
    second_weight = 1.0 / (1.0 + jnp.exp(route_logits[:, 0] - route_logits[:, 1]))
    coef = jnp.where(route_ids[:, 0:1] == expert_at[None, :], first_weight[:, None], 0.0)
    coef = coef + jnp.where(route_ids[:, 1:2] == expert_at[None, :], second_weight[:, None], 0.0)
    coef = jnp.pad(coef, ((0, 0), (0, LANES - n)))
    table, coef = lax.optimization_barrier((table, coef))
    in_line = near_square_root(n) == 4 and n == 16
    shares = (4, 5, 6, 8) if in_line else (3, 4, 5, 6, 8)
    levels = sorted({max(1, half * eighths // 8) for eighths in shares})
    call = call_line if in_line else call_layer
    crossing = jnp.sum(crosses) // 2
    level = sum((crossing > most).astype(jnp.int32) for most in levels[:-1])
    branches = [functools.partial(call, n, most, i) for i, most in enumerate(levels)]
    return lax.switch(level, branches, table, tokens, coef, held_gate, held_up, held_down)


def solution(mesh):
    split = ("groups", "expert")
    placed = (
        P(split, None),
        P(split, None),
        P(split, None),
        P(),
        P(),
        P(split, None, None),
        P(split, None, None),
        P(split, None, None),
    )
    return jax.shard_map(
        per_device,
        mesh=mesh,
        in_specs=placed,
        out_specs=(
            P(split, None),
            P(split, None, None),
            P(split, None, None),
            P(split, None, None),
        ),
        check_vma=False,
    )
```

```python
import functools

import jax
import jax.numpy as jnp
from jax import lax
from jax.experimental import pallas as pl
from jax.experimental.pallas import tpu as pltpu
from jax.sharding import PartitionSpec as P

EXPERTS = 8
LANES = 128
MESH = pl.DeviceIdType.MESH
VMEM_BYTES = 63_000_000


def near_square_root(n):
    size = 1
    while size * size < n:
        size *= 2
    return size


def layer_kernel(
    n,
    most,
    table,
    tok,
    coef,
    held_g,
    held_u,
    held_d,
    out,
    moved_g,
    moved_u,
    moved_d,
    tok_all,
    coef_all,
    w_gu,
    w_d,
    pieces_g,
    pieces_u,
    pieces_d,
    crossed_g,
    crossed_u,
    crossed_d,
    ordered,
    hidden,
    contrib,
    part_in,
    plane_sum,
    half_in,
    cross_out,
    cross_in,
    load_sem,
    tok_send,
    fwd_send,
    plane_send,
    tok_recv,
    one_send,
    one_recv,
    two_send,
    two_recv,
    three_send,
    three_recv,
    part_send,
    part_recv,
    half_send,
    half_recv,
    cross_send,
    cross_recv,
):
    me = lax.axis_index("expert")
    half = n // 2
    base = (me // half) * half
    lane = me - base
    twin = lax.rem(me + half, n)
    rows, width = tok.shape
    band = width // half
    size = near_square_root(n)
    planes = n // size
    half_planes = planes // 2
    plane = me // size
    seat = me - plane * size
    my_plane_of_half = lane // size
    held = (held_g, held_u, held_d)
    moved = (moved_g, moved_u, moved_d)
    pieces = (pieces_g, pieces_u, pieces_d)
    crossed = (crossed_g, crossed_u, crossed_d)

    barrier = pltpu.get_barrier_semaphore()

    @pl.loop(1, n)
    def _(k):
        pl.semaphore_signal(
            barrier, inc=1, device_id={"expert": lax.rem(me + k, n)}, device_id_type=MESH
        )

    loads = (
        pltpu.make_async_copy(held_g.at[0], w_gu.at[:, pl.ds(0, LANES)], load_sem.at[0]),
        pltpu.make_async_copy(held_u.at[0], w_gu.at[:, pl.ds(LANES, LANES)], load_sem.at[1]),
        pltpu.make_async_copy(held_d.at[0], w_d, load_sem.at[2]),
    )
    for load in loads:
        load.start()

    def token_rows(owner):
        return pl.ds(pl.multiple_of(owner * rows, rows), rows)

    def band_rows(owner):
        return pl.ds(pl.multiple_of(owner * band, band), band)

    def near(k):
        return base + lax.rem(lane + k, half)

    def column(k):
        return base + lax.rem(lane + k * size, half)

    def mate(k):
        return plane * size + lax.rem(seat + k, size)

    def seated(other_plane):
        return other_plane * size + seat

    tok_all[token_rows(me), :] = tok[...]
    coef_all[token_rows(me), :] = coef[...]
    pl.semaphore_wait(barrier, n - 1)

    def send(source, target, send_sem, recv_sem, peer):
        return pltpu.make_async_remote_copy(
            src_ref=source, dst_ref=target, send_sem=send_sem, recv_sem=recv_sem,
            device_id={"expert": peer}, device_id_type=MESH,
        )

    def own_tokens(peer):
        at = token_rows(me)
        return (
            send(tok, tok_all.at[at], tok_send.at[0, peer], tok_recv.at[0, me], peer),
            send(coef, coef_all.at[at], tok_send.at[1, peer], tok_recv.at[1, me], peer),
        )

    def passed_tokens(owner, peer, sems):
        at = token_rows(owner)
        return (
            send(tok_all.at[at], tok_all.at[at], sems[0], tok_recv.at[0, owner], peer),
            send(coef_all.at[at], coef_all.at[at], sems[1], tok_recv.at[1, owner], peer),
        )

    def twin_tokens(peer):
        return passed_tokens(twin, peer, (fwd_send.at[0, peer], fwd_send.at[1, peer]))

    def plane_tokens(other_plane, k):
        sems = (plane_send.at[0, other_plane, k], plane_send.at[1, other_plane, k])
        return passed_tokens(seated(other_plane), mate(k), sems)

    def tokens_arrive(owner):
        pltpu.make_async_copy(tok, tok_all.at[token_rows(owner)], tok_recv.at[0, owner]).wait()
        pltpu.make_async_copy(coef, coef_all.at[token_rows(owner)], tok_recv.at[1, owner]).wait()

    def spread(array):
        pltpu.make_async_copy(
            held[array].at[0, band_rows(lane)], pieces[array].at[lane], one_recv.at[array]
        ).start()

        @pl.loop(1, half)
        def _(k):
            peer = near(k)
            send(
                held[array].at[0, band_rows(peer - base)], pieces[array].at[lane],
                one_send.at[array], one_recv.at[array], peer,
            ).start()

    def swap(array):
        return send(
            ordered.at[array, pl.ds(0, most)], crossed[array],
            two_send.at[array], two_recv.at[array], twin,
        )

    def cross_over(array):
        pltpu.make_async_copy(pieces[array], pieces[array], one_recv.at[array]).wait()

        @pl.loop(0, most)
        def _(m):
            ordered[array, m] = pieces[array][table[base + m]]

        swap(array).start()

    def deliver(array):
        swap(array).wait()

        @pl.loop(0, half)
        def _(place):
            at = base + place
            own = pieces[array][table[2 * n + at]]
            other = crossed[array][table[3 * n + at]]
            ordered[array, place] = jnp.where(table[n + at] == 1, other, own)

        pltpu.make_async_copy(
            ordered.at[array, lane], moved[array].at[0, band_rows(lane)], three_recv.at[array]
        ).start()

        @pl.loop(1, half)
        def _(k):
            peer = near(k)
            send(
                ordered.at[array, peer - base], moved[array].at[0, band_rows(lane)],
                three_send.at[array], three_recv.at[array], peer,
            ).start()

    for copy in own_tokens(twin):
        copy.start()

    @pl.loop(1, half_planes)
    def _(k):
        for copy in own_tokens(column(k)):
            copy.start()

    @pl.loop(1, size)
    def _(k):
        for copy in own_tokens(mate(k)):
            copy.start()

    spread(0)
    tokens_arrive(twin)

    @pl.loop(1, half_planes)
    def _(k):
        for copy in twin_tokens(column(k)):
            copy.start()

    spread(1)

    @pl.loop(1, half_planes)
    def _(k):
        tokens_arrive(column(k))
        tokens_arrive(lax.rem(column(k) + half, n))

    @pl.loop(1, planes)
    def _(shift):
        @pl.loop(1, size)
        def _(k):
            for copy in plane_tokens(lax.rem(plane + shift, planes), k):
                copy.start()

    spread(2)
    cross_over(0)
    cross_over(1)

    @pl.loop(0, planes)
    def _(other_plane):
        @pl.loop(1, size)
        def _(k):
            tokens_arrive(other_plane * size + lax.rem(seat + k, size))

    for load in loads:
        load.wait()

    step = min(256, n * rows)
    columns = 512

    @pl.loop(0, n * rows // step)
    def _(block):
        at = pl.ds(pl.multiple_of(block * step, step), step)
        both = jnp.dot(tok_all[at, :], w_gu[...], preferred_element_type=jnp.float32)
        gate_value = both[:, :LANES]
        up_value = both[:, LANES:]
        hidden[...] = (gate_value / (1.0 + jnp.exp(-gate_value)) * up_value).astype(jnp.bfloat16)
        lanes = lax.broadcasted_iota(jnp.int32, (step, LANES), 1)
        scale = jnp.sum(jnp.where(lanes == me, coef_all[at, :], 0.0), axis=1, keepdims=True)

        @pl.loop(0, width // columns)
        def _(part):
            cols = pl.ds(pl.multiple_of(part * columns, columns), columns)
            value = lax.dot_general(
                hidden[...], w_d[cols, :], (((1,), (1,)), ((), ())),
                preferred_element_type=jnp.float32,
            )
            value = value.astype(jnp.bfloat16).astype(jnp.float32)
            contrib[at, cols] = (value * scale).astype(jnp.bfloat16)

    def part_copy(k, other_plane):
        peer = mate(k)
        owner = other_plane * size + lax.rem(seat + k, size)
        return send(
            contrib.at[token_rows(owner)], part_in.at[seat, other_plane],
            part_send.at[k, other_plane], part_recv.at[seat, other_plane], peer,
        )

    def half_copy(k, kind):
        peer = column(k)
        target = peer // size if kind == 0 else lax.rem(peer // size + half_planes, planes)
        return send(
            plane_sum.at[target], half_in.at[kind, my_plane_of_half],
            half_send.at[kind, k], half_recv.at[kind, my_plane_of_half], peer,
        )

    @pl.loop(0, planes)
    def _(other_plane):
        @pl.loop(1, size)
        def _(k):
            part_copy(k, other_plane).start()

    def add_plane():
        @pl.loop(0, planes)
        def _(other_plane):
            @pl.loop(1, size)
            def _(k):
                spot = part_in.at[lax.rem(seat + k, size), other_plane]
                pltpu.make_async_copy(
                    spot, spot, part_recv.at[lax.rem(seat + k, size), other_plane]
                ).wait()

            @pl.loop(0, width // columns)
            def _(part):
                cols = pl.ds(pl.multiple_of(part * columns, columns), columns)

                def more(k, total):
                    other = lax.rem(seat + k, size)
                    return total + part_in[other, other_plane, :, cols].astype(jnp.float32)

                total = contrib[token_rows(seated(other_plane)), cols].astype(jnp.float32)
                total = lax.fori_loop(1, size, more, total)
                plane_sum[other_plane, :, cols] = total.astype(jnp.bfloat16)

        for kind in (1, 0):

            @pl.loop(1, half_planes)
            def _(k):
                half_copy(k, kind).start()

    def add_half(kind, own_plane, extra, target):
        @pl.loop(1, half_planes)
        def _(k):
            other = lax.rem(my_plane_of_half + k, half_planes)
            spot = half_in.at[kind, other]
            pltpu.make_async_copy(spot, spot, half_recv.at[kind, other]).wait()

        @pl.loop(0, width // columns)
        def _(part):
            cols = pl.ds(pl.multiple_of(part * columns, columns), columns)

            def more(k, total):
                other = lax.rem(my_plane_of_half + k, half_planes)
                return total + half_in[kind, other, :, cols].astype(jnp.float32)

            total = plane_sum[own_plane, :, cols].astype(jnp.float32)
            if extra is not None:
                total = total + extra[:, cols].astype(jnp.float32)
            target[:, cols] = lax.fori_loop(1, half_planes, more, total).astype(jnp.bfloat16)

    deliver(0)
    cross_over(2)
    add_plane()
    deliver(1)
    add_half(1, lax.rem(plane + half_planes, planes), None, cross_out)
    cross = send(cross_out, cross_in, cross_send, cross_recv, twin)
    cross.start()
    deliver(2)
    cross.wait()
    add_half(0, plane, cross_in, out)

    for copy in own_tokens(twin):
        copy.wait_send()

    @pl.loop(1, half_planes)
    def _(k):
        for copy in own_tokens(column(k)):
            copy.wait_send()
        for copy in twin_tokens(column(k)):
            copy.wait_send()
        half_copy(k, 0).wait_send()
        half_copy(k, 1).wait_send()

    @pl.loop(1, size)
    def _(k):
        for copy in own_tokens(mate(k)):
            copy.wait_send()

        @pl.loop(0, planes)
        def _(other_plane):
            part_copy(k, other_plane).wait_send()

        @pl.loop(1, planes)
        def _(shift):
            for copy in plane_tokens(lax.rem(plane + shift, planes), k):
                copy.wait_send()

    for array in range(3):
        sent = pieces[array].at[pl.ds(0, half - 1)]
        pltpu.make_async_copy(sent, sent, one_send.at[array]).wait()
        pltpu.make_async_copy(sent, sent, three_send.at[array]).wait()
        pltpu.make_async_copy(
            moved[array].at[0], moved[array].at[0], three_recv.at[array]
        ).wait()


def call_layer(n, most, which, table, tokens, coef, held_gate, held_up, held_down):
    rows, width = tokens.shape
    half = n // 2
    band = width // half
    size = near_square_root(n)
    planes = n // size
    vmem = pl.BlockSpec(memory_space=pltpu.VMEM)
    anywhere = pl.BlockSpec(memory_space=pl.ANY)
    dma = pltpu.SemaphoreType.DMA
    moved_shape = jax.ShapeDtypeStruct(held_gate.shape, held_gate.dtype)

    def block(*shape):
        return pltpu.VMEM(shape, jnp.bfloat16)

    return pl.pallas_call(
        functools.partial(layer_kernel, n, most),
        out_shape=(jax.ShapeDtypeStruct((rows, width), jnp.bfloat16),) + (moved_shape,) * 3,
        in_specs=[pl.BlockSpec(memory_space=pltpu.SMEM), vmem, vmem] + [anywhere] * 3,
        out_specs=(vmem, anywhere, anywhere, anywhere),
        scratch_shapes=[
            block(n * rows, width),
            pltpu.VMEM((n * rows, LANES), jnp.float32),
            block(width, 2 * LANES),
            block(width, LANES),
            block(half, band, LANES),
            block(half, band, LANES),
            block(half, band, LANES),
            block(most, band, LANES),
            block(most, band, LANES),
            block(most, band, LANES),
            block(3, half, band, LANES),
            block(min(256, n * rows), LANES),
            block(n * rows, width),
            block(size, planes, rows, width),
            block(planes, rows, width),
            block(2, planes // 2, rows, width),
            block(rows, width),
            block(rows, width),
            dma((3,)),
            dma((2, n)),
            dma((2, n)),
            dma((2, planes, size)),
            dma((2, n)),
            dma((3,)),
            dma((3,)),
            dma((3,)),
            dma((3,)),
            dma((3,)),
            dma((3,)),
            dma((size, planes)),
            dma((size, planes)),
            dma((2, planes // 2)),
            dma((2, planes // 2)),
            dma,
            dma,
        ],
        compiler_params=pltpu.CompilerParams(
            collective_id=which, has_side_effects=True, vmem_limit_bytes=VMEM_BYTES
        ),
    )(table, tokens, coef, held_gate, held_up, held_down)


O, I, J, K = range(4)
(
    OWN, SEAT_TOKENS, SIDE_TOKENS, SPREAD, OUTER_IN, INNER_IN, INNER_OUT, OUTER_OUT,
    COMPUTE, PAIR_ADD, SIDE_ADD, FINISH,
) = range(12)


def chunk_plan(quarter, cuts):
    plan = []
    for array in range(3):
        start = 0
        for cut in cuts[array]:
            size = quarter * cut // 16
            plan.append((array, start, size))
            start += size
        assert start == quarter
    return tuple(plan)


def line_kernel(
    n, most, plan, order, table, tok, coef, held_g, held_u, held_d, out, moved_g, moved_u, moved_d, *rest
):
    count = len(plan)
    gathered, rest = rest[:count], rest[count:]
    crossed, rest = rest[:count], rest[count:]
    (
        leaving, ordered, tok_all, coef_all, w_gu, w_d, hidden, contrib,
        pair_in, side_out, side_in, chain_in, chain_out, over_in, both_in, both_out,
        load_sem, tok_send, tok_recv,
        one_send, one_recv, two_send, two_recv, cross_send, cross_recv,
        back_send, back_recv, three_send, three_recv,
        pair_send, pair_recv, side_send, side_recv, chain_send, chain_recv,
        over_recv, both_send, both_recv,
    ) = rest
    size = 4
    last = n // size - 1
    me = lax.axis_index("expert")
    plane = me // size
    seat = me - plane * size
    half = plane // 2
    base = half * (n // 2)
    own_at = lax.rem(plane, 2) * size
    other_at = size - own_at
    inner = (plane == 1) | (plane == 2)
    outer = (plane == 0) | (plane == last)
    side = lax.rem(seat + 2, size)
    pair = seat + 1 - 2 * lax.rem(seat, 2)
    diagonal = lax.rem(pair + 2, size)
    my_row = seat // 2
    rows, width = tok.shape
    quarter = width // size
    held = (held_g, held_u, held_d)
    moved = (moved_g, moved_u, moved_d)
    plane_of = (last * half, 1 + half, last - 1 - half, last - last * half)

    def at_plane(other, other_seat):
        return other * size + other_seat

    near_outer, near_inner = at_plane(plane_of[O], seat), at_plane(plane_of[I], seat)
    far_inner = at_plane(plane_of[J], seat)
    beside, across = at_plane(plane, pair), at_plane(plane, side)

    barrier = pltpu.get_barrier_semaphore()

    def greet(peer):
        pl.semaphore_signal(barrier, inc=1, device_id={"expert": peer}, device_id_type=MESH)

    @pl.loop(1, size)
    def _(k):
        greet(at_plane(plane, lax.rem(seat + k, size)))

    @pl.when(outer)
    def _():
        greet(near_inner)

    @pl.when(inner)
    def _():
        greet(near_outer)
        greet(far_inner)

    loads = (
        pltpu.make_async_copy(held_g.at[0], w_gu.at[:, pl.ds(0, LANES)], load_sem.at[0]),
        pltpu.make_async_copy(held_u.at[0], w_gu.at[:, pl.ds(LANES, LANES)], load_sem.at[1]),
        pltpu.make_async_copy(held_d.at[0], w_d, load_sem.at[2]),
    )

    def token_rows(owner):
        return pl.ds(pl.multiple_of(owner * rows, rows), rows)

    tok_all[token_rows(me), :] = tok[...]
    coef_all[token_rows(me), :] = coef[...]

    @pl.when(inner)
    def _():
        pl.semaphore_wait(barrier, size + 1)

    @pl.when(outer)
    def _():
        pl.semaphore_wait(barrier, size)

    def send(source, target, send_sem, recv_sem, peer):
        return pltpu.make_async_remote_copy(
            src_ref=source, dst_ref=target, send_sem=send_sem, recv_sem=recv_sem,
            device_id={"expert": peer}, device_id_type=MESH,
        )

    def landed(spot, sem):
        pltpu.make_async_copy(spot, spot, sem).wait()

    sent = {True: [], False: []}

    def go(role, *copies):
        for copy in copies:
            copy.start()
        sent[role].extend(copies)

    def tokens_to(q, owner_seat, peer, path, own=False):
        owner_plane = plane_of[q]
        owner = at_plane(owner_plane, owner_seat)
        at = token_rows(owner)
        token_source, coef_source = (tok, coef) if own else (tok_all.at[at], coef_all.at[at])
        return (
            send(token_source, tok_all.at[at], tok_send.at[0, owner_plane, path], tok_recv.at[0, owner], peer),
            send(coef_source, coef_all.at[at], tok_send.at[1, owner_plane, path], tok_recv.at[1, owner], peer),
        )

    def tokens_arrive(q, owner_seat):
        owner = at_plane(plane_of[q], owner_seat)
        landed(tok_all.at[token_rows(owner)], tok_recv.at[0, owner])
        landed(coef_all.at[token_rows(owner)], tok_recv.at[1, owner])

    def own_tokens(is_outer):
        if is_outer:
            go(True, *tokens_to(O, seat, near_inner, 0, True))
        else:
            go(False, *tokens_to(I, seat, near_outer, 0, True))
            go(False, *tokens_to(I, seat, far_inner, 1, True))
        mine = O if is_outer else I
        go(is_outer, *tokens_to(mine, seat, across, 2, True))
        go(is_outer, *tokens_to(mine, seat, beside, 3, True))

    def seat_tokens(is_outer, q):
        tokens_arrive(q, seat)
        if not is_outer:
            if q == O:
                go(False, *tokens_to(q, seat, far_inner, 1))
            else:
                go(False, *tokens_to(q, seat, near_outer, 0))
        if (is_outer, q) not in ((True, I), (False, O)):
            go(is_outer, *tokens_to(q, seat, across, 2))
        go(is_outer, *tokens_to(q, seat, beside, 3))

    def side_tokens(is_outer, q):
        tokens_arrive(q, side)
        if (is_outer, q) == (True, O):
            go(True, *tokens_to(q, side, near_inner, 5))
        if (is_outer, q) == (False, I):
            go(False, *tokens_to(q, side, near_outer, 5))
        go(is_outer, *tokens_to(q, side, beside, 4))

    def band(chunk, owner):
        _, first, length = plan[chunk]
        return pl.ds(pl.multiple_of(owner * quarter + first, 16), length)

    def spread(is_outer, chunk):
        array = plan[chunk][0]
        spot = gathered[chunk].at[own_at + seat]
        pltpu.make_async_copy(held[array].at[0, band(chunk, seat)], spot, one_recv.at[chunk]).start()
        for k in (2, 1, 3):
            peer = lax.rem(seat + k, size)
            send(
                held[array].at[0, band(chunk, peer)], spot, one_send.at[chunk],
                one_recv.at[chunk], at_plane(plane, peer),
            ).start()

    def own_part(chunk):
        return gathered[chunk].at[pl.ds(own_at, size)]

    def other_part(chunk):
        return gathered[chunk].at[pl.ds(other_at, size)]

    def flat_at(chunk):
        return pl.ds(sum(length for _, _, length in plan[:chunk]), plan[chunk][2])

    def deliver(chunk, piece_of):
        array = plan[chunk][0]
        target = moved[array].at[0, band(chunk, seat)]
        for k in (2, 1, 3):
            peer = lax.rem(seat + k, size)
            send(
                piece_of(peer), target, three_send.at[chunk], three_recv.at[array],
                at_plane(plane, peer),
            ).start()
        pltpu.make_async_copy(piece_of(seat), target, three_recv.at[array]).start()

    def outer_in(is_outer, chunk):
        landed(own_part(chunk), one_recv.at[chunk])
        go(True, send(
            own_part(chunk), own_part(chunk), two_send.at[chunk], two_recv.at[chunk], near_inner
        ))

    def inner_in(is_outer, chunk):
        landed(own_part(chunk), one_recv.at[chunk])
        landed(other_part(chunk), two_recv.at[chunk])
        flat = flat_at(chunk)

        @pl.loop(0, most)
        def _(m):
            leaving[m, flat] = gathered[chunk][table[base + m]]

        go(False, send(
            leaving.at[:, flat], crossed[chunk], cross_send.at[chunk], cross_recv.at[chunk], far_inner
        ))

    def inner_out(is_outer, chunk):
        landed(crossed[chunk], cross_recv.at[chunk])
        flat = flat_at(chunk)

        @pl.loop(0, 2 * size)
        def _(place):
            at = base + place
            own = gathered[chunk][table[2 * n + at]]
            other = crossed[chunk][table[3 * n + at]]
            ordered[place, flat] = jnp.where(table[n + at] == 1, other, own)

        go(False, send(
            ordered.at[pl.ds(other_at, size), flat], own_part(chunk), back_send.at[chunk],
            back_recv.at[chunk], near_outer,
        ))
        deliver(chunk, lambda s: ordered.at[own_at + s, flat])

    def outer_out(is_outer, chunk):
        landed(other_part(chunk), back_recv.at[chunk])
        deliver(chunk, lambda s: gathered[chunk].at[other_at + s])

    block = size * rows
    columns = 512

    def compute(is_outer, q):
        tokens_arrive(q, pair)
        tokens_arrive(q, diagonal)
        at = pl.ds(pl.multiple_of(plane_of[q] * block, block), block)

        def more(part, both):
            depth = pl.ds(pl.multiple_of(part * quarter, quarter), quarter)
            return both + jnp.dot(
                tok_all[at, depth], w_gu[depth, :], preferred_element_type=jnp.float32
            )

        both = lax.fori_loop(0, size, more, jnp.zeros((block, 2 * LANES), jnp.float32))
        gate_value = both[:, :LANES]
        up_value = both[:, LANES:]
        hidden[...] = (gate_value / (1.0 + jnp.exp(-gate_value)) * up_value).astype(jnp.bfloat16)
        lanes = lax.broadcasted_iota(jnp.int32, (block, LANES), 1)
        scale = jnp.sum(jnp.where(lanes == me, coef_all[at, :], 0.0), axis=1, keepdims=True)

        @pl.loop(0, width // columns)
        def _(part):
            cols = pl.ds(pl.multiple_of(part * columns, columns), columns)
            value = lax.dot_general(
                hidden[...], w_d[cols, :], (((1,), (1,)), ((), ())),
                preferred_element_type=jnp.float32,
            )
            value = value.astype(jnp.bfloat16).astype(jnp.float32)
            contrib[at, cols] = (value * scale).astype(jnp.bfloat16)

        for row in range(2):
            owner = at_plane(plane_of[q], row * 2 + lax.rem(pair, 2))
            go(is_outer, send(
                contrib.at[token_rows(owner)], pair_in.at[plane_of[q], row],
                pair_send.at[plane_of[q], row], pair_recv.at[plane_of[q], row], beside,
            ))

    def add_rows(parts, target):
        @pl.loop(0, width // columns)
        def _(part):
            cols = pl.ds(pl.multiple_of(part * columns, columns), columns)
            total = sum(source(cols).astype(jnp.float32) for source in parts)
            target[:, cols] = total.astype(jnp.bfloat16)

    def chip_part(q, mine):
        owner_seat, row = (seat, my_row) if mine else (side, 1 - my_row)
        return [
            lambda cols: contrib[token_rows(at_plane(plane_of[q], owner_seat)), cols],
            lambda cols: pair_in[plane_of[q], row, :, cols],
        ]

    def taken(source, sem):
        landed(source, sem)
        return lambda cols: source[:, cols]

    def side_taken(q):
        return taken(side_in.at[plane_of[q]], side_recv.at[plane_of[q]])

    def chain_taken(q):
        return taken(chain_in.at[plane_of[q]], chain_recv.at[plane_of[q]])

    def over_taken(q):
        return taken(over_in.at[plane_of[q]], over_recv.at[plane_of[q]])

    def both_taken():
        return taken(both_in, both_recv)

    def pass_on(is_outer, q, parts):
        at = plane_of[q]
        add_rows(parts, chain_out.at[at])
        if is_outer:
            copy = send(chain_out.at[at], chain_in.at[at], chain_send.at[at], chain_recv.at[at], near_inner)
        elif q == O:
            copy = send(chain_out.at[at], chain_in.at[at], chain_send.at[at], chain_recv.at[at], near_outer)
        else:
            copy = send(chain_out.at[at], over_in.at[at], chain_send.at[at], over_recv.at[at], far_inner)
        go(is_outer, copy)

    def pass_both(is_outer, q):
        add_rows(chip_part(q, False), both_out)
        go(is_outer, send(both_out, both_in, both_send, both_recv, near_inner if is_outer else near_outer))

    def pair_add(is_outer, q):
        at = plane_of[q]
        for row in range(2):
            landed(pair_in.at[at, row], pair_recv.at[at, row])
        if (is_outer, q) == (True, I):
            pass_both(True, q)
            pass_on(True, q, chip_part(q, True))
            return
        if (is_outer, q) == (False, O):
            pass_both(False, q)
            return
        parts = chip_part(q, False)
        if q == (O if is_outer else I):
            parts = parts + [both_taken()]
        add_rows(parts, side_out.at[at])
        go(is_outer, send(side_out.at[at], side_in.at[at], side_send.at[at], side_recv.at[at], across))

    def side_add(is_outer, q):
        parts = chip_part(q, True)
        if is_outer or q != O:
            parts.append(side_taken(q))
        if not is_outer:
            parts.append(over_taken(q) if q == O else chain_taken(q))
        pass_on(is_outer, q, parts)

    def finish_rows(is_outer):
        q = O if is_outer else I
        parts = chip_part(q, True) + [side_taken(q), chain_taken(q)]
        if not is_outer:
            parts.append(over_taken(q))
        add_rows(parts, out)

    steps = (
        own_tokens, seat_tokens, side_tokens, spread, outer_in, inner_in, inner_out, outer_out,
        compute, pair_add, side_add, finish_rows,
    )

    for is_outer, role in ((True, outer), (False, inner)):

        @pl.when(role)
        def _():
            loaded = False
            for place, (name, *arguments) in enumerate(order[0 if is_outer else 1]):
                if name == COMPUTE and not loaded:
                    for load in loads:
                        load.wait()
                    loaded = True
                steps[name](is_outer, *arguments)
                if place == START_LOADS:
                    for load in loads:
                        load.start()
            for copy in sent[is_outer]:
                copy.wait_send()

    for chunk in range(count):
        left = gathered[chunk].at[pl.ds(0, size - 1)]
        landed(left, one_send.at[chunk])
        landed(left, three_send.at[chunk])

    for array in range(3):
        landed(moved[array].at[0], three_recv.at[array])


START_LOADS = 6
LINE_VMEM_BYTES = 59_000_000
LINE_ORDERS = {
    4: (
        ((1, 1, 2, 2, 2, 2, 2, 2, 2), (2, 2, 2, 2, 2, 2, 2, 2), (2, 2, 2, 2, 2, 2, 2, 1, 1)),
        (
            (
            (SPREAD, 0), (SPREAD, 1), (SPREAD, 2), (SPREAD, 3), (OWN,), (OUTER_IN, 0),
            (OUTER_IN, 1), (SPREAD, 4), (SEAT_TOKENS, I), (OUTER_IN, 2), (SPREAD, 5),
            (OUTER_IN, 3), (SPREAD, 6), (SPREAD, 7), (SIDE_TOKENS, I), (SIDE_TOKENS, O),
            (SPREAD, 8), (COMPUTE, I), (SPREAD, 9), (OUTER_IN, 4), (COMPUTE, O), (PAIR_ADD, I),
            (SEAT_TOKENS, J), (OUTER_IN, 5), (OUTER_IN, 6), (SEAT_TOKENS, K), (OUTER_IN, 7),
            (OUTER_OUT, 0), (OUTER_IN, 8), (OUTER_OUT, 1), (OUTER_IN, 9), (SPREAD, 10),
            (OUTER_OUT, 2), (SIDE_TOKENS, J), (COMPUTE, J), (SPREAD, 11), (SIDE_TOKENS, K),
            (OUTER_OUT, 3), (PAIR_ADD, J), (COMPUTE, K), (OUTER_IN, 10), (PAIR_ADD, O),
            (PAIR_ADD, K), (OUTER_IN, 11), (OUTER_OUT, 4), (SIDE_ADD, J), (SPREAD, 12),
            (OUTER_OUT, 5), (SPREAD, 13), (SIDE_ADD, K), (OUTER_OUT, 6), (SPREAD, 14),
            (OUTER_IN, 12), (OUTER_OUT, 7), (SPREAD, 15), (OUTER_IN, 13), (OUTER_OUT, 8),
            (SPREAD, 16), (OUTER_IN, 14), (OUTER_OUT, 9), (SPREAD, 17), (OUTER_IN, 15),
            (OUTER_OUT, 10), (SPREAD, 18), (OUTER_IN, 16), (OUTER_OUT, 11), (SPREAD, 19),
            (OUTER_IN, 17), (SPREAD, 20), (SPREAD, 21), (OUTER_IN, 18), (FINISH,), (SPREAD, 22),
            (SPREAD, 23), (OUTER_IN, 19), (OUTER_OUT, 12), (OUTER_IN, 20), (SPREAD, 24),
            (OUTER_IN, 21), (SPREAD, 25), (OUTER_OUT, 13), (OUTER_IN, 22), (OUTER_IN, 23),
            (OUTER_OUT, 14), (OUTER_IN, 24), (OUTER_IN, 25), (OUTER_OUT, 15), (OUTER_OUT, 16),
            (OUTER_OUT, 17), (OUTER_OUT, 18), (OUTER_OUT, 19), (OUTER_OUT, 20), (OUTER_OUT, 21),
            (OUTER_OUT, 22), (OUTER_OUT, 23), (OUTER_OUT, 24), (OUTER_OUT, 25),
            ),
            (
            (OWN,), (SPREAD, 0), (SPREAD, 1), (SPREAD, 2), (SPREAD, 3), (SPREAD, 4),
            (SIDE_TOKENS, I), (SEAT_TOKENS, J), (SEAT_TOKENS, O), (COMPUTE, I), (INNER_IN, 0),
            (INNER_IN, 1), (SPREAD, 5), (SEAT_TOKENS, K), (INNER_OUT, 0), (INNER_IN, 2),
            (INNER_OUT, 1), (SIDE_TOKENS, J), (INNER_IN, 3), (SPREAD, 6), (COMPUTE, J),
            (SPREAD, 7), (INNER_OUT, 2), (SIDE_TOKENS, O), (PAIR_ADD, J), (COMPUTE, O),
            (INNER_OUT, 3), (INNER_IN, 4), (SIDE_TOKENS, K), (PAIR_ADD, O), (COMPUTE, K),
            (PAIR_ADD, I), (PAIR_ADD, K), (INNER_OUT, 4), (INNER_IN, 5), (SPREAD, 8),
            (INNER_IN, 6), (SPREAD, 9), (INNER_OUT, 5), (INNER_IN, 7), (SPREAD, 10),
            (INNER_OUT, 6), (INNER_IN, 8), (SPREAD, 11), (INNER_OUT, 7), (INNER_IN, 9),
            (SPREAD, 12), (INNER_OUT, 8), (INNER_IN, 10), (SPREAD, 13), (INNER_OUT, 9),
            (INNER_IN, 11), (SPREAD, 14), (INNER_OUT, 10), (SIDE_ADD, J), (SPREAD, 15),
            (INNER_OUT, 11), (SIDE_ADD, K), (SPREAD, 16), (FINISH,), (SPREAD, 17), (INNER_IN, 12),
            (SPREAD, 18), (SIDE_ADD, O), (SPREAD, 19), (INNER_IN, 13), (SPREAD, 20),
            (INNER_OUT, 12), (INNER_IN, 14), (SPREAD, 21), (INNER_OUT, 13), (INNER_IN, 15),
            (SPREAD, 22), (INNER_OUT, 14), (INNER_IN, 16), (SPREAD, 23), (INNER_OUT, 15),
            (INNER_IN, 17), (SPREAD, 24), (SPREAD, 25), (INNER_OUT, 16), (INNER_IN, 18),
            (INNER_OUT, 17), (INNER_IN, 19), (INNER_OUT, 18), (INNER_IN, 20), (INNER_OUT, 19),
            (INNER_IN, 21), (INNER_OUT, 20), (INNER_IN, 22), (INNER_OUT, 21), (INNER_IN, 23),
            (INNER_IN, 24), (INNER_OUT, 22), (INNER_IN, 25), (INNER_OUT, 23), (INNER_OUT, 24),
            (INNER_OUT, 25),
            ),
        ),
    ),
    5: (
        ((1, 1, 2, 2, 2, 2, 2, 2, 2), (2, 2, 2, 2, 2, 2, 2, 2), (2, 2, 2, 2, 2, 2, 2, 1, 1)),
        (
            (
            (SPREAD, 0), (SPREAD, 1), (SPREAD, 2), (SPREAD, 3), (SPREAD, 4), (SPREAD, 5),
            (SPREAD, 6), (SPREAD, 7), (SPREAD, 8), (SPREAD, 9), (SPREAD, 10), (OWN,),
            (OUTER_IN, 0), (OUTER_IN, 1), (SPREAD, 11), (OUTER_IN, 2), (SEAT_TOKENS, I),
            (SPREAD, 12), (OUTER_IN, 3), (SPREAD, 13), (OUTER_IN, 4), (SPREAD, 14), (OUTER_IN, 5),
            (SEAT_TOKENS, J), (OUTER_IN, 6), (OUTER_IN, 7), (SPREAD, 15), (OUTER_IN, 8),
            (SEAT_TOKENS, K), (OUTER_IN, 9), (OUTER_OUT, 0), (OUTER_IN, 10), (OUTER_OUT, 1),
            (SPREAD, 16), (SIDE_TOKENS, O), (SPREAD, 17), (COMPUTE, O), (SPREAD, 18),
            (OUTER_OUT, 2), (OUTER_IN, 11), (OUTER_IN, 12), (OUTER_IN, 13), (SIDE_TOKENS, I),
            (SPREAD, 19), (OUTER_IN, 14), (COMPUTE, I), (SPREAD, 20), (OUTER_OUT, 3),
            (SIDE_TOKENS, J), (PAIR_ADD, I), (SPREAD, 21), (COMPUTE, J), (SPREAD, 22),
            (OUTER_OUT, 4), (OUTER_IN, 15), (PAIR_ADD, J), (SIDE_TOKENS, K), (OUTER_OUT, 5),
            (COMPUTE, K), (OUTER_IN, 16), (OUTER_OUT, 6), (PAIR_ADD, K), (OUTER_IN, 17),
            (OUTER_IN, 18), (OUTER_OUT, 7), (OUTER_IN, 19), (OUTER_IN, 20), (SPREAD, 23),
            (OUTER_OUT, 8), (OUTER_IN, 21), (SPREAD, 24), (OUTER_IN, 22), (SPREAD, 25),
            (PAIR_ADD, O), (OUTER_OUT, 9), (SIDE_ADD, J), (OUTER_OUT, 10), (OUTER_OUT, 11),
            (SIDE_ADD, K), (OUTER_OUT, 12), (OUTER_IN, 23), (OUTER_OUT, 13), (OUTER_IN, 24),
            (OUTER_IN, 25), (OUTER_OUT, 14), (OUTER_OUT, 15), (OUTER_OUT, 16), (OUTER_OUT, 17),
            (OUTER_OUT, 18), (OUTER_OUT, 19), (OUTER_OUT, 20), (OUTER_OUT, 21), (OUTER_OUT, 22),
            (FINISH,), (OUTER_OUT, 23), (OUTER_OUT, 24), (OUTER_OUT, 25),
            ),
            (
            (SPREAD, 0), (SPREAD, 1), (SPREAD, 2), (SPREAD, 3), (SPREAD, 4), (SPREAD, 5),
            (SPREAD, 6), (SPREAD, 7), (SPREAD, 8), (SPREAD, 9), (SPREAD, 10), (OWN,), (SPREAD, 11),
            (SEAT_TOKENS, O), (SEAT_TOKENS, J), (INNER_IN, 0), (INNER_IN, 1), (SPREAD, 12),
            (SEAT_TOKENS, K), (INNER_IN, 2), (INNER_OUT, 0), (INNER_OUT, 1), (INNER_IN, 3),
            (SPREAD, 13), (SPREAD, 14), (INNER_OUT, 2), (INNER_IN, 4), (SPREAD, 15),
            (SIDE_TOKENS, I), (INNER_IN, 5), (SPREAD, 16), (COMPUTE, I), (SPREAD, 17),
            (INNER_OUT, 3), (INNER_IN, 6), (SIDE_TOKENS, J), (INNER_OUT, 4), (COMPUTE, J),
            (INNER_IN, 7), (SPREAD, 18), (SPREAD, 19), (PAIR_ADD, J), (INNER_OUT, 5),
            (SIDE_TOKENS, K), (INNER_IN, 8), (COMPUTE, K), (INNER_OUT, 6), (INNER_IN, 9),
            (PAIR_ADD, K), (INNER_IN, 10), (INNER_OUT, 7), (SIDE_TOKENS, O), (COMPUTE, O),
            (SPREAD, 20), (INNER_OUT, 8), (INNER_IN, 11), (PAIR_ADD, O), (SPREAD, 21),
            (INNER_OUT, 9), (INNER_IN, 12), (SPREAD, 22), (INNER_OUT, 10), (INNER_IN, 13),
            (SPREAD, 23), (INNER_IN, 14), (SPREAD, 24), (INNER_OUT, 11), (SPREAD, 25),
            (PAIR_ADD, I), (INNER_OUT, 12), (INNER_OUT, 13), (INNER_IN, 15), (INNER_OUT, 14),
            (INNER_IN, 16), (INNER_IN, 17), (INNER_OUT, 15), (INNER_IN, 18), (INNER_OUT, 16),
            (INNER_IN, 19), (INNER_OUT, 17), (INNER_IN, 20), (INNER_OUT, 18), (INNER_IN, 21),
            (INNER_IN, 22), (INNER_OUT, 19), (SIDE_ADD, J), (INNER_OUT, 20), (SIDE_ADD, K),
            (INNER_OUT, 21), (INNER_IN, 23), (INNER_IN, 24), (INNER_OUT, 22), (INNER_IN, 25),
            (FINISH,), (SIDE_ADD, O), (INNER_OUT, 23), (INNER_OUT, 24), (INNER_OUT, 25),
            ),
        ),
    ),
    6: (
        ((1, 1, 2, 2, 2, 2, 2, 2, 2), (2, 2, 2, 2, 2, 2, 2, 2), (2, 2, 2, 2, 2, 2, 2, 1, 1)),
        (
            (
            (SPREAD, 0), (SPREAD, 1), (SPREAD, 2), (SPREAD, 3), (OWN,), (OUTER_IN, 0),
            (OUTER_IN, 1), (SPREAD, 4), (OUTER_IN, 2), (SEAT_TOKENS, I), (SPREAD, 5),
            (OUTER_IN, 3), (SPREAD, 6), (SPREAD, 7), (SEAT_TOKENS, J), (SIDE_TOKENS, O),
            (COMPUTE, O), (OUTER_IN, 4), (SIDE_TOKENS, I), (OUTER_IN, 5), (SPREAD, 8),
            (COMPUTE, I), (OUTER_IN, 6), (OUTER_IN, 7), (SPREAD, 9), (SEAT_TOKENS, K),
            (PAIR_ADD, I), (OUTER_OUT, 0), (OUTER_OUT, 1), (SIDE_TOKENS, J), (COMPUTE, J),
            (OUTER_IN, 8), (SPREAD, 10), (OUTER_IN, 9), (SPREAD, 11), (PAIR_ADD, J),
            (SIDE_TOKENS, K), (OUTER_OUT, 2), (COMPUTE, K), (OUTER_IN, 10), (PAIR_ADD, O),
            (PAIR_ADD, K), (OUTER_IN, 11), (OUTER_OUT, 3), (SIDE_ADD, J), (OUTER_OUT, 4),
            (OUTER_OUT, 5), (SPREAD, 12), (SIDE_ADD, K), (SPREAD, 13), (OUTER_OUT, 6),
            (SPREAD, 14), (SPREAD, 15), (OUTER_IN, 12), (OUTER_OUT, 7), (OUTER_IN, 13),
            (SPREAD, 16), (SPREAD, 17), (OUTER_IN, 14), (OUTER_OUT, 8), (OUTER_IN, 15),
            (SPREAD, 18), (SPREAD, 19), (OUTER_IN, 16), (OUTER_OUT, 9), (OUTER_IN, 17),
            (SPREAD, 20), (SPREAD, 21), (OUTER_IN, 18), (OUTER_OUT, 10), (OUTER_IN, 19),
            (SPREAD, 22), (SPREAD, 23), (OUTER_IN, 20), (OUTER_OUT, 11), (OUTER_IN, 21),
            (SPREAD, 24), (SPREAD, 25), (OUTER_IN, 22), (OUTER_IN, 23), (FINISH,), (OUTER_IN, 24),
            (OUTER_IN, 25), (OUTER_OUT, 12), (OUTER_OUT, 13), (OUTER_OUT, 14), (OUTER_OUT, 15),
            (OUTER_OUT, 16), (OUTER_OUT, 17), (OUTER_OUT, 18), (OUTER_OUT, 19), (OUTER_OUT, 20),
            (OUTER_OUT, 21), (OUTER_OUT, 22), (OUTER_OUT, 23), (OUTER_OUT, 24), (OUTER_OUT, 25),
            ),
            (
            (OWN,), (SPREAD, 0), (SPREAD, 1), (SPREAD, 2), (SPREAD, 3), (SPREAD, 4),
            (SEAT_TOKENS, J), (SIDE_TOKENS, I), (SEAT_TOKENS, O), (COMPUTE, I), (INNER_IN, 0),
            (INNER_IN, 1), (SPREAD, 5), (SEAT_TOKENS, K), (INNER_IN, 2), (INNER_OUT, 0),
            (SIDE_TOKENS, J), (INNER_OUT, 1), (INNER_IN, 3), (SPREAD, 6), (COMPUTE, J),
            (SPREAD, 7), (SIDE_TOKENS, O), (SPREAD, 8), (PAIR_ADD, J), (COMPUTE, O),
            (INNER_OUT, 2), (INNER_IN, 4), (SIDE_TOKENS, K), (PAIR_ADD, O), (COMPUTE, K),
            (INNER_OUT, 3), (INNER_IN, 5), (PAIR_ADD, K), (INNER_IN, 6), (INNER_OUT, 4),
            (INNER_IN, 7), (SPREAD, 9), (SPREAD, 10), (INNER_OUT, 5), (PAIR_ADD, I),
            (INNER_OUT, 6), (INNER_IN, 8), (SPREAD, 11), (SPREAD, 12), (INNER_OUT, 7),
            (INNER_IN, 9), (SPREAD, 13), (INNER_IN, 10), (SPREAD, 14), (INNER_OUT, 8),
            (INNER_IN, 11), (SPREAD, 15), (SPREAD, 16), (INNER_OUT, 9), (SIDE_ADD, J),
            (SPREAD, 17), (SIDE_ADD, K), (SPREAD, 18), (INNER_OUT, 10), (INNER_IN, 12),
            (SPREAD, 19), (SPREAD, 20), (INNER_OUT, 11), (INNER_IN, 13), (SPREAD, 21), (FINISH,),
            (INNER_IN, 14), (SPREAD, 22), (SPREAD, 23), (SIDE_ADD, O), (INNER_IN, 15),
            (SPREAD, 24), (SPREAD, 25), (INNER_IN, 16), (INNER_OUT, 12), (INNER_IN, 17),
            (INNER_OUT, 13), (INNER_IN, 18), (INNER_IN, 19), (INNER_OUT, 14), (INNER_IN, 20),
            (INNER_OUT, 15), (INNER_IN, 21), (INNER_IN, 22), (INNER_OUT, 16), (INNER_IN, 23),
            (INNER_IN, 24), (INNER_OUT, 17), (INNER_IN, 25), (INNER_OUT, 18), (INNER_OUT, 19),
            (INNER_OUT, 20), (INNER_OUT, 21), (INNER_OUT, 22), (INNER_OUT, 23), (INNER_OUT, 24),
            (INNER_OUT, 25),
            ),
        ),
    ),
    8: (
        ((1, 1, 2, 2, 2, 2, 2, 2, 2), (2, 2, 2, 2, 2, 2, 2, 2), (2, 2, 2, 2, 2, 2, 2, 1, 1)),
        (
            (
            (SPREAD, 0), (SPREAD, 1), (SPREAD, 2), (SPREAD, 3), (SPREAD, 4), (SPREAD, 5),
            (SPREAD, 6), (SPREAD, 7), (SPREAD, 8), (SPREAD, 9), (SPREAD, 10), (OWN,),
            (OUTER_IN, 0), (OUTER_IN, 1), (SPREAD, 11), (OUTER_IN, 2), (SEAT_TOKENS, I),
            (SPREAD, 12), (OUTER_IN, 3), (SPREAD, 13), (OUTER_IN, 4), (SPREAD, 14),
            (SIDE_TOKENS, I), (OUTER_IN, 5), (SPREAD, 15), (COMPUTE, I), (OUTER_IN, 6),
            (SPREAD, 16), (SEAT_TOKENS, J), (OUTER_IN, 7), (PAIR_ADD, I), (OUTER_IN, 8),
            (SEAT_TOKENS, K), (OUTER_IN, 9), (OUTER_OUT, 0), (OUTER_IN, 10), (OUTER_OUT, 1),
            (SIDE_TOKENS, O), (SPREAD, 17), (COMPUTE, O), (OUTER_IN, 11), (SPREAD, 18),
            (OUTER_IN, 12), (SPREAD, 19), (OUTER_IN, 13), (SPREAD, 20), (OUTER_IN, 14),
            (OUTER_OUT, 2), (OUTER_IN, 15), (SPREAD, 21), (OUTER_IN, 16), (SPREAD, 22),
            (SPREAD, 23), (SIDE_TOKENS, J), (OUTER_OUT, 3), (COMPUTE, J), (SPREAD, 24),
            (SIDE_TOKENS, K), (SPREAD, 25), (PAIR_ADD, J), (COMPUTE, K), (OUTER_IN, 17),
            (OUTER_OUT, 4), (PAIR_ADD, K), (OUTER_IN, 18), (OUTER_IN, 19), (OUTER_IN, 20),
            (OUTER_OUT, 5), (OUTER_IN, 21), (OUTER_IN, 22), (OUTER_IN, 23), (OUTER_IN, 24),
            (OUTER_IN, 25), (OUTER_OUT, 6), (SIDE_ADD, J), (PAIR_ADD, O), (OUTER_OUT, 7),
            (SIDE_ADD, K), (OUTER_OUT, 8), (OUTER_OUT, 9), (OUTER_OUT, 10), (OUTER_OUT, 11),
            (OUTER_OUT, 12), (OUTER_OUT, 13), (OUTER_OUT, 14), (OUTER_OUT, 15), (OUTER_OUT, 16),
            (OUTER_OUT, 17), (OUTER_OUT, 18), (OUTER_OUT, 19), (OUTER_OUT, 20), (OUTER_OUT, 21),
            (OUTER_OUT, 22), (OUTER_OUT, 23), (OUTER_OUT, 24), (OUTER_OUT, 25), (FINISH,),
            ),
            (
            (OWN,), (SPREAD, 0), (SPREAD, 1), (SPREAD, 2), (SPREAD, 3), (SPREAD, 4), (SPREAD, 5),
            (SPREAD, 6), (SPREAD, 7), (SPREAD, 8), (SPREAD, 9), (SPREAD, 10), (SPREAD, 11),
            (SIDE_TOKENS, I), (SEAT_TOKENS, J), (SEAT_TOKENS, O), (COMPUTE, I), (INNER_IN, 0),
            (INNER_IN, 1), (SPREAD, 12), (SEAT_TOKENS, K), (INNER_IN, 2), (INNER_OUT, 0),
            (SPREAD, 13), (INNER_IN, 3), (SPREAD, 14), (INNER_OUT, 1), (INNER_IN, 4), (SPREAD, 15),
            (SPREAD, 16), (INNER_IN, 5), (SPREAD, 17), (INNER_OUT, 2), (INNER_IN, 6), (SPREAD, 18),
            (SIDE_TOKENS, J), (SPREAD, 19), (COMPUTE, J), (INNER_IN, 7), (SPREAD, 20),
            (INNER_OUT, 3), (PAIR_ADD, J), (SIDE_TOKENS, K), (PAIR_ADD, I), (COMPUTE, K),
            (PAIR_ADD, K), (INNER_OUT, 4), (INNER_IN, 8), (INNER_IN, 9), (INNER_OUT, 5),
            (INNER_IN, 10), (SPREAD, 21), (SPREAD, 22), (SIDE_TOKENS, O), (SPREAD, 23),
            (COMPUTE, O), (SPREAD, 24), (SPREAD, 25), (INNER_OUT, 6), (INNER_IN, 11),
            (PAIR_ADD, O), (INNER_IN, 12), (INNER_OUT, 7), (INNER_IN, 13), (INNER_IN, 14),
            (INNER_OUT, 8), (INNER_IN, 15), (INNER_IN, 16), (INNER_OUT, 9), (INNER_IN, 17),
            (INNER_IN, 18), (INNER_OUT, 10), (INNER_IN, 19), (INNER_IN, 20), (INNER_OUT, 11),
            (INNER_IN, 21), (INNER_IN, 22), (INNER_OUT, 12), (INNER_IN, 23), (INNER_IN, 24),
            (INNER_IN, 25), (INNER_OUT, 13), (SIDE_ADD, J), (SIDE_ADD, K), (INNER_OUT, 14),
            (INNER_OUT, 15), (INNER_OUT, 16), (INNER_OUT, 17), (INNER_OUT, 18), (INNER_OUT, 19),
            (INNER_OUT, 20), (INNER_OUT, 21), (INNER_OUT, 22), (INNER_OUT, 23), (INNER_OUT, 24),
            (INNER_OUT, 25), (FINISH,), (SIDE_ADD, O),
            ),
        ),
    ),
}


def call_line(n, most, which, table, tokens, coef, held_gate, held_up, held_down):
    rows, width = tokens.shape
    size = 4
    planes = n // size
    quarter = width // size
    cuts, order = LINE_ORDERS[most]
    plan = chunk_plan(quarter, cuts)
    count = len(plan)
    vmem = pl.BlockSpec(memory_space=pltpu.VMEM)
    anywhere = pl.BlockSpec(memory_space=pl.ANY)
    dma = pltpu.SemaphoreType.DMA
    moved_shape = jax.ShapeDtypeStruct(held_gate.shape, held_gate.dtype)

    def block(*shape):
        return pltpu.VMEM(shape, jnp.bfloat16)

    return pl.pallas_call(
        functools.partial(line_kernel, n, most, plan, order),
        out_shape=(jax.ShapeDtypeStruct((rows, width), jnp.bfloat16),) + (moved_shape,) * 3,
        in_specs=[pl.BlockSpec(memory_space=pltpu.SMEM), vmem, vmem] + [anywhere] * 3,
        out_specs=(vmem, anywhere, anywhere, anywhere),
        scratch_shapes=[
            *(block(2 * size, length, LANES) for _, _, length in plan),
            *(block(most, length, LANES) for _, _, length in plan),
            block(most, 3 * quarter, LANES),
            block(2 * size, 3 * quarter, LANES),
            block(n * rows, width),
            pltpu.VMEM((n * rows, LANES), jnp.float32),
            block(width, 2 * LANES),
            block(width, LANES),
            block(size * rows, LANES),
            block(n * rows, width),
            block(planes, 2, rows, width),
            block(planes, rows, width),
            block(planes, rows, width),
            block(planes, rows, width),
            block(planes, rows, width),
            block(planes, rows, width),
            block(rows, width),
            block(rows, width),
            dma((3,)),
            dma((2, planes, 6)),
            dma((2, n)),
            dma((count,)),
            dma((count,)),
            dma((count,)),
            dma((count,)),
            dma((count,)),
            dma((count,)),
            dma((count,)),
            dma((count,)),
            dma((count,)),
            dma((3,)),
            dma((planes, 2)),
            dma((planes, 2)),
            dma((planes,)),
            dma((planes,)),
            dma((planes,)),
            dma((planes,)),
            dma((planes,)),
            dma,
            dma,
        ],
        compiler_params=pltpu.CompilerParams(
            collective_id=which, has_side_effects=True, vmem_limit_bytes=LINE_VMEM_BYTES
        ),
    )(table, tokens, coef, held_gate, held_up, held_down)


def plan_kernel(n, levels, old, new, ids, logits, table, level, coef, target):
    half = n // 2
    blocks = n // EXPERTS
    rows = coef.shape[0]

    @pl.loop(0, n)
    def _(slot):
        target[old[slot]] = new[slot]

    @pl.loop(0, half)
    def _(place):
        table[place] = 0
        table[half + place] = 0

    crossing = jnp.int32(0)
    for side in range(2):

        def place_one(lane, turn):
            goes_to = target[side * half + lane]
            crosses = ((goes_to >= half).astype(jnp.int32) + side) % 2

            @pl.when(crosses == 1)
            def _():
                table[side * half + turn] = lane

            table[n + goes_to] = crosses
            table[2 * n + goes_to] = (1 - crosses) * lane
            table[3 * n + goes_to] = crosses * turn
            return turn + crosses

        crossing = lax.fori_loop(0, half, place_one, jnp.int32(0))
    level[0] = sum((crossing > most).astype(jnp.int32) for most in levels[:-1])

    lanes = lax.broadcasted_iota(jnp.int32, (rows, LANES), 1)
    expert_at = jnp.full((rows, LANES), -1, jnp.int32)
    for slot in range(n):
        expert_at = jnp.where(lanes == old[slot], slot // blocks, expert_at)
    eye = lax.broadcasted_iota(jnp.int32, (rows, rows), 0) == lax.broadcasted_iota(
        jnp.int32, (rows, rows), 1
    )

    def column(ref, row):
        return jnp.sum(jnp.where(eye, ref[row : row + 1, :], 0), axis=1, keepdims=True)

    first, second = column(logits, 0), column(logits, 1)
    first_weight = 1.0 / (1.0 + jnp.exp(second - first))
    second_weight = 1.0 / (1.0 + jnp.exp(first - second))
    total = jnp.where(column(ids, 0) == expert_at, first_weight, 0.0)
    coef[...] = total + jnp.where(column(ids, 1) == expert_at, second_weight, 0.0)


def write_kernel(*refs):
    sources, targets, held, sems, held_sems = refs[:4], refs[4:8], refs[8], refs[9], refs[10]
    parts = held_sems.shape[0]
    length = held.shape[0] // parts
    copies = [
        pltpu.make_async_copy(source, target, sems.at[at])
        for at, (source, target) in enumerate(zip(sources[:3], targets[:3]))
    ]
    taken, given = [], []
    for part in range(parts):
        at = pl.ds(part * length, length)
        taken.append(pltpu.make_async_copy(sources[3].at[0, at], held.at[at], held_sems.at[part, 0]))
        given.append(pltpu.make_async_copy(held.at[at], targets[3].at[0, at], held_sems.at[part, 1]))
    for copy in taken + copies:
        copy.start()
    for first, second in zip(taken, given):
        first.wait()
        second.start()
    for copy in copies + given:
        copy.wait()


def line_layer(
    tokens, route_ids, route_logits, old_place, new_place, held_gate, held_up, held_down
):
    n = lax.axis_size("expert")
    levels = sorted(LINE_ORDERS)
    rows = tokens.shape[0]
    smem = pl.BlockSpec(memory_space=pltpu.SMEM)
    vmem = pl.BlockSpec(memory_space=pltpu.VMEM)
    table, level, coef = pl.pallas_call(
        functools.partial(plan_kernel, n, levels),
        out_shape=(
            jax.ShapeDtypeStruct((4 * n,), jnp.int32),
            jax.ShapeDtypeStruct((1,), jnp.int32),
            jax.ShapeDtypeStruct((rows, LANES), jnp.float32),
        ),
        in_specs=[smem, smem, vmem, vmem],
        out_specs=(smem, smem, vmem),
        scratch_shapes=[pltpu.SMEM((n,), jnp.int32)],
    )(old_place, new_place, route_ids.T, route_logits.T)
    branches = [functools.partial(call_line, n, most, i) for i, most in enumerate(levels)]
    results = lax.switch(level[0], branches, table, tokens, coef, held_gate, held_up, held_down)
    anywhere = pl.BlockSpec(memory_space=pl.ANY)
    return pl.pallas_call(
        write_kernel,
        out_shape=tuple(jax.ShapeDtypeStruct(array.shape, array.dtype) for array in results),
        in_specs=[anywhere] * 4,
        out_specs=(anywhere,) * 4,
        scratch_shapes=[
            pltpu.VMEM(held_down.shape[1:], held_down.dtype),
            pltpu.SemaphoreType.DMA((3,)),
            pltpu.SemaphoreType.DMA((4, 2)),
        ],
    )(*results)


def per_device(
    tokens, route_ids, route_logits, old_place, new_place, held_gate, held_up, held_down
):
    n = lax.axis_size("expert")
    if n == 16 and tokens.shape[1] % 512 == 0:
        return line_layer(
            tokens, route_ids, route_logits, old_place, new_place, held_gate, held_up, held_down
        )
    half = n // 2
    device_ids = jnp.arange(n, dtype=jnp.int32)
    blocks = n // EXPERTS
    at_old = (old_place[:, None] == device_ids[None, :]).astype(jnp.int32)
    dest_of = jnp.sum(at_old * new_place[:, None], axis=0)
    expert_at = jnp.sum(at_old * device_ids[:, None], axis=0) // blocks
    half_of = device_ids // half
    crosses = (dest_of // half != half_of).astype(jnp.int32)
    earlier = (half_of[:, None] == half_of[None, :]) & (device_ids[:, None] < device_ids[None, :])
    turn = jnp.sum(earlier.astype(jnp.int32) * crosses[:, None], axis=0)
    lane_of = device_ids - half_of * half
    leaving = (half_of[:, None] * half + turn[:, None] == device_ids[None, :]).astype(jnp.int32)
    leaving = jnp.sum(leaving * (crosses * lane_of)[:, None], axis=0)
    arriving = (dest_of[:, None] == device_ids[None, :]).astype(jnp.int32)
    table = jnp.concatenate([
        leaving,
        jnp.sum(arriving * crosses[:, None], axis=0),
        jnp.sum(arriving * ((1 - crosses) * lane_of)[:, None], axis=0),
        jnp.sum(arriving * (crosses * turn)[:, None], axis=0),
    ])
    first_weight = 1.0 / (1.0 + jnp.exp(route_logits[:, 1] - route_logits[:, 0]))
    second_weight = 1.0 / (1.0 + jnp.exp(route_logits[:, 0] - route_logits[:, 1]))
    coef = jnp.where(route_ids[:, 0:1] == expert_at[None, :], first_weight[:, None], 0.0)
    coef = coef + jnp.where(route_ids[:, 1:2] == expert_at[None, :], second_weight[:, None], 0.0)
    coef = jnp.pad(coef, ((0, 0), (0, LANES - n)))
    table, coef = lax.optimization_barrier((table, coef))
    levels = sorted({max(1, half * eighths // 8) for eighths in (3, 4, 5, 6, 8)})
    crossing = jnp.sum(crosses) // 2
    level = sum((crossing > most).astype(jnp.int32) for most in levels[:-1])
    branches = [functools.partial(call_layer, n, most, i) for i, most in enumerate(levels)]
    return lax.switch(level, branches, table, tokens, coef, held_gate, held_up, held_down)


def solution(mesh):
    split = ("groups", "expert")
    placed = (
        P(split, None),
        P(split, None),
        P(split, None),
        P(),
        P(),
        P(split, None, None),
        P(split, None, None),
        P(split, None, None),
    )
    return jax.shard_map(
        per_device,
        mesh=mesh,
        in_specs=placed,
        out_specs=(
            P(split, None),
            P(split, None, None),
            P(split, None, None),
            P(split, None, None),
        ),
        check_vma=False,
    )
```

```python
import functools

import jax
import jax.numpy as jnp
from jax import lax
from jax.experimental import pallas as pl
from jax.experimental.pallas import tpu as pltpu
from jax.sharding import PartitionSpec as P

EXPERTS = 8
LANES = 128
MESH = pl.DeviceIdType.MESH
VMEM_BYTES = 63_000_000


def near_square_root(n):
    size = 1
    while size * size < n:
        size *= 2
    return size


def layer_kernel(
    n,
    most,
    table,
    tok,
    coef,
    held_g,
    held_u,
    held_d,
    out,
    moved_g,
    moved_u,
    moved_d,
    tok_all,
    coef_all,
    w_gu,
    w_d,
    pieces_g,
    pieces_u,
    pieces_d,
    crossed_g,
    crossed_u,
    crossed_d,
    ordered,
    hidden,
    contrib,
    part_in,
    plane_sum,
    half_in,
    cross_out,
    cross_in,
    load_sem,
    tok_send,
    fwd_send,
    plane_send,
    tok_recv,
    one_send,
    one_recv,
    two_send,
    two_recv,
    three_send,
    three_recv,
    part_send,
    part_recv,
    half_send,
    half_recv,
    cross_send,
    cross_recv,
):
    me = lax.axis_index("expert")
    half = n // 2
    base = (me // half) * half
    lane = me - base
    twin = lax.rem(me + half, n)
    rows, width = tok.shape
    band = width // half
    size = near_square_root(n)
    planes = n // size
    half_planes = planes // 2
    plane = me // size
    seat = me - plane * size
    my_plane_of_half = lane // size
    held = (held_g, held_u, held_d)
    moved = (moved_g, moved_u, moved_d)
    pieces = (pieces_g, pieces_u, pieces_d)
    crossed = (crossed_g, crossed_u, crossed_d)

    barrier = pltpu.get_barrier_semaphore()

    @pl.loop(1, n)
    def _(k):
        pl.semaphore_signal(
            barrier, inc=1, device_id={"expert": lax.rem(me + k, n)}, device_id_type=MESH
        )

    loads = (
        pltpu.make_async_copy(held_g.at[0], w_gu.at[:, pl.ds(0, LANES)], load_sem.at[0]),
        pltpu.make_async_copy(held_u.at[0], w_gu.at[:, pl.ds(LANES, LANES)], load_sem.at[1]),
        pltpu.make_async_copy(held_d.at[0], w_d, load_sem.at[2]),
    )
    for load in loads:
        load.start()

    def token_rows(owner):
        return pl.ds(pl.multiple_of(owner * rows, rows), rows)

    def band_rows(owner):
        return pl.ds(pl.multiple_of(owner * band, band), band)

    def near(k):
        return base + lax.rem(lane + k, half)

    def column(k):
        return base + lax.rem(lane + k * size, half)

    def mate(k):
        return plane * size + lax.rem(seat + k, size)

    def seated(other_plane):
        return other_plane * size + seat

    tok_all[token_rows(me), :] = tok[...]
    coef_all[token_rows(me), :] = coef[...]
    pl.semaphore_wait(barrier, n - 1)

    def send(source, target, send_sem, recv_sem, peer):
        return pltpu.make_async_remote_copy(
            src_ref=source, dst_ref=target, send_sem=send_sem, recv_sem=recv_sem,
            device_id={"expert": peer}, device_id_type=MESH,
        )

    def own_tokens(peer):
        at = token_rows(me)
        return (
            send(tok, tok_all.at[at], tok_send.at[0, peer], tok_recv.at[0, me], peer),
            send(coef, coef_all.at[at], tok_send.at[1, peer], tok_recv.at[1, me], peer),
        )

    def passed_tokens(owner, peer, sems):
        at = token_rows(owner)
        return (
            send(tok_all.at[at], tok_all.at[at], sems[0], tok_recv.at[0, owner], peer),
            send(coef_all.at[at], coef_all.at[at], sems[1], tok_recv.at[1, owner], peer),
        )

    def twin_tokens(peer):
        return passed_tokens(twin, peer, (fwd_send.at[0, peer], fwd_send.at[1, peer]))

    def plane_tokens(other_plane, k):
        sems = (plane_send.at[0, other_plane, k], plane_send.at[1, other_plane, k])
        return passed_tokens(seated(other_plane), mate(k), sems)

    def tokens_arrive(owner):
        pltpu.make_async_copy(tok, tok_all.at[token_rows(owner)], tok_recv.at[0, owner]).wait()
        pltpu.make_async_copy(coef, coef_all.at[token_rows(owner)], tok_recv.at[1, owner]).wait()

    def spread(array):
        pltpu.make_async_copy(
            held[array].at[0, band_rows(lane)], pieces[array].at[lane], one_recv.at[array]
        ).start()

        @pl.loop(1, half)
        def _(k):
            peer = near(k)
            send(
                held[array].at[0, band_rows(peer - base)], pieces[array].at[lane],
                one_send.at[array], one_recv.at[array], peer,
            ).start()

    def swap(array):
        return send(
            ordered.at[array, pl.ds(0, most)], crossed[array],
            two_send.at[array], two_recv.at[array], twin,
        )

    def cross_over(array):
        pltpu.make_async_copy(pieces[array], pieces[array], one_recv.at[array]).wait()

        @pl.loop(0, most)
        def _(m):
            ordered[array, m] = pieces[array][table[base + m]]

        swap(array).start()

    def deliver(array):
        swap(array).wait()

        @pl.loop(0, half)
        def _(place):
            at = base + place
            own = pieces[array][table[2 * n + at]]
            other = crossed[array][table[3 * n + at]]
            ordered[array, place] = jnp.where(table[n + at] == 1, other, own)

        pltpu.make_async_copy(
            ordered.at[array, lane], moved[array].at[0, band_rows(lane)], three_recv.at[array]
        ).start()

        @pl.loop(1, half)
        def _(k):
            peer = near(k)
            send(
                ordered.at[array, peer - base], moved[array].at[0, band_rows(lane)],
                three_send.at[array], three_recv.at[array], peer,
            ).start()

    for copy in own_tokens(twin):
        copy.start()

    @pl.loop(1, half_planes)
    def _(k):
        for copy in own_tokens(column(k)):
            copy.start()

    @pl.loop(1, size)
    def _(k):
        for copy in own_tokens(mate(k)):
            copy.start()

    spread(0)
    tokens_arrive(twin)

    @pl.loop(1, half_planes)
    def _(k):
        for copy in twin_tokens(column(k)):
            copy.start()

    spread(1)

    @pl.loop(1, half_planes)
    def _(k):
        tokens_arrive(column(k))
        tokens_arrive(lax.rem(column(k) + half, n))

    @pl.loop(1, planes)
    def _(shift):
        @pl.loop(1, size)
        def _(k):
            for copy in plane_tokens(lax.rem(plane + shift, planes), k):
                copy.start()

    spread(2)
    cross_over(0)
    cross_over(1)

    @pl.loop(0, planes)
    def _(other_plane):
        @pl.loop(1, size)
        def _(k):
            tokens_arrive(other_plane * size + lax.rem(seat + k, size))

    for load in loads:
        load.wait()

    step = min(256, n * rows)
    columns = 512

    @pl.loop(0, n * rows // step)
    def _(block):
        at = pl.ds(pl.multiple_of(block * step, step), step)
        both = jnp.dot(tok_all[at, :], w_gu[...], preferred_element_type=jnp.float32)
        gate_value = both[:, :LANES]
        up_value = both[:, LANES:]
        hidden[...] = (gate_value / (1.0 + jnp.exp(-gate_value)) * up_value).astype(jnp.bfloat16)
        lanes = lax.broadcasted_iota(jnp.int32, (step, LANES), 1)
        scale = jnp.sum(jnp.where(lanes == me, coef_all[at, :], 0.0), axis=1, keepdims=True)

        @pl.loop(0, width // columns)
        def _(part):
            cols = pl.ds(pl.multiple_of(part * columns, columns), columns)
            value = lax.dot_general(
                hidden[...], w_d[cols, :], (((1,), (1,)), ((), ())),
                preferred_element_type=jnp.float32,
            )
            value = value.astype(jnp.bfloat16).astype(jnp.float32)
            contrib[at, cols] = (value * scale).astype(jnp.bfloat16)

    def part_copy(k, other_plane):
        peer = mate(k)
        owner = other_plane * size + lax.rem(seat + k, size)
        return send(
            contrib.at[token_rows(owner)], part_in.at[seat, other_plane],
            part_send.at[k, other_plane], part_recv.at[seat, other_plane], peer,
        )

    def half_copy(k, kind):
        peer = column(k)
        target = peer // size if kind == 0 else lax.rem(peer // size + half_planes, planes)
        return send(
            plane_sum.at[target], half_in.at[kind, my_plane_of_half],
            half_send.at[kind, k], half_recv.at[kind, my_plane_of_half], peer,
        )

    @pl.loop(0, planes)
    def _(other_plane):
        @pl.loop(1, size)
        def _(k):
            part_copy(k, other_plane).start()

    def add_plane():
        @pl.loop(0, planes)
        def _(other_plane):
            @pl.loop(1, size)
            def _(k):
                spot = part_in.at[lax.rem(seat + k, size), other_plane]
                pltpu.make_async_copy(
                    spot, spot, part_recv.at[lax.rem(seat + k, size), other_plane]
                ).wait()

            @pl.loop(0, width // columns)
            def _(part):
                cols = pl.ds(pl.multiple_of(part * columns, columns), columns)

                def more(k, total):
                    other = lax.rem(seat + k, size)
                    return total + part_in[other, other_plane, :, cols].astype(jnp.float32)

                total = contrib[token_rows(seated(other_plane)), cols].astype(jnp.float32)
                total = lax.fori_loop(1, size, more, total)
                plane_sum[other_plane, :, cols] = total.astype(jnp.bfloat16)

        for kind in (1, 0):

            @pl.loop(1, half_planes)
            def _(k):
                half_copy(k, kind).start()

    def add_half(kind, own_plane, extra, target):
        @pl.loop(1, half_planes)
        def _(k):
            other = lax.rem(my_plane_of_half + k, half_planes)
            spot = half_in.at[kind, other]
            pltpu.make_async_copy(spot, spot, half_recv.at[kind, other]).wait()

        @pl.loop(0, width // columns)
        def _(part):
            cols = pl.ds(pl.multiple_of(part * columns, columns), columns)

            def more(k, total):
                other = lax.rem(my_plane_of_half + k, half_planes)
                return total + half_in[kind, other, :, cols].astype(jnp.float32)

            total = plane_sum[own_plane, :, cols].astype(jnp.float32)
            if extra is not None:
                total = total + extra[:, cols].astype(jnp.float32)
            target[:, cols] = lax.fori_loop(1, half_planes, more, total).astype(jnp.bfloat16)

    deliver(0)
    cross_over(2)
    add_plane()
    deliver(1)
    add_half(1, lax.rem(plane + half_planes, planes), None, cross_out)
    cross = send(cross_out, cross_in, cross_send, cross_recv, twin)
    cross.start()
    deliver(2)
    cross.wait()
    add_half(0, plane, cross_in, out)

    for copy in own_tokens(twin):
        copy.wait_send()

    @pl.loop(1, half_planes)
    def _(k):
        for copy in own_tokens(column(k)):
            copy.wait_send()
        for copy in twin_tokens(column(k)):
            copy.wait_send()
        half_copy(k, 0).wait_send()
        half_copy(k, 1).wait_send()

    @pl.loop(1, size)
    def _(k):
        for copy in own_tokens(mate(k)):
            copy.wait_send()

        @pl.loop(0, planes)
        def _(other_plane):
            part_copy(k, other_plane).wait_send()

        @pl.loop(1, planes)
        def _(shift):
            for copy in plane_tokens(lax.rem(plane + shift, planes), k):
                copy.wait_send()

    for array in range(3):
        sent = pieces[array].at[pl.ds(0, half - 1)]
        pltpu.make_async_copy(sent, sent, one_send.at[array]).wait()
        pltpu.make_async_copy(sent, sent, three_send.at[array]).wait()
        pltpu.make_async_copy(
            moved[array].at[0], moved[array].at[0], three_recv.at[array]
        ).wait()


def call_layer(n, most, which, table, tokens, coef, held_gate, held_up, held_down):
    rows, width = tokens.shape
    half = n // 2
    band = width // half
    size = near_square_root(n)
    planes = n // size
    vmem = pl.BlockSpec(memory_space=pltpu.VMEM)
    anywhere = pl.BlockSpec(memory_space=pl.ANY)
    dma = pltpu.SemaphoreType.DMA
    moved_shape = jax.ShapeDtypeStruct(held_gate.shape, held_gate.dtype)

    def block(*shape):
        return pltpu.VMEM(shape, jnp.bfloat16)

    return pl.pallas_call(
        functools.partial(layer_kernel, n, most),
        out_shape=(jax.ShapeDtypeStruct((rows, width), jnp.bfloat16),) + (moved_shape,) * 3,
        in_specs=[pl.BlockSpec(memory_space=pltpu.SMEM), vmem, vmem] + [anywhere] * 3,
        out_specs=(vmem, anywhere, anywhere, anywhere),
        scratch_shapes=[
            block(n * rows, width),
            pltpu.VMEM((n * rows, LANES), jnp.float32),
            block(width, 2 * LANES),
            block(width, LANES),
            block(half, band, LANES),
            block(half, band, LANES),
            block(half, band, LANES),
            block(most, band, LANES),
            block(most, band, LANES),
            block(most, band, LANES),
            block(3, half, band, LANES),
            block(min(256, n * rows), LANES),
            block(n * rows, width),
            block(size, planes, rows, width),
            block(planes, rows, width),
            block(2, planes // 2, rows, width),
            block(rows, width),
            block(rows, width),
            dma((3,)),
            dma((2, n)),
            dma((2, n)),
            dma((2, planes, size)),
            dma((2, n)),
            dma((3,)),
            dma((3,)),
            dma((3,)),
            dma((3,)),
            dma((3,)),
            dma((3,)),
            dma((size, planes)),
            dma((size, planes)),
            dma((2, planes // 2)),
            dma((2, planes // 2)),
            dma,
            dma,
        ],
        compiler_params=pltpu.CompilerParams(
            collective_id=which, has_side_effects=True, vmem_limit_bytes=VMEM_BYTES
        ),
    )(table, tokens, coef, held_gate, held_up, held_down)


O, I, J, K = range(4)
(
    OWN, SEAT_TOKENS, SIDE_TOKENS, SPREAD, OUTER_IN, INNER_IN, INNER_OUT, OUTER_OUT,
    COMPUTE, PAIR_ADD, SIDE_ADD, FINISH,
) = range(12)


def chunk_plan(quarter, cuts):
    plan = []
    for array in range(3):
        start = 0
        for cut in cuts[array]:
            size = quarter * cut // 16
            plan.append((array, start, size))
            start += size
        assert start == quarter
    return tuple(plan)


def line_kernel(
    n, most, plan, order, table, tok, coef, held_g, held_u, held_d, out, moved_g, moved_u, moved_d, *rest
):
    count = len(plan)
    gathered, rest = rest[:count], rest[count:]
    crossed, rest = rest[:count], rest[count:]
    (
        leaving, ordered, tok_all, coef_all, w_gu, w_d, hidden, contrib,
        pair_in, side_out, side_in, chain_in, chain_out, over_in, both_in, both_out,
        load_sem, tok_send, tok_recv,
        one_send, one_recv, two_send, two_recv, cross_send, cross_recv,
        back_send, back_recv, three_send, three_recv,
        pair_send, pair_recv, side_send, side_recv, chain_send, chain_recv,
        over_recv, both_send, both_recv,
    ) = rest
    size = 4
    last = n // size - 1
    me = lax.axis_index("expert")
    plane = me // size
    seat = me - plane * size
    half = plane // 2
    base = half * (n // 2)
    own_at = lax.rem(plane, 2) * size
    other_at = size - own_at
    inner = (plane == 1) | (plane == 2)
    outer = (plane == 0) | (plane == last)
    side = lax.rem(seat + 2, size)
    pair = seat + 1 - 2 * lax.rem(seat, 2)
    diagonal = lax.rem(pair + 2, size)
    my_row = seat // 2
    rows, width = tok.shape
    quarter = width // size
    held = (held_g, held_u, held_d)
    moved = (moved_g, moved_u, moved_d)
    plane_of = (last * half, 1 + half, last - 1 - half, last - last * half)

    def at_plane(other, other_seat):
        return other * size + other_seat

    near_outer, near_inner = at_plane(plane_of[O], seat), at_plane(plane_of[I], seat)
    far_inner = at_plane(plane_of[J], seat)
    beside, across = at_plane(plane, pair), at_plane(plane, side)

    def token_rows(owner):
        return pl.ds(pl.multiple_of(owner * rows, rows), rows)

    own_load = pltpu.make_async_copy(tok, tok_all.at[token_rows(me)], load_sem.at[3])
    own_load.start()
    barrier = pltpu.get_barrier_semaphore()

    def greet(peer):
        pl.semaphore_signal(barrier, inc=1, device_id={"expert": peer}, device_id_type=MESH)

    @pl.loop(1, size)
    def _(k):
        greet(at_plane(plane, lax.rem(seat + k, size)))

    @pl.when(outer)
    def _():
        greet(near_inner)

    @pl.when(inner)
    def _():
        greet(near_outer)
        greet(far_inner)

    loads = (
        pltpu.make_async_copy(held_g.at[0], w_gu.at[:, pl.ds(0, LANES)], load_sem.at[0]),
        pltpu.make_async_copy(held_u.at[0], w_gu.at[:, pl.ds(LANES, LANES)], load_sem.at[1]),
        pltpu.make_async_copy(held_d.at[0], w_d, load_sem.at[2]),
    )

    coef_all[token_rows(me), :] = coef[...]

    @pl.when(inner)
    def _():
        pl.semaphore_wait(barrier, size + 1)

    @pl.when(outer)
    def _():
        pl.semaphore_wait(barrier, size)

    def send(source, target, send_sem, recv_sem, peer):
        return pltpu.make_async_remote_copy(
            src_ref=source, dst_ref=target, send_sem=send_sem, recv_sem=recv_sem,
            device_id={"expert": peer}, device_id_type=MESH,
        )

    def landed(spot, sem):
        pltpu.make_async_copy(spot, spot, sem).wait()

    sent = {True: [], False: []}

    def go(role, *copies):
        for copy in copies:
            copy.start()
        sent[role].extend(copies)

    def tokens_to(q, owner_seat, peer, path, own=False):
        owner_plane = plane_of[q]
        owner = at_plane(owner_plane, owner_seat)
        at = token_rows(owner)
        coef_source = coef if own else coef_all.at[at]
        return (
            send(tok_all.at[at], tok_all.at[at], tok_send.at[0, owner_plane, path], tok_recv.at[0, owner], peer),
            send(coef_source, coef_all.at[at], tok_send.at[1, owner_plane, path], tok_recv.at[1, owner], peer),
        )

    def tokens_arrive(q, owner_seat):
        owner = at_plane(plane_of[q], owner_seat)
        landed(tok_all.at[token_rows(owner)], tok_recv.at[0, owner])
        landed(coef_all.at[token_rows(owner)], tok_recv.at[1, owner])

    def own_tokens(is_outer):
        own_load.wait()
        if is_outer:
            go(True, *tokens_to(O, seat, near_inner, 0, True))
        else:
            go(False, *tokens_to(I, seat, near_outer, 0, True))
            go(False, *tokens_to(I, seat, far_inner, 1, True))
        mine = O if is_outer else I
        go(is_outer, *tokens_to(mine, seat, across, 2, True))
        go(is_outer, *tokens_to(mine, seat, beside, 3, True))

    def seat_tokens(is_outer, q):
        tokens_arrive(q, seat)
        if not is_outer:
            if q == O:
                go(False, *tokens_to(q, seat, far_inner, 1))
            else:
                go(False, *tokens_to(q, seat, near_outer, 0))
        if (is_outer, q) not in ((True, I), (False, O)):
            go(is_outer, *tokens_to(q, seat, across, 2))
        go(is_outer, *tokens_to(q, seat, beside, 3))

    def side_tokens(is_outer, q):
        tokens_arrive(q, side)
        if (is_outer, q) == (True, O):
            go(True, *tokens_to(q, side, near_inner, 5))
        if (is_outer, q) == (False, I):
            go(False, *tokens_to(q, side, near_outer, 5))
        go(is_outer, *tokens_to(q, side, beside, 4))

    def band(chunk, owner):
        _, first, length = plan[chunk]
        return pl.ds(pl.multiple_of(owner * quarter + first, 16), length)

    def spread(is_outer, chunk):
        array = plan[chunk][0]
        spot = gathered[chunk].at[own_at + seat]
        pltpu.make_async_copy(held[array].at[0, band(chunk, seat)], spot, one_recv.at[chunk]).start()
        for k in (2, 1, 3):
            peer = lax.rem(seat + k, size)
            send(
                held[array].at[0, band(chunk, peer)], spot, one_send.at[chunk],
                one_recv.at[chunk], at_plane(plane, peer),
            ).start()

    def own_part(chunk):
        return gathered[chunk].at[pl.ds(own_at, size)]

    def other_part(chunk):
        return gathered[chunk].at[pl.ds(other_at, size)]

    def flat_at(chunk):
        return pl.ds(sum(length for _, _, length in plan[:chunk]), plan[chunk][2])

    def deliver(chunk, piece_of):
        array = plan[chunk][0]
        target = moved[array].at[0, band(chunk, seat)]
        for k in (2, 1, 3):
            peer = lax.rem(seat + k, size)
            send(
                piece_of(peer), target, three_send.at[chunk], three_recv.at[array],
                at_plane(plane, peer),
            ).start()
        pltpu.make_async_copy(piece_of(seat), target, three_recv.at[array]).start()

    def outer_in(is_outer, chunk):
        landed(own_part(chunk), one_recv.at[chunk])
        go(True, send(
            own_part(chunk), own_part(chunk), two_send.at[chunk], two_recv.at[chunk], near_inner
        ))

    def inner_in(is_outer, chunk):
        landed(own_part(chunk), one_recv.at[chunk])
        landed(other_part(chunk), two_recv.at[chunk])
        flat = flat_at(chunk)

        @pl.loop(0, most)
        def _(m):
            leaving[m, flat] = gathered[chunk][table[base + m]]

        go(False, send(
            leaving.at[:, flat], crossed[chunk], cross_send.at[chunk], cross_recv.at[chunk], far_inner
        ))

    def inner_out(is_outer, chunk):
        landed(crossed[chunk], cross_recv.at[chunk])
        flat = flat_at(chunk)

        @pl.loop(0, 2 * size)
        def _(place):
            at = base + place
            own = gathered[chunk][table[2 * n + at]]
            other = crossed[chunk][table[3 * n + at]]
            ordered[place, flat] = jnp.where(table[n + at] == 1, other, own)

        go(False, send(
            ordered.at[pl.ds(other_at, size), flat], own_part(chunk), back_send.at[chunk],
            back_recv.at[chunk], near_outer,
        ))
        deliver(chunk, lambda s: ordered.at[own_at + s, flat])

    def outer_out(is_outer, chunk):
        landed(other_part(chunk), back_recv.at[chunk])
        deliver(chunk, lambda s: gathered[chunk].at[other_at + s])

    block = size * rows
    columns = 512

    def compute(is_outer, q):
        tokens_arrive(q, pair)
        tokens_arrive(q, diagonal)
        at = pl.ds(pl.multiple_of(plane_of[q] * block, block), block)

        def more(part, both):
            depth = pl.ds(pl.multiple_of(part * quarter, quarter), quarter)
            return both + jnp.dot(
                tok_all[at, depth], w_gu[depth, :], preferred_element_type=jnp.float32
            )

        both = lax.fori_loop(0, size, more, jnp.zeros((block, 2 * LANES), jnp.float32))
        gate_value = both[:, :LANES]
        up_value = both[:, LANES:]
        hidden[...] = (gate_value / (1.0 + jnp.exp(-gate_value)) * up_value).astype(jnp.bfloat16)
        lanes = lax.broadcasted_iota(jnp.int32, (block, LANES), 1)
        scale = jnp.sum(jnp.where(lanes == me, coef_all[at, :], 0.0), axis=1, keepdims=True)

        @pl.loop(0, width // columns)
        def _(part):
            cols = pl.ds(pl.multiple_of(part * columns, columns), columns)
            value = lax.dot_general(
                hidden[...], w_d[cols, :], (((1,), (1,)), ((), ())),
                preferred_element_type=jnp.float32,
            )
            value = value.astype(jnp.bfloat16).astype(jnp.float32)
            contrib[at, cols] = (value * scale).astype(jnp.bfloat16)

        for row in range(2):
            owner = at_plane(plane_of[q], row * 2 + lax.rem(pair, 2))
            go(is_outer, send(
                contrib.at[token_rows(owner)], pair_in.at[plane_of[q], row],
                pair_send.at[plane_of[q], row], pair_recv.at[plane_of[q], row], beside,
            ))

    def add_rows(parts, target):
        @pl.loop(0, width // columns)
        def _(part):
            cols = pl.ds(pl.multiple_of(part * columns, columns), columns)
            total = sum(source(cols).astype(jnp.float32) for source in parts)
            target[:, cols] = total.astype(jnp.bfloat16)

    def chip_part(q, mine):
        owner_seat, row = (seat, my_row) if mine else (side, 1 - my_row)
        return [
            lambda cols: contrib[token_rows(at_plane(plane_of[q], owner_seat)), cols],
            lambda cols: pair_in[plane_of[q], row, :, cols],
        ]

    def taken(source, sem):
        landed(source, sem)
        return lambda cols: source[:, cols]

    def side_taken(q):
        return taken(side_in.at[plane_of[q]], side_recv.at[plane_of[q]])

    def chain_taken(q):
        return taken(chain_in.at[plane_of[q]], chain_recv.at[plane_of[q]])

    def over_taken(q):
        return taken(over_in.at[plane_of[q]], over_recv.at[plane_of[q]])

    def both_taken():
        return taken(both_in, both_recv)

    def pass_on(is_outer, q, parts):
        at = plane_of[q]
        add_rows(parts, chain_out.at[at])
        if is_outer:
            copy = send(chain_out.at[at], chain_in.at[at], chain_send.at[at], chain_recv.at[at], near_inner)
        elif q == O:
            copy = send(chain_out.at[at], chain_in.at[at], chain_send.at[at], chain_recv.at[at], near_outer)
        else:
            copy = send(chain_out.at[at], over_in.at[at], chain_send.at[at], over_recv.at[at], far_inner)
        go(is_outer, copy)

    def pass_both(is_outer, q):
        add_rows(chip_part(q, False), both_out)
        go(is_outer, send(both_out, both_in, both_send, both_recv, near_inner if is_outer else near_outer))

    def pair_add(is_outer, q):
        at = plane_of[q]
        for row in range(2):
            landed(pair_in.at[at, row], pair_recv.at[at, row])
        if (is_outer, q) == (True, I):
            pass_both(True, q)
            pass_on(True, q, chip_part(q, True))
            return
        if (is_outer, q) == (False, O):
            pass_both(False, q)
            return
        parts = chip_part(q, False)
        if q == (O if is_outer else I):
            parts = parts + [both_taken()]
        add_rows(parts, side_out.at[at])
        go(is_outer, send(side_out.at[at], side_in.at[at], side_send.at[at], side_recv.at[at], across))

    def side_add(is_outer, q):
        parts = chip_part(q, True)
        if is_outer or q != O:
            parts.append(side_taken(q))
        if not is_outer:
            parts.append(over_taken(q) if q == O else chain_taken(q))
        pass_on(is_outer, q, parts)

    def finish_rows(is_outer):
        q = O if is_outer else I
        parts = chip_part(q, True) + [side_taken(q), chain_taken(q)]
        if not is_outer:
            parts.append(over_taken(q))
        add_rows(parts, out)

    steps = (
        own_tokens, seat_tokens, side_tokens, spread, outer_in, inner_in, inner_out, outer_out,
        compute, pair_add, side_add, finish_rows,
    )

    for is_outer, role in ((True, outer), (False, inner)):

        @pl.when(role)
        def _():
            loaded = False
            for place, (name, *arguments) in enumerate(order[0 if is_outer else 1]):
                if name == COMPUTE and not loaded:
                    for load in loads:
                        load.wait()
                    loaded = True
                steps[name](is_outer, *arguments)
                if place == START_LOADS:
                    for load in loads:
                        load.start()
            for copy in sent[is_outer]:
                copy.wait_send()

    for chunk in range(count):
        left = gathered[chunk].at[pl.ds(0, size - 1)]
        landed(left, one_send.at[chunk])
        landed(left, three_send.at[chunk])

    for array in range(3):
        landed(moved[array].at[0], three_recv.at[array])


START_LOADS = 6
LINE_VMEM_BYTES = 59_000_000
LINE_ORDERS = {
    4: (
        ((1, 1, 2, 2, 2, 2, 2, 2, 2), (2, 2, 2, 2, 2, 2, 2, 2), (2, 2, 2, 2, 2, 2, 1, 1, 1, 1)),
        (
            (
            (SPREAD, 0), (SPREAD, 1), (SPREAD, 2), (SPREAD, 3), (OWN,), (OUTER_IN, 0),
            (OUTER_IN, 1), (SPREAD, 4), (SEAT_TOKENS, I), (OUTER_IN, 2), (SPREAD, 5),
            (OUTER_IN, 3), (SPREAD, 6), (SPREAD, 7), (SIDE_TOKENS, O), (SPREAD, 8), (OUTER_IN, 4),
            (SPREAD, 9), (SEAT_TOKENS, J), (OUTER_IN, 5), (OUTER_IN, 6), (SEAT_TOKENS, K),
            (OUTER_IN, 7), (OUTER_OUT, 0), (OUTER_IN, 8), (OUTER_OUT, 1), (OUTER_IN, 9),
            (SPREAD, 10), (OUTER_OUT, 2), (SPREAD, 11), (OUTER_OUT, 3), (SPREAD, 12),
            (OUTER_IN, 10), (SPREAD, 13), (SPREAD, 14), (OUTER_OUT, 4), (OUTER_IN, 11),
            (SPREAD, 15), (OUTER_OUT, 5), (OUTER_IN, 12), (OUTER_IN, 13), (SPREAD, 16),
            (OUTER_OUT, 6), (OUTER_IN, 14), (SPREAD, 17), (OUTER_OUT, 7), (OUTER_IN, 15),
            (SPREAD, 18), (OUTER_OUT, 8), (OUTER_IN, 16), (SPREAD, 19), (OUTER_OUT, 9),
            (OUTER_IN, 17), (SPREAD, 20), (OUTER_OUT, 10), (OUTER_IN, 18), (SPREAD, 21),
            (OUTER_OUT, 11), (OUTER_IN, 19), (SPREAD, 22), (OUTER_OUT, 12), (OUTER_IN, 20),
            (SPREAD, 23), (OUTER_OUT, 13), (OUTER_IN, 21), (SPREAD, 24), (SPREAD, 25),
            (OUTER_OUT, 14), (OUTER_IN, 22), (SPREAD, 26), (OUTER_IN, 23), (OUTER_OUT, 15),
            (SIDE_TOKENS, K), (OUTER_IN, 24), (COMPUTE, K), (OUTER_IN, 25), (OUTER_OUT, 16),
            (SIDE_TOKENS, J), (OUTER_IN, 26), (PAIR_ADD, K), (COMPUTE, J), (OUTER_OUT, 17),
            (PAIR_ADD, J), (OUTER_OUT, 18), (SIDE_TOKENS, I), (SIDE_ADD, K), (COMPUTE, O),
            (COMPUTE, I), (PAIR_ADD, O), (OUTER_OUT, 19), (SIDE_ADD, J), (OUTER_OUT, 20),
            (PAIR_ADD, I), (OUTER_OUT, 21), (OUTER_OUT, 22), (OUTER_OUT, 23), (OUTER_OUT, 24),
            (OUTER_OUT, 25), (OUTER_OUT, 26), (FINISH,),
            ),
            (
            (OWN,), (SPREAD, 0), (SPREAD, 1), (SPREAD, 2), (SPREAD, 3), (SPREAD, 4),
            (SIDE_TOKENS, I), (SEAT_TOKENS, J), (SEAT_TOKENS, O), (INNER_IN, 0), (INNER_IN, 1),
            (SPREAD, 5), (SEAT_TOKENS, K), (INNER_IN, 2), (INNER_OUT, 0), (INNER_OUT, 1),
            (INNER_IN, 3), (SPREAD, 6), (INNER_OUT, 2), (SIDE_TOKENS, O), (SPREAD, 7),
            (COMPUTE, O), (SIDE_TOKENS, K), (SIDE_TOKENS, J), (INNER_OUT, 3), (INNER_IN, 4),
            (PAIR_ADD, O), (SPREAD, 8), (COMPUTE, K), (SPREAD, 9), (INNER_IN, 5), (SPREAD, 10),
            (INNER_OUT, 4), (INNER_IN, 6), (SPREAD, 11), (INNER_OUT, 5), (INNER_IN, 7),
            (SPREAD, 12), (INNER_OUT, 6), (INNER_IN, 8), (SPREAD, 13), (INNER_OUT, 7),
            (INNER_IN, 9), (SPREAD, 14), (INNER_OUT, 8), (INNER_IN, 10), (SPREAD, 15),
            (INNER_OUT, 9), (INNER_IN, 11), (SPREAD, 16), (COMPUTE, I), (INNER_OUT, 10),
            (INNER_IN, 12), (SPREAD, 17), (INNER_OUT, 11), (INNER_IN, 13), (SPREAD, 18),
            (INNER_OUT, 12), (INNER_IN, 14), (SPREAD, 19), (INNER_OUT, 13), (COMPUTE, J),
            (INNER_IN, 15), (SPREAD, 20), (INNER_OUT, 14), (PAIR_ADD, J), (INNER_IN, 16),
            (INNER_OUT, 15), (INNER_IN, 17), (SPREAD, 21), (INNER_OUT, 16), (INNER_IN, 18),
            (SPREAD, 22), (INNER_OUT, 17), (INNER_IN, 19), (SPREAD, 23), (INNER_OUT, 18),
            (INNER_IN, 20), (SPREAD, 24), (SPREAD, 25), (INNER_OUT, 19), (INNER_IN, 21),
            (SPREAD, 26), (PAIR_ADD, K), (INNER_OUT, 20), (INNER_IN, 22), (INNER_IN, 23),
            (INNER_OUT, 21), (INNER_IN, 24), (INNER_IN, 25), (INNER_OUT, 22), (INNER_IN, 26),
            (INNER_OUT, 23), (INNER_OUT, 24), (SIDE_ADD, K), (INNER_OUT, 25), (INNER_OUT, 26),
            (SIDE_ADD, J), (SIDE_ADD, O), (PAIR_ADD, I), (FINISH,),
            ),
        ),
    ),
    5: (
        ((1, 1, 2, 2, 2, 2, 2, 2, 2), (2, 2, 2, 2, 2, 2, 2, 2), (2, 2, 2, 2, 2, 2, 2, 1, 1)),
        (
            (
            (SPREAD, 0), (SPREAD, 1), (SPREAD, 2), (OWN,), (OUTER_IN, 0), (SPREAD, 3),
            (OUTER_IN, 1), (SPREAD, 4), (OUTER_IN, 2), (SPREAD, 5), (SPREAD, 6), (SPREAD, 7),
            (OUTER_IN, 3), (SEAT_TOKENS, I), (SPREAD, 8), (OUTER_IN, 4), (SPREAD, 9),
            (OUTER_IN, 5), (SPREAD, 10), (OUTER_IN, 6), (SPREAD, 11), (OUTER_IN, 7),
            (OUTER_OUT, 0), (OUTER_IN, 8), (SPREAD, 12), (OUTER_OUT, 1), (OUTER_IN, 9),
            (SPREAD, 13), (OUTER_IN, 10), (SPREAD, 14), (OUTER_OUT, 2), (OUTER_IN, 11),
            (OUTER_IN, 12), (SPREAD, 15), (OUTER_OUT, 3), (OUTER_IN, 13), (SPREAD, 16),
            (SIDE_TOKENS, O), (OUTER_IN, 14), (COMPUTE, O), (SPREAD, 17), (OUTER_OUT, 4),
            (OUTER_IN, 15), (SEAT_TOKENS, K), (OUTER_OUT, 5), (OUTER_IN, 16), (OUTER_IN, 17),
            (OUTER_OUT, 6), (SPREAD, 18), (SIDE_TOKENS, I), (COMPUTE, I), (SIDE_TOKENS, K),
            (SPREAD, 19), (OUTER_OUT, 7), (PAIR_ADD, I), (COMPUTE, K), (SPREAD, 20), (SPREAD, 21),
            (OUTER_OUT, 8), (OUTER_IN, 18), (OUTER_IN, 19), (SPREAD, 22), (OUTER_OUT, 9),
            (OUTER_IN, 20), (SPREAD, 23), (OUTER_IN, 21), (OUTER_OUT, 10), (SPREAD, 24),
            (OUTER_IN, 22), (SPREAD, 25), (OUTER_OUT, 11), (OUTER_IN, 23), (PAIR_ADD, O),
            (OUTER_IN, 24), (OUTER_IN, 25), (OUTER_OUT, 12), (OUTER_OUT, 13), (OUTER_OUT, 14),
            (OUTER_OUT, 15), (OUTER_OUT, 16), (PAIR_ADD, K), (SEAT_TOKENS, J), (OUTER_OUT, 17),
            (SIDE_ADD, K), (OUTER_OUT, 18), (SIDE_TOKENS, J), (COMPUTE, J), (OUTER_OUT, 19),
            (PAIR_ADD, J), (OUTER_OUT, 20), (SIDE_ADD, J), (OUTER_OUT, 21), (OUTER_OUT, 22),
            (OUTER_OUT, 23), (OUTER_OUT, 24), (OUTER_OUT, 25), (FINISH,),
            ),
            (
            (SPREAD, 0), (SPREAD, 1), (SPREAD, 2), (OWN,), (SPREAD, 3), (SEAT_TOKENS, O),
            (SPREAD, 4), (INNER_IN, 0), (SPREAD, 5), (SIDE_TOKENS, I), (INNER_IN, 1), (SPREAD, 6),
            (COMPUTE, I), (SPREAD, 7), (SEAT_TOKENS, K), (INNER_IN, 2), (INNER_OUT, 0),
            (INNER_OUT, 1), (INNER_IN, 3), (SPREAD, 8), (INNER_OUT, 2), (INNER_IN, 4),
            (SIDE_TOKENS, K), (SPREAD, 9), (SPREAD, 10), (INNER_IN, 5), (INNER_OUT, 3),
            (COMPUTE, K), (SPREAD, 11), (INNER_IN, 6), (INNER_OUT, 4), (SPREAD, 12), (INNER_IN, 7),
            (SPREAD, 13), (INNER_OUT, 5), (INNER_IN, 8), (SPREAD, 14), (INNER_OUT, 6),
            (INNER_IN, 9), (SPREAD, 15), (SPREAD, 16), (INNER_IN, 10), (INNER_OUT, 7),
            (SPREAD, 17), (INNER_IN, 11), (INNER_OUT, 8), (SPREAD, 18), (INNER_IN, 12),
            (SPREAD, 19), (INNER_OUT, 9), (INNER_IN, 13), (SPREAD, 20), (INNER_OUT, 10),
            (SIDE_TOKENS, O), (COMPUTE, O), (SPREAD, 21), (SPREAD, 22), (INNER_IN, 14),
            (INNER_OUT, 11), (PAIR_ADD, O), (SPREAD, 23), (INNER_IN, 15), (INNER_OUT, 12),
            (SPREAD, 24), (INNER_IN, 16), (SPREAD, 25), (INNER_OUT, 13), (INNER_IN, 17),
            (INNER_OUT, 14), (PAIR_ADD, I), (INNER_OUT, 15), (INNER_IN, 18), (INNER_OUT, 16),
            (PAIR_ADD, K), (INNER_IN, 19), (SEAT_TOKENS, J), (INNER_OUT, 17), (INNER_IN, 20),
            (INNER_OUT, 18), (INNER_IN, 21), (SIDE_TOKENS, J), (COMPUTE, J), (INNER_IN, 22),
            (INNER_OUT, 19), (PAIR_ADD, J), (INNER_IN, 23), (INNER_OUT, 20), (INNER_IN, 24),
            (INNER_IN, 25), (INNER_OUT, 21), (SIDE_ADD, K), (INNER_OUT, 22), (INNER_OUT, 23),
            (SIDE_ADD, J), (INNER_OUT, 24), (INNER_OUT, 25), (SIDE_ADD, O), (FINISH,),
            ),
        ),
    ),
    6: (
        ((1, 1, 2, 2, 2, 2, 2, 2, 2), (2, 2, 2, 2, 2, 2, 2, 2), (2, 2, 2, 2, 2, 2, 2, 1, 1)),
        (
            (
            (SPREAD, 0), (SPREAD, 1), (SPREAD, 2), (OWN,), (OUTER_IN, 0), (SPREAD, 3),
            (OUTER_IN, 1), (SPREAD, 4), (OUTER_IN, 2), (SPREAD, 5), (SPREAD, 6), (SPREAD, 7),
            (OUTER_IN, 3), (SPREAD, 8), (OUTER_IN, 4), (SPREAD, 9), (OUTER_IN, 5), (SPREAD, 10),
            (OUTER_IN, 6), (OUTER_OUT, 0), (OUTER_IN, 7), (SPREAD, 11), (OUTER_OUT, 1),
            (OUTER_IN, 8), (SPREAD, 12), (OUTER_IN, 9), (SPREAD, 13), (OUTER_IN, 10), (SPREAD, 14),
            (SIDE_TOKENS, O), (OUTER_IN, 11), (SPREAD, 15), (OUTER_OUT, 2), (OUTER_IN, 12),
            (SPREAD, 16), (OUTER_IN, 13), (SPREAD, 17), (OUTER_OUT, 3), (OUTER_IN, 14),
            (OUTER_IN, 15), (SPREAD, 18), (SPREAD, 19), (OUTER_OUT, 4), (OUTER_IN, 16),
            (OUTER_IN, 17), (SPREAD, 20), (SPREAD, 21), (OUTER_OUT, 5), (OUTER_IN, 18),
            (OUTER_IN, 19), (SPREAD, 22), (SPREAD, 23), (OUTER_OUT, 6), (OUTER_IN, 20),
            (OUTER_IN, 21), (SPREAD, 24), (SPREAD, 25), (OUTER_OUT, 7), (OUTER_IN, 22),
            (OUTER_IN, 23), (OUTER_IN, 24), (SEAT_TOKENS, I), (OUTER_OUT, 8), (OUTER_IN, 25),
            (OUTER_OUT, 9), (OUTER_OUT, 10), (OUTER_OUT, 11), (SEAT_TOKENS, K), (OUTER_OUT, 12),
            (COMPUTE, O), (SIDE_TOKENS, K), (OUTER_OUT, 13), (COMPUTE, K), (PAIR_ADD, K),
            (OUTER_OUT, 14), (SIDE_TOKENS, I), (COMPUTE, I), (SIDE_ADD, K), (SEAT_TOKENS, J),
            (PAIR_ADD, I), (OUTER_OUT, 15), (SIDE_TOKENS, J), (COMPUTE, J), (PAIR_ADD, O),
            (PAIR_ADD, J), (OUTER_OUT, 16), (OUTER_OUT, 17), (SIDE_ADD, J), (OUTER_OUT, 18),
            (OUTER_OUT, 19), (OUTER_OUT, 20), (OUTER_OUT, 21), (OUTER_OUT, 22), (OUTER_OUT, 23),
            (OUTER_OUT, 24), (OUTER_OUT, 25), (FINISH,),
            ),
            (
            (SPREAD, 0), (SPREAD, 1), (SPREAD, 2), (OWN,), (SPREAD, 3), (SEAT_TOKENS, O),
            (SPREAD, 4), (INNER_IN, 0), (SPREAD, 5), (INNER_IN, 1), (SPREAD, 6), (SPREAD, 7),
            (INNER_IN, 2), (SPREAD, 8), (INNER_OUT, 0), (SPREAD, 9), (INNER_OUT, 1), (INNER_IN, 3),
            (SPREAD, 10), (SPREAD, 11), (INNER_IN, 4), (INNER_OUT, 2), (SPREAD, 12), (INNER_IN, 5),
            (SPREAD, 13), (INNER_OUT, 3), (INNER_IN, 6), (SPREAD, 14), (SPREAD, 15), (INNER_IN, 7),
            (INNER_OUT, 4), (SPREAD, 16), (INNER_IN, 8), (SPREAD, 17), (INNER_OUT, 5),
            (INNER_IN, 9), (SPREAD, 18), (SPREAD, 19), (INNER_IN, 10), (INNER_OUT, 6),
            (SPREAD, 20), (SIDE_TOKENS, O), (SPREAD, 21), (INNER_OUT, 7), (INNER_IN, 11),
            (SPREAD, 22), (SPREAD, 23), (INNER_IN, 12), (INNER_OUT, 8), (SPREAD, 24),
            (INNER_IN, 13), (SPREAD, 25), (INNER_OUT, 9), (INNER_IN, 14), (SEAT_TOKENS, K),
            (INNER_IN, 15), (INNER_OUT, 10), (INNER_IN, 16), (INNER_OUT, 11), (INNER_IN, 17),
            (SIDE_TOKENS, K), (COMPUTE, K), (INNER_OUT, 12), (INNER_IN, 18), (PAIR_ADD, K),
            (INNER_IN, 19), (INNER_OUT, 13), (INNER_IN, 20), (INNER_IN, 21), (INNER_OUT, 14),
            (INNER_IN, 22), (SIDE_TOKENS, I), (COMPUTE, O), (COMPUTE, I), (SEAT_TOKENS, J),
            (INNER_OUT, 15), (PAIR_ADD, O), (INNER_IN, 23), (INNER_IN, 24), (INNER_IN, 25),
            (INNER_OUT, 16), (SIDE_TOKENS, J), (COMPUTE, J), (INNER_OUT, 17), (PAIR_ADD, J),
            (SIDE_ADD, K), (INNER_OUT, 18), (PAIR_ADD, I), (INNER_OUT, 19), (INNER_OUT, 20),
            (SIDE_ADD, J), (INNER_OUT, 21), (INNER_OUT, 22), (INNER_OUT, 23), (INNER_OUT, 24),
            (INNER_OUT, 25), (SIDE_ADD, O), (FINISH,),
            ),
        ),
    ),
    8: (
        ((1, 1, 2, 2, 2, 2, 2, 2, 2), (2, 2, 2, 2, 2, 2, 2, 2), (2, 2, 2, 2, 2, 2, 2, 1, 1)),
        (
            (
            (SPREAD, 0), (OWN,), (OUTER_IN, 0), (SPREAD, 1), (SPREAD, 2), (SEAT_TOKENS, I),
            (SPREAD, 3), (OUTER_IN, 1), (SPREAD, 4), (OUTER_IN, 2), (SPREAD, 5), (OUTER_IN, 3),
            (SPREAD, 6), (OUTER_IN, 4), (SPREAD, 7), (OUTER_IN, 5), (SPREAD, 8), (OUTER_IN, 6),
            (SPREAD, 9), (OUTER_IN, 7), (SPREAD, 10), (OUTER_OUT, 0), (OUTER_IN, 8), (SPREAD, 11),
            (OUTER_OUT, 1), (OUTER_IN, 9), (OUTER_IN, 10), (SPREAD, 12), (SPREAD, 13),
            (OUTER_IN, 11), (SPREAD, 14), (OUTER_IN, 12), (SPREAD, 15), (OUTER_OUT, 2),
            (OUTER_IN, 13), (OUTER_IN, 14), (SPREAD, 16), (OUTER_IN, 15), (SPREAD, 17),
            (SPREAD, 18), (OUTER_OUT, 3), (OUTER_IN, 16), (OUTER_IN, 17), (SPREAD, 19),
            (OUTER_IN, 18), (SPREAD, 20), (SPREAD, 21), (OUTER_OUT, 4), (OUTER_IN, 19),
            (OUTER_IN, 20), (SPREAD, 22), (OUTER_IN, 21), (SPREAD, 23), (SPREAD, 24), (SPREAD, 25),
            (OUTER_OUT, 5), (OUTER_IN, 22), (OUTER_IN, 23), (OUTER_IN, 24), (OUTER_IN, 25),
            (SEAT_TOKENS, K), (OUTER_OUT, 6), (SIDE_TOKENS, K), (COMPUTE, K), (OUTER_OUT, 7),
            (SIDE_TOKENS, O), (PAIR_ADD, K), (COMPUTE, O), (OUTER_OUT, 8), (SIDE_ADD, K),
            (SIDE_TOKENS, I), (COMPUTE, I), (PAIR_ADD, I), (OUTER_OUT, 9), (SEAT_TOKENS, J),
            (OUTER_OUT, 10), (SIDE_TOKENS, J), (COMPUTE, J), (OUTER_OUT, 11), (PAIR_ADD, J),
            (SIDE_ADD, J), (OUTER_OUT, 12), (PAIR_ADD, O), (OUTER_OUT, 13), (OUTER_OUT, 14),
            (OUTER_OUT, 15), (OUTER_OUT, 16), (OUTER_OUT, 17), (OUTER_OUT, 18), (OUTER_OUT, 19),
            (OUTER_OUT, 20), (OUTER_OUT, 21), (OUTER_OUT, 22), (OUTER_OUT, 23), (OUTER_OUT, 24),
            (OUTER_OUT, 25), (FINISH,),
            ),
            (
            (OWN,), (SPREAD, 0), (SPREAD, 1), (SPREAD, 2), (SEAT_TOKENS, O), (SPREAD, 3),
            (INNER_IN, 0), (SPREAD, 4), (SPREAD, 5), (INNER_IN, 1), (SPREAD, 6), (SIDE_TOKENS, I),
            (SPREAD, 7), (COMPUTE, I), (INNER_OUT, 0), (INNER_IN, 2), (SPREAD, 8), (SPREAD, 9),
            (INNER_OUT, 1), (INNER_IN, 3), (SPREAD, 10), (INNER_IN, 4), (SPREAD, 11), (SPREAD, 12),
            (INNER_OUT, 2), (INNER_IN, 5), (SPREAD, 13), (INNER_IN, 6), (SPREAD, 14), (SPREAD, 15),
            (INNER_OUT, 3), (INNER_IN, 7), (SPREAD, 16), (INNER_IN, 8), (SPREAD, 17), (SPREAD, 18),
            (INNER_OUT, 4), (INNER_IN, 9), (SPREAD, 19), (INNER_IN, 10), (SPREAD, 20),
            (SPREAD, 21), (INNER_OUT, 5), (SEAT_TOKENS, J), (INNER_IN, 11), (INNER_IN, 12),
            (SEAT_TOKENS, K), (INNER_OUT, 6), (INNER_IN, 13), (SIDE_TOKENS, J), (COMPUTE, J),
            (INNER_IN, 14), (SPREAD, 22), (SIDE_TOKENS, K), (PAIR_ADD, J), (COMPUTE, K),
            (INNER_OUT, 7), (INNER_IN, 15), (INNER_IN, 16), (SPREAD, 23), (SPREAD, 24),
            (INNER_OUT, 8), (INNER_IN, 17), (SPREAD, 25), (INNER_IN, 18), (INNER_OUT, 9),
            (INNER_IN, 19), (INNER_IN, 20), (INNER_OUT, 10), (INNER_IN, 21), (INNER_IN, 22),
            (INNER_OUT, 11), (INNER_IN, 23), (PAIR_ADD, K), (INNER_IN, 24), (INNER_IN, 25),
            (INNER_OUT, 12), (SIDE_TOKENS, O), (COMPUTE, O), (SIDE_ADD, K), (PAIR_ADD, O),
            (INNER_OUT, 13), (PAIR_ADD, I), (INNER_OUT, 14), (SIDE_ADD, J), (INNER_OUT, 15),
            (INNER_OUT, 16), (INNER_OUT, 17), (INNER_OUT, 18), (INNER_OUT, 19), (INNER_OUT, 20),
            (INNER_OUT, 21), (INNER_OUT, 22), (INNER_OUT, 23), (INNER_OUT, 24), (INNER_OUT, 25),
            (SIDE_ADD, O), (FINISH,),
            ),
        ),
    ),
}


def call_line(n, most, which, table, tokens, coef, held_gate, held_up, held_down):
    rows, width = tokens.shape
    size = 4
    planes = n // size
    quarter = width // size
    cuts, order = LINE_ORDERS[most]
    plan = chunk_plan(quarter, cuts)
    count = len(plan)
    vmem = pl.BlockSpec(memory_space=pltpu.VMEM)
    anywhere = pl.BlockSpec(memory_space=pl.ANY)
    dma = pltpu.SemaphoreType.DMA
    moved_shape = jax.ShapeDtypeStruct(held_gate.shape, held_gate.dtype)

    def block(*shape):
        return pltpu.VMEM(shape, jnp.bfloat16)

    return pl.pallas_call(
        functools.partial(line_kernel, n, most, plan, order),
        out_shape=(jax.ShapeDtypeStruct((rows, width), jnp.bfloat16),) + (moved_shape,) * 3,
        in_specs=[pl.BlockSpec(memory_space=pltpu.SMEM), anywhere, vmem] + [anywhere] * 3,
        out_specs=(vmem, anywhere, anywhere, anywhere),
        scratch_shapes=[
            *(block(2 * size, length, LANES) for _, _, length in plan),
            *(block(most, length, LANES) for _, _, length in plan),
            block(most, 3 * quarter, LANES),
            block(2 * size, 3 * quarter, LANES),
            block(n * rows, width),
            pltpu.VMEM((n * rows, LANES), jnp.float32),
            block(width, 2 * LANES),
            block(width, LANES),
            block(size * rows, LANES),
            block(n * rows, width),
            block(planes, 2, rows, width),
            block(planes, rows, width),
            block(planes, rows, width),
            block(planes, rows, width),
            block(planes, rows, width),
            block(planes, rows, width),
            block(rows, width),
            block(rows, width),
            dma((4,)),
            dma((2, planes, 6)),
            dma((2, n)),
            dma((count,)),
            dma((count,)),
            dma((count,)),
            dma((count,)),
            dma((count,)),
            dma((count,)),
            dma((count,)),
            dma((count,)),
            dma((count,)),
            dma((3,)),
            dma((planes, 2)),
            dma((planes, 2)),
            dma((planes,)),
            dma((planes,)),
            dma((planes,)),
            dma((planes,)),
            dma((planes,)),
            dma,
            dma,
        ],
        compiler_params=pltpu.CompilerParams(
            collective_id=which, has_side_effects=True, vmem_limit_bytes=LINE_VMEM_BYTES
        ),
    )(table, tokens, coef, held_gate, held_up, held_down)


def plan_kernel(n, levels, old, new, ids, logits, table, level, coef, target):
    half = n // 2
    blocks = n // EXPERTS
    rows = coef.shape[0]

    @pl.loop(0, n)
    def _(slot):
        target[old[slot]] = new[slot]

    @pl.loop(0, half)
    def _(place):
        table[place] = 0
        table[half + place] = 0

    crossing = jnp.int32(0)
    for side in range(2):

        def place_one(lane, turn):
            goes_to = target[side * half + lane]
            crosses = ((goes_to >= half).astype(jnp.int32) + side) % 2

            @pl.when(crosses == 1)
            def _():
                table[side * half + turn] = lane

            table[n + goes_to] = crosses
            table[2 * n + goes_to] = (1 - crosses) * lane
            table[3 * n + goes_to] = crosses * turn
            return turn + crosses

        crossing = lax.fori_loop(0, half, place_one, jnp.int32(0))
    level[0] = sum((crossing > most).astype(jnp.int32) for most in levels[:-1])

    lanes = lax.broadcasted_iota(jnp.int32, (rows, LANES), 1)
    expert_at = jnp.full((rows, LANES), -1, jnp.int32)
    for slot in range(n):
        expert_at = jnp.where(lanes == old[slot], slot // blocks, expert_at)
    eye = lax.broadcasted_iota(jnp.int32, (rows, rows), 0) == lax.broadcasted_iota(
        jnp.int32, (rows, rows), 1
    )

    def column(ref, row):
        return jnp.sum(jnp.where(eye, ref[row : row + 1, :], 0), axis=1, keepdims=True)

    first, second = column(logits, 0), column(logits, 1)
    first_weight = 1.0 / (1.0 + jnp.exp(second - first))
    second_weight = 1.0 / (1.0 + jnp.exp(first - second))
    total = jnp.where(column(ids, 0) == expert_at, first_weight, 0.0)
    coef[...] = total + jnp.where(column(ids, 1) == expert_at, second_weight, 0.0)


def write_kernel(*refs):
    sources, targets, held, sems, held_sems = refs[:4], refs[4:8], refs[8], refs[9], refs[10]
    parts = held_sems.shape[0]
    length = held.shape[0] // parts
    copies = [
        pltpu.make_async_copy(source, target, sems.at[at])
        for at, (source, target) in enumerate(zip(sources[:3], targets[:3]))
    ]
    taken, given = [], []
    for part in range(parts):
        at = pl.ds(part * length, length)
        taken.append(pltpu.make_async_copy(sources[3].at[0, at], held.at[at], held_sems.at[part, 0]))
        given.append(pltpu.make_async_copy(held.at[at], targets[3].at[0, at], held_sems.at[part, 1]))
    for copy in taken + copies:
        copy.start()
    for first, second in zip(taken, given):
        first.wait()
        second.start()
    for copy in copies + given:
        copy.wait()


def line_layer(
    tokens, route_ids, route_logits, old_place, new_place, held_gate, held_up, held_down
):
    n = lax.axis_size("expert")
    levels = sorted(LINE_ORDERS)
    rows = tokens.shape[0]
    smem = pl.BlockSpec(memory_space=pltpu.SMEM)
    vmem = pl.BlockSpec(memory_space=pltpu.VMEM)
    table, level, coef = pl.pallas_call(
        functools.partial(plan_kernel, n, levels),
        out_shape=(
            jax.ShapeDtypeStruct((4 * n,), jnp.int32),
            jax.ShapeDtypeStruct((1,), jnp.int32),
            jax.ShapeDtypeStruct((rows, LANES), jnp.float32),
        ),
        in_specs=[smem, smem, vmem, vmem],
        out_specs=(smem, smem, vmem),
        scratch_shapes=[pltpu.SMEM((n,), jnp.int32)],
    )(old_place, new_place, route_ids.T, route_logits.T)
    branches = [functools.partial(call_line, n, most, i) for i, most in enumerate(levels)]
    results = lax.switch(level[0], branches, table, tokens, coef, held_gate, held_up, held_down)
    anywhere = pl.BlockSpec(memory_space=pl.ANY)
    return pl.pallas_call(
        write_kernel,
        out_shape=tuple(jax.ShapeDtypeStruct(array.shape, array.dtype) for array in results),
        in_specs=[anywhere] * 4,
        out_specs=(anywhere,) * 4,
        scratch_shapes=[
            pltpu.VMEM(held_down.shape[1:], held_down.dtype),
            pltpu.SemaphoreType.DMA((3,)),
            pltpu.SemaphoreType.DMA((4, 2)),
        ],
    )(*results)


def per_device(
    tokens, route_ids, route_logits, old_place, new_place, held_gate, held_up, held_down
):
    n = lax.axis_size("expert")
    if n == 16 and tokens.shape[1] % 512 == 0:
        return line_layer(
            tokens, route_ids, route_logits, old_place, new_place, held_gate, held_up, held_down
        )
    half = n // 2
    device_ids = jnp.arange(n, dtype=jnp.int32)
    blocks = n // EXPERTS
    at_old = (old_place[:, None] == device_ids[None, :]).astype(jnp.int32)
    dest_of = jnp.sum(at_old * new_place[:, None], axis=0)
    expert_at = jnp.sum(at_old * device_ids[:, None], axis=0) // blocks
    half_of = device_ids // half
    crosses = (dest_of // half != half_of).astype(jnp.int32)
    earlier = (half_of[:, None] == half_of[None, :]) & (device_ids[:, None] < device_ids[None, :])
    turn = jnp.sum(earlier.astype(jnp.int32) * crosses[:, None], axis=0)
    lane_of = device_ids - half_of * half
    leaving = (half_of[:, None] * half + turn[:, None] == device_ids[None, :]).astype(jnp.int32)
    leaving = jnp.sum(leaving * (crosses * lane_of)[:, None], axis=0)
    arriving = (dest_of[:, None] == device_ids[None, :]).astype(jnp.int32)
    table = jnp.concatenate([
        leaving,
        jnp.sum(arriving * crosses[:, None], axis=0),
        jnp.sum(arriving * ((1 - crosses) * lane_of)[:, None], axis=0),
        jnp.sum(arriving * (crosses * turn)[:, None], axis=0),
    ])
    first_weight = 1.0 / (1.0 + jnp.exp(route_logits[:, 1] - route_logits[:, 0]))
    second_weight = 1.0 / (1.0 + jnp.exp(route_logits[:, 0] - route_logits[:, 1]))
    coef = jnp.where(route_ids[:, 0:1] == expert_at[None, :], first_weight[:, None], 0.0)
    coef = coef + jnp.where(route_ids[:, 1:2] == expert_at[None, :], second_weight[:, None], 0.0)
    coef = jnp.pad(coef, ((0, 0), (0, LANES - n)))
    table, coef = lax.optimization_barrier((table, coef))
    levels = sorted({max(1, half * eighths // 8) for eighths in (3, 4, 5, 6, 8)})
    crossing = jnp.sum(crosses) // 2
    level = sum((crossing > most).astype(jnp.int32) for most in levels[:-1])
    branches = [functools.partial(call_layer, n, most, i) for i, most in enumerate(levels)]
    return lax.switch(level, branches, table, tokens, coef, held_gate, held_up, held_down)


def solution(mesh):
    split = ("groups", "expert")
    placed = (
        P(split, None),
        P(split, None),
        P(split, None),
        P(),
        P(),
        P(split, None, None),
        P(split, None, None),
        P(split, None, None),
    )
    return jax.shard_map(
        per_device,
        mesh=mesh,
        in_specs=placed,
        out_specs=(
            P(split, None),
            P(split, None, None),
            P(split, None, None),
            P(split, None, None),
        ),
        check_vma=False,
    )
```

```python
import functools

import jax
import jax.numpy as jnp
from jax import lax
from jax.experimental import pallas as pl
from jax.experimental.pallas import tpu as pltpu
from jax.sharding import PartitionSpec as P

EXPERTS = 8
LANES = 128
MESH = pl.DeviceIdType.MESH
VMEM_BYTES = 63_000_000


def near_square_root(n):
    size = 1
    while size * size < n:
        size *= 2
    return size


def layer_kernel(
    n,
    most,
    table,
    tok,
    coef,
    held_g,
    held_u,
    held_d,
    out,
    moved_g,
    moved_u,
    moved_d,
    tok_all,
    coef_all,
    w_gu,
    w_d,
    pieces_g,
    pieces_u,
    pieces_d,
    crossed_g,
    crossed_u,
    crossed_d,
    ordered,
    hidden,
    contrib,
    part_in,
    plane_sum,
    half_in,
    cross_out,
    cross_in,
    load_sem,
    tok_send,
    fwd_send,
    plane_send,
    tok_recv,
    one_send,
    one_recv,
    two_send,
    two_recv,
    three_send,
    three_recv,
    part_send,
    part_recv,
    half_send,
    half_recv,
    cross_send,
    cross_recv,
):
    me = lax.axis_index("expert")
    half = n // 2
    base = (me // half) * half
    lane = me - base
    twin = lax.rem(me + half, n)
    rows, width = tok.shape
    band = width // half
    size = near_square_root(n)
    planes = n // size
    half_planes = planes // 2
    plane = me // size
    seat = me - plane * size
    my_plane_of_half = lane // size
    held = (held_g, held_u, held_d)
    moved = (moved_g, moved_u, moved_d)
    pieces = (pieces_g, pieces_u, pieces_d)
    crossed = (crossed_g, crossed_u, crossed_d)

    barrier = pltpu.get_barrier_semaphore()

    @pl.loop(1, n)
    def _(k):
        pl.semaphore_signal(
            barrier, inc=1, device_id={"expert": lax.rem(me + k, n)}, device_id_type=MESH
        )

    loads = (
        pltpu.make_async_copy(held_g.at[0], w_gu.at[:, pl.ds(0, LANES)], load_sem.at[0]),
        pltpu.make_async_copy(held_u.at[0], w_gu.at[:, pl.ds(LANES, LANES)], load_sem.at[1]),
        pltpu.make_async_copy(held_d.at[0], w_d, load_sem.at[2]),
    )
    for load in loads:
        load.start()

    def token_rows(owner):
        return pl.ds(pl.multiple_of(owner * rows, rows), rows)

    def band_rows(owner):
        return pl.ds(pl.multiple_of(owner * band, band), band)

    def near(k):
        return base + lax.rem(lane + k, half)

    def column(k):
        return base + lax.rem(lane + k * size, half)

    def mate(k):
        return plane * size + lax.rem(seat + k, size)

    def seated(other_plane):
        return other_plane * size + seat

    tok_all[token_rows(me), :] = tok[...]
    coef_all[token_rows(me), :] = coef[...]
    pl.semaphore_wait(barrier, n - 1)

    def send(source, target, send_sem, recv_sem, peer):
        return pltpu.make_async_remote_copy(
            src_ref=source, dst_ref=target, send_sem=send_sem, recv_sem=recv_sem,
            device_id={"expert": peer}, device_id_type=MESH,
        )

    def own_tokens(peer):
        at = token_rows(me)
        return (
            send(tok, tok_all.at[at], tok_send.at[0, peer], tok_recv.at[0, me], peer),
            send(coef, coef_all.at[at], tok_send.at[1, peer], tok_recv.at[1, me], peer),
        )

    def passed_tokens(owner, peer, sems):
        at = token_rows(owner)
        return (
            send(tok_all.at[at], tok_all.at[at], sems[0], tok_recv.at[0, owner], peer),
            send(coef_all.at[at], coef_all.at[at], sems[1], tok_recv.at[1, owner], peer),
        )

    def twin_tokens(peer):
        return passed_tokens(twin, peer, (fwd_send.at[0, peer], fwd_send.at[1, peer]))

    def plane_tokens(other_plane, k):
        sems = (plane_send.at[0, other_plane, k], plane_send.at[1, other_plane, k])
        return passed_tokens(seated(other_plane), mate(k), sems)

    def tokens_arrive(owner):
        pltpu.make_async_copy(tok, tok_all.at[token_rows(owner)], tok_recv.at[0, owner]).wait()
        pltpu.make_async_copy(coef, coef_all.at[token_rows(owner)], tok_recv.at[1, owner]).wait()

    def spread(array):
        pltpu.make_async_copy(
            held[array].at[0, band_rows(lane)], pieces[array].at[lane], one_recv.at[array]
        ).start()

        @pl.loop(1, half)
        def _(k):
            peer = near(k)
            send(
                held[array].at[0, band_rows(peer - base)], pieces[array].at[lane],
                one_send.at[array], one_recv.at[array], peer,
            ).start()

    def swap(array):
        return send(
            ordered.at[array, pl.ds(0, most)], crossed[array],
            two_send.at[array], two_recv.at[array], twin,
        )

    def cross_over(array):
        pltpu.make_async_copy(pieces[array], pieces[array], one_recv.at[array]).wait()

        @pl.loop(0, most)
        def _(m):
            ordered[array, m] = pieces[array][table[base + m]]

        swap(array).start()

    def deliver(array):
        swap(array).wait()

        @pl.loop(0, half)
        def _(place):
            at = base + place
            own = pieces[array][table[2 * n + at]]
            other = crossed[array][table[3 * n + at]]
            ordered[array, place] = jnp.where(table[n + at] == 1, other, own)

        pltpu.make_async_copy(
            ordered.at[array, lane], moved[array].at[0, band_rows(lane)], three_recv.at[array]
        ).start()

        @pl.loop(1, half)
        def _(k):
            peer = near(k)
            send(
                ordered.at[array, peer - base], moved[array].at[0, band_rows(lane)],
                three_send.at[array], three_recv.at[array], peer,
            ).start()

    for copy in own_tokens(twin):
        copy.start()

    @pl.loop(1, half_planes)
    def _(k):
        for copy in own_tokens(column(k)):
            copy.start()

    @pl.loop(1, size)
    def _(k):
        for copy in own_tokens(mate(k)):
            copy.start()

    spread(0)
    tokens_arrive(twin)

    @pl.loop(1, half_planes)
    def _(k):
        for copy in twin_tokens(column(k)):
            copy.start()

    spread(1)

    @pl.loop(1, half_planes)
    def _(k):
        tokens_arrive(column(k))
        tokens_arrive(lax.rem(column(k) + half, n))

    @pl.loop(1, planes)
    def _(shift):
        @pl.loop(1, size)
        def _(k):
            for copy in plane_tokens(lax.rem(plane + shift, planes), k):
                copy.start()

    spread(2)
    cross_over(0)
    cross_over(1)

    @pl.loop(0, planes)
    def _(other_plane):
        @pl.loop(1, size)
        def _(k):
            tokens_arrive(other_plane * size + lax.rem(seat + k, size))

    for load in loads:
        load.wait()

    step = min(256, n * rows)
    columns = 512

    @pl.loop(0, n * rows // step)
    def _(block):
        at = pl.ds(pl.multiple_of(block * step, step), step)
        both = jnp.dot(tok_all[at, :], w_gu[...], preferred_element_type=jnp.float32)
        gate_value = both[:, :LANES]
        up_value = both[:, LANES:]
        hidden[...] = (gate_value / (1.0 + jnp.exp(-gate_value)) * up_value).astype(jnp.bfloat16)
        lanes = lax.broadcasted_iota(jnp.int32, (step, LANES), 1)
        scale = jnp.sum(jnp.where(lanes == me, coef_all[at, :], 0.0), axis=1, keepdims=True)

        @pl.loop(0, width // columns)
        def _(part):
            cols = pl.ds(pl.multiple_of(part * columns, columns), columns)
            value = lax.dot_general(
                hidden[...], w_d[cols, :], (((1,), (1,)), ((), ())),
                preferred_element_type=jnp.float32,
            )
            value = value.astype(jnp.bfloat16).astype(jnp.float32)
            contrib[at, cols] = (value * scale).astype(jnp.bfloat16)

    def part_copy(k, other_plane):
        peer = mate(k)
        owner = other_plane * size + lax.rem(seat + k, size)
        return send(
            contrib.at[token_rows(owner)], part_in.at[seat, other_plane],
            part_send.at[k, other_plane], part_recv.at[seat, other_plane], peer,
        )

    def half_copy(k, kind):
        peer = column(k)
        target = peer // size if kind == 0 else lax.rem(peer // size + half_planes, planes)
        return send(
            plane_sum.at[target], half_in.at[kind, my_plane_of_half],
            half_send.at[kind, k], half_recv.at[kind, my_plane_of_half], peer,
        )

    @pl.loop(0, planes)
    def _(other_plane):
        @pl.loop(1, size)
        def _(k):
            part_copy(k, other_plane).start()

    def add_plane():
        @pl.loop(0, planes)
        def _(other_plane):
            @pl.loop(1, size)
            def _(k):
                spot = part_in.at[lax.rem(seat + k, size), other_plane]
                pltpu.make_async_copy(
                    spot, spot, part_recv.at[lax.rem(seat + k, size), other_plane]
                ).wait()

            @pl.loop(0, width // columns)
            def _(part):
                cols = pl.ds(pl.multiple_of(part * columns, columns), columns)

                def more(k, total):
                    other = lax.rem(seat + k, size)
                    return total + part_in[other, other_plane, :, cols].astype(jnp.float32)

                total = contrib[token_rows(seated(other_plane)), cols].astype(jnp.float32)
                total = lax.fori_loop(1, size, more, total)
                plane_sum[other_plane, :, cols] = total.astype(jnp.bfloat16)

        for kind in (1, 0):

            @pl.loop(1, half_planes)
            def _(k):
                half_copy(k, kind).start()

    def add_half(kind, own_plane, extra, target):
        @pl.loop(1, half_planes)
        def _(k):
            other = lax.rem(my_plane_of_half + k, half_planes)
            spot = half_in.at[kind, other]
            pltpu.make_async_copy(spot, spot, half_recv.at[kind, other]).wait()

        @pl.loop(0, width // columns)
        def _(part):
            cols = pl.ds(pl.multiple_of(part * columns, columns), columns)

            def more(k, total):
                other = lax.rem(my_plane_of_half + k, half_planes)
                return total + half_in[kind, other, :, cols].astype(jnp.float32)

            total = plane_sum[own_plane, :, cols].astype(jnp.float32)
            if extra is not None:
                total = total + extra[:, cols].astype(jnp.float32)
            target[:, cols] = lax.fori_loop(1, half_planes, more, total).astype(jnp.bfloat16)

    deliver(0)
    cross_over(2)
    add_plane()
    deliver(1)
    add_half(1, lax.rem(plane + half_planes, planes), None, cross_out)
    cross = send(cross_out, cross_in, cross_send, cross_recv, twin)
    cross.start()
    deliver(2)
    cross.wait()
    add_half(0, plane, cross_in, out)

    for copy in own_tokens(twin):
        copy.wait_send()

    @pl.loop(1, half_planes)
    def _(k):
        for copy in own_tokens(column(k)):
            copy.wait_send()
        for copy in twin_tokens(column(k)):
            copy.wait_send()
        half_copy(k, 0).wait_send()
        half_copy(k, 1).wait_send()

    @pl.loop(1, size)
    def _(k):
        for copy in own_tokens(mate(k)):
            copy.wait_send()

        @pl.loop(0, planes)
        def _(other_plane):
            part_copy(k, other_plane).wait_send()

        @pl.loop(1, planes)
        def _(shift):
            for copy in plane_tokens(lax.rem(plane + shift, planes), k):
                copy.wait_send()

    for array in range(3):
        sent = pieces[array].at[pl.ds(0, half - 1)]
        pltpu.make_async_copy(sent, sent, one_send.at[array]).wait()
        pltpu.make_async_copy(sent, sent, three_send.at[array]).wait()
        pltpu.make_async_copy(
            moved[array].at[0], moved[array].at[0], three_recv.at[array]
        ).wait()


def call_layer(n, most, which, table, tokens, coef, held_gate, held_up, held_down):
    rows, width = tokens.shape
    half = n // 2
    band = width // half
    size = near_square_root(n)
    planes = n // size
    vmem = pl.BlockSpec(memory_space=pltpu.VMEM)
    anywhere = pl.BlockSpec(memory_space=pl.ANY)
    dma = pltpu.SemaphoreType.DMA
    moved_shape = jax.ShapeDtypeStruct(held_gate.shape, held_gate.dtype)

    def block(*shape):
        return pltpu.VMEM(shape, jnp.bfloat16)

    return pl.pallas_call(
        functools.partial(layer_kernel, n, most),
        out_shape=(jax.ShapeDtypeStruct((rows, width), jnp.bfloat16),) + (moved_shape,) * 3,
        in_specs=[pl.BlockSpec(memory_space=pltpu.SMEM), vmem, vmem] + [anywhere] * 3,
        out_specs=(vmem, anywhere, anywhere, anywhere),
        scratch_shapes=[
            block(n * rows, width),
            pltpu.VMEM((n * rows, LANES), jnp.float32),
            block(width, 2 * LANES),
            block(width, LANES),
            block(half, band, LANES),
            block(half, band, LANES),
            block(half, band, LANES),
            block(most, band, LANES),
            block(most, band, LANES),
            block(most, band, LANES),
            block(3, half, band, LANES),
            block(min(256, n * rows), LANES),
            block(n * rows, width),
            block(size, planes, rows, width),
            block(planes, rows, width),
            block(2, planes // 2, rows, width),
            block(rows, width),
            block(rows, width),
            dma((3,)),
            dma((2, n)),
            dma((2, n)),
            dma((2, planes, size)),
            dma((2, n)),
            dma((3,)),
            dma((3,)),
            dma((3,)),
            dma((3,)),
            dma((3,)),
            dma((3,)),
            dma((size, planes)),
            dma((size, planes)),
            dma((2, planes // 2)),
            dma((2, planes // 2)),
            dma,
            dma,
        ],
        compiler_params=pltpu.CompilerParams(
            collective_id=which, has_side_effects=True, vmem_limit_bytes=VMEM_BYTES
        ),
    )(table, tokens, coef, held_gate, held_up, held_down)


O, I, J, K = range(4)
(
    OWN, SEAT_TOKENS, SIDE_TOKENS, SPREAD, OUTER_IN, INNER_IN, INNER_OUT, OUTER_OUT,
    COMPUTE, PAIR_ADD, SIDE_ADD, FINISH,
) = range(12)


def chunk_plan(quarter, cuts):
    plan = []
    for array in range(3):
        start = 0
        for cut in cuts[array]:
            size = quarter * cut // 16
            plan.append((array, start, size))
            start += size
        assert start == quarter
    return tuple(plan)


def line_kernel(
    n, most, plan, order, table, tok, coef, held_g, held_u, held_d, out, moved_g, moved_u, moved_d, *rest
):
    count = len(plan)
    gathered, rest = rest[:count], rest[count:]
    crossed, rest = rest[:count], rest[count:]
    (
        leaving, ordered, tok_all, coef_all, w_gu, w_d, hidden, contrib,
        pair_in, side_out, side_in, chain_in, chain_out, over_in, both_in, both_out,
        load_sem, tok_send, tok_recv,
        one_send, one_recv, two_send, two_recv, cross_send, cross_recv,
        back_send, back_recv, three_send, three_recv,
        pair_send, pair_recv, side_send, side_recv, chain_send, chain_recv,
        over_recv, both_send, both_recv,
    ) = rest
    size = 4
    last = n // size - 1
    me = lax.axis_index("expert")
    plane = me // size
    seat = me - plane * size
    half = plane // 2
    base = half * (n // 2)
    own_at = lax.rem(plane, 2) * size
    other_at = size - own_at
    inner = (plane == 1) | (plane == 2)
    outer = (plane == 0) | (plane == last)
    side = lax.rem(seat + 2, size)
    pair = seat + 1 - 2 * lax.rem(seat, 2)
    diagonal = lax.rem(pair + 2, size)
    my_row = seat // 2
    rows, width = tok.shape
    quarter = width // size
    held = (held_g, held_u, held_d)
    moved = (moved_g, moved_u, moved_d)
    plane_of = (last * half, 1 + half, last - 1 - half, last - last * half)

    def at_plane(other, other_seat):
        return other * size + other_seat

    near_outer, near_inner = at_plane(plane_of[O], seat), at_plane(plane_of[I], seat)
    far_inner = at_plane(plane_of[J], seat)
    beside, across = at_plane(plane, pair), at_plane(plane, side)

    def token_rows(owner):
        return pl.ds(pl.multiple_of(owner * rows, rows), rows)

    own_load = pltpu.make_async_copy(tok, tok_all.at[token_rows(me)], load_sem.at[3])
    own_load.start()
    barrier = pltpu.get_barrier_semaphore()

    def greet(peer):
        pl.semaphore_signal(barrier, inc=1, device_id={"expert": peer}, device_id_type=MESH)

    @pl.loop(1, size)
    def _(k):
        greet(at_plane(plane, lax.rem(seat + k, size)))

    @pl.when(outer)
    def _():
        greet(near_inner)

    @pl.when(inner)
    def _():
        greet(near_outer)
        greet(far_inner)

    loads = (
        pltpu.make_async_copy(held_g.at[0], w_gu.at[:, pl.ds(0, LANES)], load_sem.at[0]),
        pltpu.make_async_copy(held_u.at[0], w_gu.at[:, pl.ds(LANES, LANES)], load_sem.at[1]),
        pltpu.make_async_copy(held_d.at[0], w_d, load_sem.at[2]),
    )

    coef_all[token_rows(me), :] = coef[...]

    @pl.when(inner)
    def _():
        pl.semaphore_wait(barrier, size + 1)

    @pl.when(outer)
    def _():
        pl.semaphore_wait(barrier, size)

    def send(source, target, send_sem, recv_sem, peer):
        return pltpu.make_async_remote_copy(
            src_ref=source, dst_ref=target, send_sem=send_sem, recv_sem=recv_sem,
            device_id={"expert": peer}, device_id_type=MESH,
        )

    def landed(spot, sem):
        pltpu.make_async_copy(spot, spot, sem).wait()

    role_now = [True]
    sent_tokens = {True: [0, 0, 0], False: [0, 0, 0]}

    def go(role, *copies):
        for copy in copies:
            copy.start()

    def tokens_to(q, owner_seat, peer, path, own=False):
        owner_plane = plane_of[q]
        owner = at_plane(owner_plane, owner_seat)
        at = token_rows(owner)
        group = TOKEN_GROUPS[path]
        sent_tokens[role_now[0]][group] += 1
        coef_source = coef if own else coef_all.at[at]
        return (
            send(tok_all.at[at], tok_all.at[at], tok_send.at[0, group], tok_recv.at[0, owner], peer),
            send(coef_source, coef_all.at[at], tok_send.at[1, group], tok_recv.at[1, owner], peer),
        )

    def tokens_arrive(q, owner_seat):
        owner = at_plane(plane_of[q], owner_seat)
        landed(tok_all.at[token_rows(owner)], tok_recv.at[0, owner])
        landed(coef_all.at[token_rows(owner)], tok_recv.at[1, owner])

    def own_tokens(is_outer):
        own_load.wait()
        if is_outer:
            go(True, *tokens_to(O, seat, near_inner, 0, True))
        else:
            go(False, *tokens_to(I, seat, near_outer, 0, True))
            go(False, *tokens_to(I, seat, far_inner, 1, True))
        mine = O if is_outer else I
        go(is_outer, *tokens_to(mine, seat, across, 2, True))
        go(is_outer, *tokens_to(mine, seat, beside, 3, True))

    def seat_tokens(is_outer, q):
        tokens_arrive(q, seat)
        if not is_outer:
            if q == O:
                go(False, *tokens_to(q, seat, far_inner, 1))
            else:
                go(False, *tokens_to(q, seat, near_outer, 0))
        if (is_outer, q) not in ((True, I), (False, O)):
            go(is_outer, *tokens_to(q, seat, across, 2))
        go(is_outer, *tokens_to(q, seat, beside, 3))

    def side_tokens(is_outer, q):
        tokens_arrive(q, side)
        if (is_outer, q) == (True, O):
            go(True, *tokens_to(q, side, near_inner, 5))
        if (is_outer, q) == (False, I):
            go(False, *tokens_to(q, side, near_outer, 5))
        go(is_outer, *tokens_to(q, side, beside, 4))

    def band(chunk, owner):
        _, first, length = plan[chunk]
        return pl.ds(pl.multiple_of(owner * quarter + first, 16), length)

    def spread(is_outer, chunk):
        array = plan[chunk][0]
        spot = gathered[chunk].at[own_at + seat]
        pltpu.make_async_copy(held[array].at[0, band(chunk, seat)], spot, one_recv.at[chunk]).start()
        for k in (2, 1, 3):
            peer = lax.rem(seat + k, size)
            send(
                held[array].at[0, band(chunk, peer)], spot, one_send.at[0],
                one_recv.at[chunk], at_plane(plane, peer),
            ).start()

    def own_part(chunk):
        return gathered[chunk].at[pl.ds(own_at, size)]

    def other_part(chunk):
        return gathered[chunk].at[pl.ds(other_at, size)]

    def flat_at(chunk):
        return pl.ds(sum(length for _, _, length in plan[:chunk]), plan[chunk][2])

    def deliver(chunk, piece_of):
        array = plan[chunk][0]
        target = moved[array].at[0, band(chunk, seat)]
        for k in (2, 1, 3):
            peer = lax.rem(seat + k, size)
            send(
                piece_of(peer), target, three_send.at[0], three_recv.at[array],
                at_plane(plane, peer),
            ).start()
        pltpu.make_async_copy(piece_of(seat), target, three_recv.at[array]).start()

    def outer_in(is_outer, chunk):
        landed(own_part(chunk), one_recv.at[chunk])
        go(True, send(
            own_part(chunk), own_part(chunk), two_send.at[0], two_recv.at[chunk], near_inner
        ))

    def inner_in(is_outer, chunk):
        landed(own_part(chunk), one_recv.at[chunk])
        landed(other_part(chunk), two_recv.at[chunk])
        flat = flat_at(chunk)

        @pl.loop(0, most)
        def _(m):
            leaving[m, flat] = gathered[chunk][table[base + m]]

        go(False, send(
            leaving.at[:, flat], crossed[chunk], cross_send.at[0], cross_recv.at[chunk], far_inner
        ))

    def inner_out(is_outer, chunk):
        landed(crossed[chunk], cross_recv.at[chunk])
        flat = flat_at(chunk)

        @pl.loop(0, 2 * size)
        def _(place):
            at = base + place
            own = gathered[chunk][table[2 * n + at]]
            other = crossed[chunk][table[3 * n + at]]
            ordered[place, flat] = jnp.where(table[n + at] == 1, other, own)

        go(False, send(
            ordered.at[pl.ds(other_at, size), flat], own_part(chunk), back_send.at[0],
            back_recv.at[chunk], near_outer,
        ))
        deliver(chunk, lambda s: ordered.at[own_at + s, flat])

    def outer_out(is_outer, chunk):
        landed(other_part(chunk), back_recv.at[chunk])
        deliver(chunk, lambda s: gathered[chunk].at[other_at + s])

    block = size * rows
    columns = 512

    def compute(is_outer, q):
        tokens_arrive(q, pair)
        tokens_arrive(q, diagonal)
        at = pl.ds(pl.multiple_of(plane_of[q] * block, block), block)

        def more(part, both):
            depth = pl.ds(pl.multiple_of(part * quarter, quarter), quarter)
            return both + jnp.dot(
                tok_all[at, depth], w_gu[depth, :], preferred_element_type=jnp.float32
            )

        both = lax.fori_loop(0, size, more, jnp.zeros((block, 2 * LANES), jnp.float32))
        gate_value = both[:, :LANES]
        up_value = both[:, LANES:]
        hidden[...] = (gate_value / (1.0 + jnp.exp(-gate_value)) * up_value).astype(jnp.bfloat16)
        lanes = lax.broadcasted_iota(jnp.int32, (block, LANES), 1)
        scale = jnp.sum(jnp.where(lanes == me, coef_all[at, :], 0.0), axis=1, keepdims=True)

        @pl.loop(0, width // columns)
        def _(part):
            cols = pl.ds(pl.multiple_of(part * columns, columns), columns)
            value = lax.dot_general(
                hidden[...], w_d[cols, :], (((1,), (1,)), ((), ())),
                preferred_element_type=jnp.float32,
            )
            value = value.astype(jnp.bfloat16).astype(jnp.float32)
            contrib[at, cols] = (value * scale).astype(jnp.bfloat16)

        for row in range(2):
            owner = at_plane(plane_of[q], row * 2 + lax.rem(pair, 2))
            go(is_outer, send(
                contrib.at[token_rows(owner)], pair_in.at[plane_of[q], row],
                pair_send.at[0], pair_recv.at[plane_of[q], row], beside,
            ))

    def add_rows(parts, target):
        @pl.loop(0, width // columns)
        def _(part):
            cols = pl.ds(pl.multiple_of(part * columns, columns), columns)
            total = sum(source(cols).astype(jnp.float32) for source in parts)
            target[:, cols] = total.astype(jnp.bfloat16)

    def chip_part(q, mine):
        owner_seat, row = (seat, my_row) if mine else (side, 1 - my_row)
        return [
            lambda cols: contrib[token_rows(at_plane(plane_of[q], owner_seat)), cols],
            lambda cols: pair_in[plane_of[q], row, :, cols],
        ]

    def taken(source, sem):
        landed(source, sem)
        return lambda cols: source[:, cols]

    def side_taken(q):
        return taken(side_in.at[plane_of[q]], side_recv.at[plane_of[q]])

    def chain_taken(q):
        return taken(chain_in.at[plane_of[q]], chain_recv.at[plane_of[q]])

    def over_taken(q):
        return taken(over_in.at[plane_of[q]], over_recv.at[plane_of[q]])

    def both_taken():
        return taken(both_in, both_recv)

    def pass_on(is_outer, q, parts):
        at = plane_of[q]
        add_rows(parts, chain_out.at[at])
        if is_outer:
            copy = send(chain_out.at[at], chain_in.at[at], chain_send.at[0], chain_recv.at[at], near_inner)
        elif q == O:
            copy = send(chain_out.at[at], chain_in.at[at], chain_send.at[0], chain_recv.at[at], near_outer)
        else:
            copy = send(chain_out.at[at], over_in.at[at], chain_send.at[0], over_recv.at[at], far_inner)
        go(is_outer, copy)

    def pass_both(is_outer, q):
        add_rows(chip_part(q, False), both_out)
        go(is_outer, send(both_out, both_in, both_send, both_recv, near_inner if is_outer else near_outer))

    def pair_add(is_outer, q):
        at = plane_of[q]
        for row in range(2):
            landed(pair_in.at[at, row], pair_recv.at[at, row])
        if (is_outer, q) == (True, I):
            pass_both(True, q)
            pass_on(True, q, chip_part(q, True))
            return
        if (is_outer, q) == (False, O):
            pass_both(False, q)
            return
        parts = chip_part(q, False)
        if q == (O if is_outer else I):
            parts = parts + [both_taken()]
        add_rows(parts, side_out.at[at])
        go(is_outer, send(side_out.at[at], side_in.at[at], side_send.at[0], side_recv.at[at], across))

    def side_add(is_outer, q):
        parts = chip_part(q, True)
        if is_outer or q != O:
            parts.append(side_taken(q))
        if not is_outer:
            parts.append(over_taken(q) if q == O else chain_taken(q))
        pass_on(is_outer, q, parts)

    def finish_rows(is_outer):
        q = O if is_outer else I
        parts = chip_part(q, True) + [side_taken(q), chain_taken(q)]
        if not is_outer:
            parts.append(over_taken(q))
        add_rows(parts, out)

    steps = (
        own_tokens, seat_tokens, side_tokens, spread, outer_in, inner_in, inner_out, outer_out,
        compute, pair_add, side_add, finish_rows,
    )

    for is_outer, role in ((True, outer), (False, inner)):

        @pl.when(role)
        def _():
            role_now[0] = is_outer
            loaded = False
            for place, (name, *arguments) in enumerate(order[0 if is_outer else 1]):
                if name == COMPUTE and not loaded:
                    for load in loads:
                        load.wait()
                    loaded = True
                steps[name](is_outer, *arguments)
                if place == START_LOADS:
                    for load in loads:
                        load.start()
            for group, number in enumerate(sent_tokens[is_outer]):
                at = pl.ds(0, number * rows)
                landed(tok_all.at[at], tok_send.at[0, group])
                landed(coef_all.at[at], tok_send.at[1, group])
            if is_outer:
                landed(ordered.at[pl.ds(0, size)], two_send.at[0])
            else:
                landed(leaving, cross_send.at[0])
                landed(ordered.at[pl.ds(0, size)], back_send.at[0])

    landed(pair_in, pair_send.at[0])
    landed(side_out.at[pl.ds(0, 3)], side_send.at[0])
    landed(chain_out.at[pl.ds(0, 3)], chain_send.at[0])
    landed(both_out, both_send)
    landed(ordered.at[pl.ds(0, size - 1)], one_send.at[0])
    landed(ordered.at[pl.ds(0, size - 1)], three_send.at[0])

    for array in range(3):
        landed(moved[array].at[0], three_recv.at[array])


START_LOADS = 6
TOKEN_GROUPS = (0, 0, 2, 1, 1, 0)
LINE_VMEM_BYTES = 59_000_000
LINE_ORDERS = {
    4: (
        ((1, 1, 2, 2, 2, 2, 2, 2, 2), (2, 2, 2, 2, 2, 2, 2, 2), (2, 2, 2, 2, 2, 2, 1, 1, 1, 1)),
        (
            (
            (SPREAD, 0), (SPREAD, 1), (SPREAD, 2), (SPREAD, 3), (OWN,), (OUTER_IN, 0),
            (OUTER_IN, 1), (SPREAD, 4), (SEAT_TOKENS, I), (OUTER_IN, 2), (SPREAD, 5),
            (OUTER_IN, 3), (SPREAD, 6), (SPREAD, 7), (SIDE_TOKENS, O), (SPREAD, 8), (OUTER_IN, 4),
            (SPREAD, 9), (SEAT_TOKENS, J), (OUTER_IN, 5), (OUTER_IN, 6), (SEAT_TOKENS, K),
            (OUTER_IN, 7), (OUTER_OUT, 0), (OUTER_IN, 8), (OUTER_OUT, 1), (OUTER_IN, 9),
            (SPREAD, 10), (OUTER_OUT, 2), (SPREAD, 11), (OUTER_OUT, 3), (SPREAD, 12),
            (OUTER_IN, 10), (SPREAD, 13), (SPREAD, 14), (OUTER_OUT, 4), (OUTER_IN, 11),
            (SPREAD, 15), (OUTER_OUT, 5), (OUTER_IN, 12), (OUTER_IN, 13), (SPREAD, 16),
            (OUTER_OUT, 6), (OUTER_IN, 14), (SPREAD, 17), (OUTER_OUT, 7), (OUTER_IN, 15),
            (SPREAD, 18), (OUTER_OUT, 8), (OUTER_IN, 16), (SPREAD, 19), (OUTER_OUT, 9),
            (OUTER_IN, 17), (SPREAD, 20), (OUTER_OUT, 10), (OUTER_IN, 18), (SPREAD, 21),
            (OUTER_OUT, 11), (OUTER_IN, 19), (SPREAD, 22), (OUTER_OUT, 12), (OUTER_IN, 20),
            (SPREAD, 23), (OUTER_OUT, 13), (OUTER_IN, 21), (SPREAD, 24), (SPREAD, 25),
            (OUTER_OUT, 14), (OUTER_IN, 22), (SPREAD, 26), (OUTER_IN, 23), (OUTER_OUT, 15),
            (SIDE_TOKENS, K), (OUTER_IN, 24), (COMPUTE, K), (OUTER_IN, 25), (OUTER_OUT, 16),
            (SIDE_TOKENS, J), (OUTER_IN, 26), (PAIR_ADD, K), (COMPUTE, J), (OUTER_OUT, 17),
            (PAIR_ADD, J), (OUTER_OUT, 18), (SIDE_TOKENS, I), (SIDE_ADD, K), (COMPUTE, O),
            (COMPUTE, I), (PAIR_ADD, O), (OUTER_OUT, 19), (SIDE_ADD, J), (OUTER_OUT, 20),
            (PAIR_ADD, I), (OUTER_OUT, 21), (OUTER_OUT, 22), (OUTER_OUT, 23), (OUTER_OUT, 24),
            (OUTER_OUT, 25), (OUTER_OUT, 26), (FINISH,),
            ),
            (
            (OWN,), (SPREAD, 0), (SPREAD, 1), (SPREAD, 2), (SPREAD, 3), (SPREAD, 4),
            (SIDE_TOKENS, I), (SEAT_TOKENS, J), (SEAT_TOKENS, O), (INNER_IN, 0), (INNER_IN, 1),
            (SPREAD, 5), (SEAT_TOKENS, K), (INNER_IN, 2), (INNER_OUT, 0), (INNER_OUT, 1),
            (INNER_IN, 3), (SPREAD, 6), (INNER_OUT, 2), (SIDE_TOKENS, O), (SPREAD, 7),
            (COMPUTE, O), (SIDE_TOKENS, K), (SIDE_TOKENS, J), (INNER_OUT, 3), (INNER_IN, 4),
            (PAIR_ADD, O), (SPREAD, 8), (COMPUTE, K), (SPREAD, 9), (INNER_IN, 5), (SPREAD, 10),
            (INNER_OUT, 4), (INNER_IN, 6), (SPREAD, 11), (INNER_OUT, 5), (INNER_IN, 7),
            (SPREAD, 12), (INNER_OUT, 6), (INNER_IN, 8), (SPREAD, 13), (INNER_OUT, 7),
            (INNER_IN, 9), (SPREAD, 14), (INNER_OUT, 8), (INNER_IN, 10), (SPREAD, 15),
            (INNER_OUT, 9), (INNER_IN, 11), (SPREAD, 16), (COMPUTE, I), (INNER_OUT, 10),
            (INNER_IN, 12), (SPREAD, 17), (INNER_OUT, 11), (INNER_IN, 13), (SPREAD, 18),
            (INNER_OUT, 12), (INNER_IN, 14), (SPREAD, 19), (INNER_OUT, 13), (COMPUTE, J),
            (INNER_IN, 15), (SPREAD, 20), (INNER_OUT, 14), (PAIR_ADD, J), (INNER_IN, 16),
            (INNER_OUT, 15), (INNER_IN, 17), (SPREAD, 21), (INNER_OUT, 16), (INNER_IN, 18),
            (SPREAD, 22), (INNER_OUT, 17), (INNER_IN, 19), (SPREAD, 23), (INNER_OUT, 18),
            (INNER_IN, 20), (SPREAD, 24), (SPREAD, 25), (INNER_OUT, 19), (INNER_IN, 21),
            (SPREAD, 26), (PAIR_ADD, K), (INNER_OUT, 20), (INNER_IN, 22), (INNER_IN, 23),
            (INNER_OUT, 21), (INNER_IN, 24), (INNER_IN, 25), (INNER_OUT, 22), (INNER_IN, 26),
            (INNER_OUT, 23), (INNER_OUT, 24), (SIDE_ADD, K), (INNER_OUT, 25), (INNER_OUT, 26),
            (SIDE_ADD, J), (SIDE_ADD, O), (PAIR_ADD, I), (FINISH,),
            ),
        ),
    ),
    5: (
        ((1, 1, 2, 2, 2, 2, 2, 2, 2), (2, 2, 2, 2, 2, 2, 2, 2), (2, 2, 2, 2, 2, 2, 1, 1, 1, 1)),
        (
            (
            (SPREAD, 0), (SPREAD, 1), (SPREAD, 2), (OWN,), (OUTER_IN, 0), (SPREAD, 3),
            (OUTER_IN, 1), (SPREAD, 4), (OUTER_IN, 2), (SPREAD, 5), (SPREAD, 6), (SPREAD, 7),
            (OUTER_IN, 3), (SPREAD, 8), (OUTER_IN, 4), (SPREAD, 9), (OUTER_IN, 5), (SPREAD, 10),
            (SEAT_TOKENS, K), (OUTER_IN, 6), (OUTER_OUT, 0), (OUTER_IN, 7), (OUTER_OUT, 1),
            (OUTER_IN, 8), (OUTER_IN, 9), (SPREAD, 11), (OUTER_IN, 10), (OUTER_OUT, 2),
            (SIDE_TOKENS, K), (SPREAD, 12), (SPREAD, 13), (OUTER_OUT, 3), (OUTER_IN, 11),
            (SPREAD, 14), (SIDE_TOKENS, O), (OUTER_OUT, 4), (COMPUTE, O), (SPREAD, 15),
            (OUTER_IN, 12), (OUTER_IN, 13), (SPREAD, 16), (OUTER_OUT, 5), (OUTER_IN, 14),
            (SPREAD, 17), (SPREAD, 18), (OUTER_IN, 15), (SPREAD, 19), (OUTER_OUT, 6),
            (OUTER_IN, 16), (SPREAD, 20), (OUTER_OUT, 7), (OUTER_IN, 17), (OUTER_IN, 18),
            (SPREAD, 21), (OUTER_OUT, 8), (OUTER_IN, 19), (SPREAD, 22), (OUTER_IN, 20),
            (SPREAD, 23), (OUTER_OUT, 9), (SIDE_TOKENS, I), (OUTER_IN, 21), (SPREAD, 24),
            (SPREAD, 25), (OUTER_OUT, 10), (SEAT_TOKENS, I), (COMPUTE, I), (SPREAD, 26),
            (OUTER_IN, 22), (OUTER_IN, 23), (OUTER_IN, 24), (PAIR_ADD, I), (OUTER_IN, 25),
            (OUTER_OUT, 11), (COMPUTE, K), (OUTER_IN, 26), (OUTER_OUT, 12), (PAIR_ADD, K),
            (OUTER_OUT, 13), (SIDE_ADD, K), (OUTER_OUT, 14), (OUTER_OUT, 15), (PAIR_ADD, O),
            (OUTER_OUT, 16), (SEAT_TOKENS, J), (OUTER_OUT, 17), (SIDE_TOKENS, J), (OUTER_OUT, 18),
            (COMPUTE, J), (OUTER_OUT, 19), (PAIR_ADD, J), (OUTER_OUT, 20), (SIDE_ADD, J),
            (OUTER_OUT, 21), (OUTER_OUT, 22), (OUTER_OUT, 23), (OUTER_OUT, 24), (OUTER_OUT, 25),
            (OUTER_OUT, 26), (FINISH,),
            ),
            (
            (OWN,), (SPREAD, 0), (SPREAD, 1), (SPREAD, 2), (SPREAD, 3), (SIDE_TOKENS, I),
            (SEAT_TOKENS, O), (SPREAD, 4), (INNER_IN, 0), (SPREAD, 5), (INNER_IN, 1), (SPREAD, 6),
            (SEAT_TOKENS, K), (INNER_IN, 2), (INNER_OUT, 0), (INNER_OUT, 1), (SPREAD, 7),
            (INNER_IN, 3), (SPREAD, 8), (SIDE_TOKENS, K), (INNER_OUT, 2), (INNER_IN, 4),
            (SPREAD, 9), (SPREAD, 10), (INNER_IN, 5), (INNER_OUT, 3), (COMPUTE, I), (SPREAD, 11),
            (INNER_IN, 6), (INNER_OUT, 4), (SPREAD, 12), (INNER_IN, 7), (SPREAD, 13),
            (INNER_OUT, 5), (INNER_IN, 8), (SPREAD, 14), (COMPUTE, K), (INNER_IN, 9), (SPREAD, 15),
            (SPREAD, 16), (INNER_OUT, 6), (INNER_IN, 10), (INNER_OUT, 7), (SPREAD, 17),
            (INNER_IN, 11), (INNER_OUT, 8), (SPREAD, 18), (SIDE_TOKENS, O), (COMPUTE, O),
            (SPREAD, 19), (SPREAD, 20), (INNER_OUT, 9), (INNER_IN, 12), (INNER_OUT, 10),
            (INNER_IN, 13), (PAIR_ADD, O), (SPREAD, 21), (SPREAD, 22), (INNER_IN, 14),
            (INNER_OUT, 11), (SPREAD, 23), (INNER_IN, 15), (SPREAD, 24), (INNER_OUT, 12),
            (SPREAD, 25), (INNER_IN, 16), (SPREAD, 26), (INNER_OUT, 13), (INNER_IN, 17),
            (INNER_OUT, 14), (PAIR_ADD, K), (INNER_IN, 18), (INNER_IN, 19), (INNER_OUT, 15),
            (INNER_IN, 20), (INNER_OUT, 16), (INNER_IN, 21), (SEAT_TOKENS, J), (INNER_OUT, 17),
            (INNER_IN, 22), (INNER_IN, 23), (SIDE_TOKENS, J), (INNER_OUT, 18), (INNER_IN, 24),
            (COMPUTE, J), (PAIR_ADD, I), (INNER_OUT, 19), (PAIR_ADD, J), (INNER_OUT, 20),
            (INNER_IN, 25), (INNER_IN, 26), (INNER_OUT, 21), (SIDE_ADD, K), (INNER_OUT, 22),
            (INNER_OUT, 23), (INNER_OUT, 24), (SIDE_ADD, J), (INNER_OUT, 25), (INNER_OUT, 26),
            (SIDE_ADD, O), (FINISH,),
            ),
        ),
    ),
    6: (
        ((1, 1, 2, 2, 2, 2, 2, 2, 2), (2, 2, 2, 2, 2, 2, 2, 2), (2, 2, 2, 2, 2, 2, 2, 1, 1)),
        (
            (
            (SPREAD, 0), (SPREAD, 1), (SPREAD, 2), (OWN,), (OUTER_IN, 0), (SPREAD, 3),
            (OUTER_IN, 1), (SPREAD, 4), (OUTER_IN, 2), (SPREAD, 5), (SPREAD, 6), (SPREAD, 7),
            (OUTER_IN, 3), (SPREAD, 8), (OUTER_IN, 4), (SPREAD, 9), (OUTER_IN, 5), (SPREAD, 10),
            (OUTER_IN, 6), (OUTER_OUT, 0), (OUTER_IN, 7), (SPREAD, 11), (OUTER_OUT, 1),
            (OUTER_IN, 8), (SPREAD, 12), (OUTER_IN, 9), (SPREAD, 13), (OUTER_IN, 10), (SPREAD, 14),
            (SIDE_TOKENS, O), (OUTER_IN, 11), (SPREAD, 15), (OUTER_OUT, 2), (OUTER_IN, 12),
            (SPREAD, 16), (OUTER_IN, 13), (SPREAD, 17), (OUTER_OUT, 3), (OUTER_IN, 14),
            (OUTER_IN, 15), (SPREAD, 18), (SPREAD, 19), (OUTER_OUT, 4), (OUTER_IN, 16),
            (OUTER_IN, 17), (SPREAD, 20), (SPREAD, 21), (OUTER_OUT, 5), (OUTER_IN, 18),
            (OUTER_IN, 19), (SPREAD, 22), (SPREAD, 23), (OUTER_OUT, 6), (OUTER_IN, 20),
            (OUTER_IN, 21), (SPREAD, 24), (SPREAD, 25), (OUTER_OUT, 7), (OUTER_IN, 22),
            (OUTER_IN, 23), (OUTER_IN, 24), (SEAT_TOKENS, I), (OUTER_OUT, 8), (OUTER_IN, 25),
            (OUTER_OUT, 9), (OUTER_OUT, 10), (OUTER_OUT, 11), (SEAT_TOKENS, K), (OUTER_OUT, 12),
            (COMPUTE, O), (SIDE_TOKENS, K), (OUTER_OUT, 13), (COMPUTE, K), (PAIR_ADD, K),
            (OUTER_OUT, 14), (SIDE_TOKENS, I), (COMPUTE, I), (SIDE_ADD, K), (SEAT_TOKENS, J),
            (PAIR_ADD, I), (OUTER_OUT, 15), (SIDE_TOKENS, J), (COMPUTE, J), (PAIR_ADD, O),
            (PAIR_ADD, J), (OUTER_OUT, 16), (OUTER_OUT, 17), (SIDE_ADD, J), (OUTER_OUT, 18),
            (OUTER_OUT, 19), (OUTER_OUT, 20), (OUTER_OUT, 21), (OUTER_OUT, 22), (OUTER_OUT, 23),
            (OUTER_OUT, 24), (OUTER_OUT, 25), (FINISH,),
            ),
            (
            (SPREAD, 0), (SPREAD, 1), (SPREAD, 2), (OWN,), (SPREAD, 3), (SEAT_TOKENS, O),
            (SPREAD, 4), (INNER_IN, 0), (SPREAD, 5), (INNER_IN, 1), (SPREAD, 6), (SPREAD, 7),
            (INNER_IN, 2), (SPREAD, 8), (INNER_OUT, 0), (SPREAD, 9), (INNER_OUT, 1), (INNER_IN, 3),
            (SPREAD, 10), (SPREAD, 11), (INNER_IN, 4), (INNER_OUT, 2), (SPREAD, 12), (INNER_IN, 5),
            (SPREAD, 13), (INNER_OUT, 3), (INNER_IN, 6), (SPREAD, 14), (SPREAD, 15), (INNER_IN, 7),
            (INNER_OUT, 4), (SPREAD, 16), (INNER_IN, 8), (SPREAD, 17), (INNER_OUT, 5),
            (INNER_IN, 9), (SPREAD, 18), (SPREAD, 19), (INNER_IN, 10), (INNER_OUT, 6),
            (SPREAD, 20), (SIDE_TOKENS, O), (SPREAD, 21), (INNER_OUT, 7), (INNER_IN, 11),
            (SPREAD, 22), (SPREAD, 23), (INNER_IN, 12), (INNER_OUT, 8), (SPREAD, 24),
            (INNER_IN, 13), (SPREAD, 25), (INNER_OUT, 9), (INNER_IN, 14), (SEAT_TOKENS, K),
            (INNER_IN, 15), (INNER_OUT, 10), (INNER_IN, 16), (INNER_OUT, 11), (INNER_IN, 17),
            (SIDE_TOKENS, K), (COMPUTE, K), (INNER_OUT, 12), (INNER_IN, 18), (PAIR_ADD, K),
            (INNER_IN, 19), (INNER_OUT, 13), (INNER_IN, 20), (INNER_IN, 21), (INNER_OUT, 14),
            (INNER_IN, 22), (SIDE_TOKENS, I), (COMPUTE, O), (COMPUTE, I), (SEAT_TOKENS, J),
            (INNER_OUT, 15), (PAIR_ADD, O), (INNER_IN, 23), (INNER_IN, 24), (INNER_IN, 25),
            (INNER_OUT, 16), (SIDE_TOKENS, J), (COMPUTE, J), (INNER_OUT, 17), (PAIR_ADD, J),
            (SIDE_ADD, K), (INNER_OUT, 18), (PAIR_ADD, I), (INNER_OUT, 19), (INNER_OUT, 20),
            (SIDE_ADD, J), (INNER_OUT, 21), (INNER_OUT, 22), (INNER_OUT, 23), (INNER_OUT, 24),
            (INNER_OUT, 25), (SIDE_ADD, O), (FINISH,),
            ),
        ),
    ),
    8: (
        ((1, 1, 2, 2, 2, 2, 2, 2, 2), (2, 2, 2, 2, 2, 2, 2, 2), (2, 2, 2, 2, 2, 2, 2, 1, 1)),
        (
            (
            (SPREAD, 0), (OWN,), (OUTER_IN, 0), (SPREAD, 1), (SPREAD, 2), (SEAT_TOKENS, I),
            (SPREAD, 3), (OUTER_IN, 1), (SPREAD, 4), (OUTER_IN, 2), (SPREAD, 5), (OUTER_IN, 3),
            (SPREAD, 6), (OUTER_IN, 4), (SPREAD, 7), (OUTER_IN, 5), (SPREAD, 8), (OUTER_IN, 6),
            (SPREAD, 9), (OUTER_IN, 7), (SPREAD, 10), (OUTER_OUT, 0), (OUTER_IN, 8), (SPREAD, 11),
            (OUTER_OUT, 1), (OUTER_IN, 9), (OUTER_IN, 10), (SPREAD, 12), (SPREAD, 13),
            (OUTER_IN, 11), (SPREAD, 14), (OUTER_IN, 12), (SPREAD, 15), (OUTER_OUT, 2),
            (OUTER_IN, 13), (OUTER_IN, 14), (SPREAD, 16), (OUTER_IN, 15), (SPREAD, 17),
            (SPREAD, 18), (OUTER_OUT, 3), (OUTER_IN, 16), (OUTER_IN, 17), (SPREAD, 19),
            (OUTER_IN, 18), (SPREAD, 20), (SPREAD, 21), (OUTER_OUT, 4), (OUTER_IN, 19),
            (OUTER_IN, 20), (SPREAD, 22), (OUTER_IN, 21), (SPREAD, 23), (SPREAD, 24), (SPREAD, 25),
            (OUTER_OUT, 5), (OUTER_IN, 22), (OUTER_IN, 23), (OUTER_IN, 24), (OUTER_IN, 25),
            (SEAT_TOKENS, K), (OUTER_OUT, 6), (SIDE_TOKENS, K), (COMPUTE, K), (OUTER_OUT, 7),
            (SIDE_TOKENS, O), (PAIR_ADD, K), (COMPUTE, O), (OUTER_OUT, 8), (SIDE_ADD, K),
            (SIDE_TOKENS, I), (COMPUTE, I), (PAIR_ADD, I), (OUTER_OUT, 9), (SEAT_TOKENS, J),
            (OUTER_OUT, 10), (SIDE_TOKENS, J), (COMPUTE, J), (OUTER_OUT, 11), (PAIR_ADD, J),
            (SIDE_ADD, J), (OUTER_OUT, 12), (PAIR_ADD, O), (OUTER_OUT, 13), (OUTER_OUT, 14),
            (OUTER_OUT, 15), (OUTER_OUT, 16), (OUTER_OUT, 17), (OUTER_OUT, 18), (OUTER_OUT, 19),
            (OUTER_OUT, 20), (OUTER_OUT, 21), (OUTER_OUT, 22), (OUTER_OUT, 23), (OUTER_OUT, 24),
            (OUTER_OUT, 25), (FINISH,),
            ),
            (
            (OWN,), (SPREAD, 0), (SPREAD, 1), (SPREAD, 2), (SEAT_TOKENS, O), (SPREAD, 3),
            (INNER_IN, 0), (SPREAD, 4), (SPREAD, 5), (INNER_IN, 1), (SPREAD, 6), (SIDE_TOKENS, I),
            (SPREAD, 7), (COMPUTE, I), (INNER_OUT, 0), (INNER_IN, 2), (SPREAD, 8), (SPREAD, 9),
            (INNER_OUT, 1), (INNER_IN, 3), (SPREAD, 10), (INNER_IN, 4), (SPREAD, 11), (SPREAD, 12),
            (INNER_OUT, 2), (INNER_IN, 5), (SPREAD, 13), (INNER_IN, 6), (SPREAD, 14), (SPREAD, 15),
            (INNER_OUT, 3), (INNER_IN, 7), (SPREAD, 16), (INNER_IN, 8), (SPREAD, 17), (SPREAD, 18),
            (INNER_OUT, 4), (INNER_IN, 9), (SPREAD, 19), (INNER_IN, 10), (SPREAD, 20),
            (SPREAD, 21), (INNER_OUT, 5), (SEAT_TOKENS, J), (INNER_IN, 11), (INNER_IN, 12),
            (SEAT_TOKENS, K), (INNER_OUT, 6), (INNER_IN, 13), (SIDE_TOKENS, J), (COMPUTE, J),
            (INNER_IN, 14), (SPREAD, 22), (SIDE_TOKENS, K), (PAIR_ADD, J), (COMPUTE, K),
            (INNER_OUT, 7), (INNER_IN, 15), (INNER_IN, 16), (SPREAD, 23), (SPREAD, 24),
            (INNER_OUT, 8), (INNER_IN, 17), (SPREAD, 25), (INNER_IN, 18), (INNER_OUT, 9),
            (INNER_IN, 19), (INNER_IN, 20), (INNER_OUT, 10), (INNER_IN, 21), (INNER_IN, 22),
            (INNER_OUT, 11), (INNER_IN, 23), (PAIR_ADD, K), (INNER_IN, 24), (INNER_IN, 25),
            (INNER_OUT, 12), (SIDE_TOKENS, O), (COMPUTE, O), (SIDE_ADD, K), (PAIR_ADD, O),
            (INNER_OUT, 13), (PAIR_ADD, I), (INNER_OUT, 14), (SIDE_ADD, J), (INNER_OUT, 15),
            (INNER_OUT, 16), (INNER_OUT, 17), (INNER_OUT, 18), (INNER_OUT, 19), (INNER_OUT, 20),
            (INNER_OUT, 21), (INNER_OUT, 22), (INNER_OUT, 23), (INNER_OUT, 24), (INNER_OUT, 25),
            (SIDE_ADD, O), (FINISH,),
            ),
        ),
    ),
}


def call_line(n, most, which, table, tokens, coef, held_gate, held_up, held_down):
    rows, width = tokens.shape
    size = 4
    planes = n // size
    quarter = width // size
    cuts, order = LINE_ORDERS[most]
    plan = chunk_plan(quarter, cuts)
    count = len(plan)
    vmem = pl.BlockSpec(memory_space=pltpu.VMEM)
    anywhere = pl.BlockSpec(memory_space=pl.ANY)
    dma = pltpu.SemaphoreType.DMA
    moved_shape = jax.ShapeDtypeStruct(held_gate.shape, held_gate.dtype)

    def block(*shape):
        return pltpu.VMEM(shape, jnp.bfloat16)

    return pl.pallas_call(
        functools.partial(line_kernel, n, most, plan, order),
        out_shape=(jax.ShapeDtypeStruct((rows, width), jnp.bfloat16),) + (moved_shape,) * 3,
        in_specs=[pl.BlockSpec(memory_space=pltpu.SMEM), anywhere, vmem] + [anywhere] * 3,
        out_specs=(vmem, anywhere, anywhere, anywhere),
        scratch_shapes=[
            *(block(2 * size, length, LANES) for _, _, length in plan),
            *(block(most, length, LANES) for _, _, length in plan),
            block(most, 3 * quarter, LANES),
            block(2 * size, 3 * quarter, LANES),
            block(n * rows, width),
            pltpu.VMEM((n * rows, LANES), jnp.float32),
            block(width, 2 * LANES),
            block(width, LANES),
            block(size * rows, LANES),
            block(n * rows, width),
            block(planes, 2, rows, width),
            block(planes, rows, width),
            block(planes, rows, width),
            block(planes, rows, width),
            block(planes, rows, width),
            block(planes, rows, width),
            block(rows, width),
            block(rows, width),
            dma((4,)),
            dma((2, 3)),
            dma((2, n)),
            dma((1,)),
            dma((count,)),
            dma((1,)),
            dma((count,)),
            dma((1,)),
            dma((count,)),
            dma((1,)),
            dma((count,)),
            dma((1,)),
            dma((3,)),
            dma((1,)),
            dma((planes, 2)),
            dma((1,)),
            dma((planes,)),
            dma((1,)),
            dma((planes,)),
            dma((planes,)),
            dma,
            dma,
        ],
        compiler_params=pltpu.CompilerParams(
            collective_id=which, has_side_effects=True, vmem_limit_bytes=LINE_VMEM_BYTES
        ),
    )(table, tokens, coef, held_gate, held_up, held_down)


def plan_kernel(n, levels, old, new, ids, logits, table, level, coef, target):
    half = n // 2
    blocks = n // EXPERTS
    rows = coef.shape[0]

    @pl.loop(0, n)
    def _(slot):
        target[old[slot]] = new[slot]

    @pl.loop(0, half)
    def _(place):
        table[place] = 0
        table[half + place] = 0

    crossing = jnp.int32(0)
    for side in range(2):

        def place_one(lane, turn):
            goes_to = target[side * half + lane]
            crosses = ((goes_to >= half).astype(jnp.int32) + side) % 2

            @pl.when(crosses == 1)
            def _():
                table[side * half + turn] = lane

            table[n + goes_to] = crosses
            table[2 * n + goes_to] = (1 - crosses) * lane
            table[3 * n + goes_to] = crosses * turn
            return turn + crosses

        crossing = lax.fori_loop(0, half, place_one, jnp.int32(0))
    level[0] = sum((crossing > most).astype(jnp.int32) for most in levels[:-1])

    lanes = lax.broadcasted_iota(jnp.int32, (rows, LANES), 1)
    expert_at = jnp.full((rows, LANES), -1, jnp.int32)
    for slot in range(n):
        expert_at = jnp.where(lanes == old[slot], slot // blocks, expert_at)
    eye = lax.broadcasted_iota(jnp.int32, (rows, rows), 0) == lax.broadcasted_iota(
        jnp.int32, (rows, rows), 1
    )

    def column(ref, row):
        return jnp.sum(jnp.where(eye, ref[row : row + 1, :], 0), axis=1, keepdims=True)

    first, second = column(logits, 0), column(logits, 1)
    first_weight = 1.0 / (1.0 + jnp.exp(second - first))
    second_weight = 1.0 / (1.0 + jnp.exp(first - second))
    total = jnp.where(column(ids, 0) == expert_at, first_weight, 0.0)
    coef[...] = total + jnp.where(column(ids, 1) == expert_at, second_weight, 0.0)


def write_kernel(*refs):
    sources, targets, held, sems, held_sems = refs[:4], refs[4:8], refs[8], refs[9], refs[10]
    parts = held_sems.shape[0]
    length = held.shape[0] // parts
    copies = [
        pltpu.make_async_copy(source, target, sems.at[at])
        for at, (source, target) in enumerate(zip(sources[:3], targets[:3]))
    ]
    taken, given = [], []
    for part in range(parts):
        at = pl.ds(part * length, length)
        taken.append(pltpu.make_async_copy(sources[3].at[0, at], held.at[at], held_sems.at[part, 0]))
        given.append(pltpu.make_async_copy(held.at[at], targets[3].at[0, at], held_sems.at[part, 1]))
    for copy in taken + copies:
        copy.start()
    for first, second in zip(taken, given):
        first.wait()
        second.start()
    for copy in copies + given:
        copy.wait()


def line_layer(
    tokens, route_ids, route_logits, old_place, new_place, held_gate, held_up, held_down
):
    n = lax.axis_size("expert")
    levels = sorted(LINE_ORDERS)
    rows = tokens.shape[0]
    smem = pl.BlockSpec(memory_space=pltpu.SMEM)
    vmem = pl.BlockSpec(memory_space=pltpu.VMEM)
    table, level, coef = pl.pallas_call(
        functools.partial(plan_kernel, n, levels),
        out_shape=(
            jax.ShapeDtypeStruct((4 * n,), jnp.int32),
            jax.ShapeDtypeStruct((1,), jnp.int32),
            jax.ShapeDtypeStruct((rows, LANES), jnp.float32),
        ),
        in_specs=[smem, smem, vmem, vmem],
        out_specs=(smem, smem, vmem),
        scratch_shapes=[pltpu.SMEM((n,), jnp.int32)],
    )(old_place, new_place, route_ids.T, route_logits.T)
    branches = [functools.partial(call_line, n, most, i) for i, most in enumerate(levels)]
    results = lax.switch(level[0], branches, table, tokens, coef, held_gate, held_up, held_down)
    anywhere = pl.BlockSpec(memory_space=pl.ANY)
    return pl.pallas_call(
        write_kernel,
        out_shape=tuple(jax.ShapeDtypeStruct(array.shape, array.dtype) for array in results),
        in_specs=[anywhere] * 4,
        out_specs=(anywhere,) * 4,
        scratch_shapes=[
            pltpu.VMEM(held_down.shape[1:], held_down.dtype),
            pltpu.SemaphoreType.DMA((3,)),
            pltpu.SemaphoreType.DMA((4, 2)),
        ],
    )(*results)


def per_device(
    tokens, route_ids, route_logits, old_place, new_place, held_gate, held_up, held_down
):
    n = lax.axis_size("expert")
    if n == 16 and tokens.shape[1] % 512 == 0:
        return line_layer(
            tokens, route_ids, route_logits, old_place, new_place, held_gate, held_up, held_down
        )
    half = n // 2
    device_ids = jnp.arange(n, dtype=jnp.int32)
    blocks = n // EXPERTS
    at_old = (old_place[:, None] == device_ids[None, :]).astype(jnp.int32)
    dest_of = jnp.sum(at_old * new_place[:, None], axis=0)
    expert_at = jnp.sum(at_old * device_ids[:, None], axis=0) // blocks
    half_of = device_ids // half
    crosses = (dest_of // half != half_of).astype(jnp.int32)
    earlier = (half_of[:, None] == half_of[None, :]) & (device_ids[:, None] < device_ids[None, :])
    turn = jnp.sum(earlier.astype(jnp.int32) * crosses[:, None], axis=0)
    lane_of = device_ids - half_of * half
    leaving = (half_of[:, None] * half + turn[:, None] == device_ids[None, :]).astype(jnp.int32)
    leaving = jnp.sum(leaving * (crosses * lane_of)[:, None], axis=0)
    arriving = (dest_of[:, None] == device_ids[None, :]).astype(jnp.int32)
    table = jnp.concatenate([
        leaving,
        jnp.sum(arriving * crosses[:, None], axis=0),
        jnp.sum(arriving * ((1 - crosses) * lane_of)[:, None], axis=0),
        jnp.sum(arriving * (crosses * turn)[:, None], axis=0),
    ])
    first_weight = 1.0 / (1.0 + jnp.exp(route_logits[:, 1] - route_logits[:, 0]))
    second_weight = 1.0 / (1.0 + jnp.exp(route_logits[:, 0] - route_logits[:, 1]))
    coef = jnp.where(route_ids[:, 0:1] == expert_at[None, :], first_weight[:, None], 0.0)
    coef = coef + jnp.where(route_ids[:, 1:2] == expert_at[None, :], second_weight[:, None], 0.0)
    coef = jnp.pad(coef, ((0, 0), (0, LANES - n)))
    table, coef = lax.optimization_barrier((table, coef))
    levels = sorted({max(1, half * eighths // 8) for eighths in (3, 4, 5, 6, 8)})
    crossing = jnp.sum(crosses) // 2
    level = sum((crossing > most).astype(jnp.int32) for most in levels[:-1])
    branches = [functools.partial(call_layer, n, most, i) for i, most in enumerate(levels)]
    return lax.switch(level, branches, table, tokens, coef, held_gate, held_up, held_down)


def solution(mesh):
    split = ("groups", "expert")
    placed = (
        P(split, None),
        P(split, None),
        P(split, None),
        P(),
        P(),
        P(split, None, None),
        P(split, None, None),
        P(split, None, None),
    )
    return jax.shard_map(
        per_device,
        mesh=mesh,
        in_specs=placed,
        out_specs=(
            P(split, None),
            P(split, None, None),
            P(split, None, None),
            P(split, None, None),
        ),
        check_vma=False,
    )
```
